256 devices in a mesh: tm: 8 (over y, x_lo), space: 32 (over z, x_hi, core).
Axes of the slice: x: 4 (x_hi: 2, x_lo: 2; x = x_hi * 2 + x_lo), y: 4, z: 8, core: 2. Of those that a mesh axis runs over, the one named last changes fastest.
Arguments:
- conserved_field: float32 [16, 10, 64, 4096], P('tm', None, None, 'space'), may hold values from -6 to 6
- face_neighbours: int32 [2, 4096], P(None, 'space'), may hold values from 0 to 4095, as said below
- counterpart_group: int32 [16], P('tm'), may hold values from 0 to 31
- counterpart_shift: int32 [16], P('tm'), may hold values from 0 to 127
- volume_operator: float32 [2, 64, 64], replicated, may hold values from -0.75 to 0.75
- flux_matrix: float32 [2, 10, 10], replicated, may hold values from -2 to 2
Outputs:
- new_state: float32 [16, 10, 64, 4096], P('tm', None, None, 'space')
- last_residual: float32 [16, 10, 64, 4096], P('tm', None, None, 'space')
The draws below stay inside these ranges and needn't reach their ends.
Inputs may be any that keep to these rules, and one draw needn't show every extreme that they name: face_neighbours[0, e] = (e - d) mod 4096 and face_neighbours[1, e] = (e + d2) mod 4096 with 1 <= d, d2 <= 4; both distances 4 occur.
All inputs are finite; a program needn't handle non-finite values.
Results may differ from the reference program's by a relative error of at most 0.0001.
Values sent between devices are 32-bit elements; how exact they have to be, the bound alone decides.
A program may use at most 64 MiB of HBM per device.

```python
import jax
import jax.numpy as jnp
from jax import lax

SAMPLE_COUNT = 16
UNKNOWN_COUNT = 10
NODE_COUNT = 64
REACH = 4
ITERS = 2
CELLS_PER_SPLIT = 128
CELL_TOTAL = 4096
GROUP_COUNT = 32


def draw_face_neighbours(key, part):
    first_key, second_key = jax.random.split(jax.random.fold_in(key, 11))
    back_gap = jax.random.randint(first_key, (CELL_TOTAL,), 1, REACH + 1)
    ahead_gap = jax.random.randint(second_key, (CELL_TOTAL,), 1, REACH + 1)
    back_gap = back_gap.at[0].set(REACH)
    ahead_gap = ahead_gap.at[CELL_TOTAL - 1].set(REACH)
    elem_index = jnp.arange(CELL_TOTAL, dtype=jnp.int32)
    lower_side = (elem_index - back_gap) % CELL_TOTAL
    upper_side = (elem_index + ahead_gap) % CELL_TOTAL
    return jnp.stack([lower_side, upper_side]).astype(jnp.int32)


def place_ends(array, own_key, smallest, top_value):
    extent = array.shape
    spot = [jax.random.randint(jax.random.fold_in(own_key, axis), (), 0, extent[axis]) for axis in range(len(extent))]
    array = array.at[tuple(spot)].set(smallest)
    longest = extent.index(max(extent))
    spot[longest] = (spot[longest] + 1) % extent[longest]
    return array.at[tuple(spot)].set(top_value)


def steps_of(rng, dims, cuts, least, largest):
    def one(dim, shards_of):
        draws = jax.random.uniform(jax.random.fold_in(jax.random.fold_in(rng, 6), dim), (shards_of,), jnp.float32, least / len(cuts), largest / len(cuts))
        return jnp.repeat(jnp.exp(draws), dims[dim] // shards_of).reshape((-1,) + (1,) * (len(dims) - dim - 1))

    level = one(*cuts[0])
    for cut in cuts[1:]:
        level = level * one(*cut)
    return level


def normal_values(own_key, extent, deviation, bound, pieces=(), kind=jnp.bfloat16):
    gain = steps_of(own_key, extent, pieces, -0.22, 0.18) if pieces else 1.0
    array = jax.random.normal(own_key, extent, jnp.float32) * deviation * gain
    return jnp.minimum(jnp.maximum(array, -bound), bound).astype(kind)


def setup_inputs(seed: int = 0) -> dict:
    seeds = jax.random.split(jax.random.key(seed), 7)
    conserved_field = normal_values(seeds[0], (SAMPLE_COUNT, UNKNOWN_COUNT, NODE_COUNT, CELL_TOTAL), 1.0, 6.0, ((0, 8), (3, 32)), jnp.float32)
    face_neighbours = draw_face_neighbours(jax.random.fold_in(seeds[6], 71), 0)
    counterpart_group = place_ends(jax.random.randint(seeds[2], (SAMPLE_COUNT,), 0, GROUP_COUNT), jax.random.fold_in(seeds[2], 1), 0, GROUP_COUNT - 1).astype(jnp.int32)
    counterpart_shift = place_ends(jax.random.randint(seeds[3], (SAMPLE_COUNT,), 0, CELLS_PER_SPLIT), jax.random.fold_in(seeds[3], 1), 0, CELLS_PER_SPLIT - 1).astype(jnp.int32)
    volume_operator = normal_values(seeds[4], (2, NODE_COUNT, NODE_COUNT), NODE_COUNT ** -0.5, 0.75, (), jnp.float32)
    flux_matrix = normal_values(seeds[5], (2, UNKNOWN_COUNT, UNKNOWN_COUNT), UNKNOWN_COUNT ** -0.5, 2.0, (), jnp.float32)
    return {"conserved_field": conserved_field, "face_neighbours": face_neighbours, "counterpart_group": counterpart_group, "counterpart_shift": counterpart_shift, "volume_operator": volume_operator, "flux_matrix": flux_matrix}


lift_scale = 2.0
dissipation = 1.5
angular_speed = 0.5
damping_factor = 4.0
pseudo_step = 0.2


def face_traces(field):
    inst_count = field.shape[0]
    elem_count = field.shape[-1]
    cube_view = field.reshape(inst_count, UNKNOWN_COUNT, 4, 4, 4, elem_count)
    lower_face = cube_view[:, :, 0].reshape(inst_count, UNKNOWN_COUNT, 16, elem_count)
    upper_face = cube_view[:, :, 3].reshape(inst_count, UNKNOWN_COUNT, 16, elem_count)
    slide_face = cube_view[:, :, :, :, 3].reshape(inst_count, UNKNOWN_COUNT, 16, elem_count)
    return lower_face, upper_face, slide_face


def momentum_turning(boundary_samples, cycle_samples):
    blade_azimuth = 2.0 * jnp.pi * cycle_samples.astype(jnp.float32) / SAMPLE_COUNT
    cosine = jnp.cos(blade_azimuth)[:, None, None]
    sine = jnp.sin(blade_azimuth)[:, None, None]
    first_comp = boundary_samples[:, 1]
    second_comp = boundary_samples[:, 2]
    turned_one = cosine * first_comp - sine * second_comp
    turned_two = sine * first_comp + cosine * second_comp
    return jnp.concatenate([boundary_samples[:, :1], turned_one[:, None], turned_two[:, None], boundary_samples[:, 3:]], axis=1)


def face_term(matrix, normal_sign, outside, inside):
    jump = outside - inside
    mixed = jnp.einsum('vw,twqe->tvqe', matrix, jump, precision=lax.Precision.HIGHEST)
    return 0.5 * lift_scale * (normal_sign * mixed - dissipation * jump)


def assemble(lower_term, upper_term, slide_term):
    inst_count = lower_term.shape[0]
    elem_count = lower_term.shape[-1]
    shaped = (inst_count, UNKNOWN_COUNT, 4, 4, elem_count)
    corrections = jnp.zeros((inst_count, UNKNOWN_COUNT, 4, 4, 4, elem_count), lower_term.dtype)
    corrections = corrections.at[:, :, 0].add(lower_term.reshape(shaped))
    corrections = corrections.at[:, :, 3].add(upper_term.reshape(shaped))
    corrections = corrections.at[:, :, :, :, 3].add(slide_term.reshape(shaped))
    return corrections.reshape(inst_count, UNKNOWN_COUNT, NODE_COUNT, elem_count)


def residual_of(field, face_neighbours, counterpart_group, counterpart_shift, volume_operator, flux_matrix):
    fluxes = jnp.einsum('dvw,twpe->dtvpe', flux_matrix, field, precision=lax.Precision.HIGHEST)
    volume = jnp.einsum('dpq,dtvqe->tvpe', volume_operator, fluxes, precision=lax.Precision.HIGHEST)
    lower_face, upper_face, slide_face = face_traces(field)
    lower_out = jnp.take(upper_face, face_neighbours[0], axis=-1)
    upper_out = jnp.take(lower_face, face_neighbours[1], axis=-1)
    elem_index = jnp.arange(CELL_TOTAL, dtype=jnp.int32)
    partner = (elem_index[None, :] + counterpart_group[:, None] * CELLS_PER_SPLIT + counterpart_shift[:, None]) % CELL_TOTAL
    paired_boundary = jax.vmap(lambda rows_all, picks: jnp.take(rows_all, picks, axis=-1))(slide_face, partner)
    paired_boundary = momentum_turning(paired_boundary, jnp.arange(SAMPLE_COUNT, dtype=jnp.int32))
    corrections = assemble(face_term(flux_matrix[0], -1.0, lower_out, lower_face),
                           face_term(flux_matrix[0], 1.0, upper_out, upper_face),
                           face_term(flux_matrix[1], 1.0, paired_boundary, slide_face))
    frequency_content = jnp.fft.rfft(field, axis=0)
    fourier_wavenumbers = jnp.arange(SAMPLE_COUNT // 2 + 1).astype(jnp.float32)
    damped_signal = angular_speed * fourier_wavenumbers * jnp.exp(-damping_factor * (fourier_wavenumbers / (SAMPLE_COUNT // 2)) ** 8)
    damped_signal = jnp.where(fourier_wavenumbers < SAMPLE_COUNT // 2, damped_signal, 0.0)
    cyclic_signal = jnp.fft.irfft(1j * damped_signal[:, None, None, None] * frequency_content, n=SAMPLE_COUNT, axis=0)
    return volume + corrections + cyclic_signal.astype(field.dtype)


def reference(conserved_field, face_neighbours, counterpart_group, counterpart_shift, volume_operator, flux_matrix):
    field = conserved_field
    residual = jnp.zeros_like(field)
    for sweep_index in range(ITERS):
        residual = residual_of(field, face_neighbours, counterpart_group, counterpart_shift, volume_operator, flux_matrix)
        field = field - pseudo_step * residual
    return field, residual
```

```python
import math

import jax
import jax.numpy as jnp
from jax import lax
from jax.experimental import pallas as pl
from jax.experimental.pallas import tpu as pltpu
from jax.sharding import PartitionSpec as P

SAMPLE_COUNT = 16
REACH = 4
ITERS = 2
VARS = 10
NODES = 64
LANES = 128

lift_scale = 2.0
dissipation = 1.5
angular_speed = 0.5
damping_factor = 4.0
pseudo_step = 0.2

MESH = pl.DeviceIdType.MESH
TM = 8
SP = 32
Z = 8
Q = 4


def spectral_weights():
    half = SAMPLE_COUNT // 2
    weights = []
    for m in range(1, half):
        total = 0.0
        for k in range(1, half):
            gain = 2.0 * angular_speed * k * math.exp(-damping_factor * (k / half) ** 8) / SAMPLE_COUNT
            total += gain * math.sin(2.0 * math.pi * k * m / SAMPLE_COUNT)
        weights.append(total)
    return weights


def pick(index, values):
    out = jnp.float32(values[0])
    for k in range(1, len(values)):
        out = jnp.where(index == k, jnp.float32(values[k]), out)
    return out


def kernel(
    u_ref, fn_ref, group_ref, shift_ref, vol_ref, flux_ref,
    new_ref, res_ref,
    ub, a_hi, a_lo, gat, der, tem, ring_00, ring_01, ring_10, ring_11, cols_00, cols_01, cols_10, cols_11,
    packs, packed, side, lo_b, up_b, sl_b, in_sem, fs, fr, bs, br, zs, zr, cs, cr, ps, pr,
):
    ring = ((ring_00, ring_01), (ring_10, ring_11))
    cols = ((cols_00, cols_01), (cols_10, cols_11))
    tm = lax.axis_index("tm")
    sp = lax.axis_index("space")
    z = sp // Q
    q = sp % Q

    def space_of(zz, qq):
        return zz * Q + qq

    z_up = space_of((z + 1) % Z, q)
    z_dn = space_of((z + Z - 1) % Z, q)
    mate = space_of(z, q + 1 - 2 * (q % 2))
    cross = space_of(z, (q + 2) % Q)
    after = (sp + 1) % SP
    before = (sp + SP - 1) % SP

    load = pltpu.make_async_copy(u_ref, ub.at[0], in_sem)
    load.start()

    barrier = pltpu.get_barrier_semaphore()
    for k in range(1, TM):
        pl.semaphore_signal(barrier, inc=1, device_id={"tm": (tm + k) % TM}, device_id_type=MESH)
    for other in (z_up, z_dn, mate, cross, after, before):
        pl.semaphore_signal(barrier, inc=1, device_id={"space": other}, device_id_type=MESH)
    load.wait()
    pl.semaphore_wait(barrier, TM - 1 + 6)

    lane16 = lax.broadcasted_iota(jnp.int32, (16, LANES), 1)
    gidx = sp * LANES + lane16
    back_gap = jnp.bitwise_and(gidx - fn_ref[0:1, :], SP * LANES - 1)
    ahead_gap = jnp.bitwise_and(fn_ref[1:2, :] - gidx, SP * LANES - 1)

    weights = spectral_weights()
    cosines = [math.cos(2.0 * math.pi * k / SAMPLE_COUNT) for k in range(SAMPLE_COUNT)]
    sines = [math.sin(2.0 * math.pi * k / SAMPLE_COUNT) for k in range(SAMPLE_COUNT)]

    def rows_of(index):
        return pl.ds(pl.multiple_of(index * 8, 8), 8)

    def forward_copy(it, k):
        peer = (tm + k) % TM
        return pltpu.make_async_remote_copy(
            src_ref=ub.at[it, :, :, rows_of(peer), :], dst_ref=gat.at[it, tm],
            send_sem=fs.at[it, k], recv_sem=fr.at[it, k], device_id={"tm": peer}, device_id_type=MESH)

    def forward_arrival(it, k):
        peer = (tm + TM - k) % TM
        return pltpu.make_async_remote_copy(
            src_ref=ub.at[it, :, :, rows_of(peer), :], dst_ref=gat.at[it, peer],
            send_sem=fs.at[it, k], recv_sem=fr.at[it, k], device_id={"tm": peer}, device_id_type=MESH)

    def back_copy(it, k):
        peer = (tm + k) % TM
        return pltpu.make_async_remote_copy(
            src_ref=der.at[it, pl.ds(2 * peer, 2)], dst_ref=tem.at[it, :, :, rows_of(tm), :],
            send_sem=bs.at[it, k], recv_sem=br.at[it, k], device_id={"tm": peer}, device_id_type=MESH)

    def back_arrival(it, k):
        peer = (tm + TM - k) % TM
        return pltpu.make_async_remote_copy(
            src_ref=der.at[it, pl.ds(2 * peer, 2)], dst_ref=tem.at[it, :, :, rows_of(peer), :],
            send_sem=bs.at[it, k], recv_sem=br.at[it, k], device_id={"tm": peer}, device_id_type=MESH)

    def ring_copy(it, step, way, t):
        if way == 0:
            origin, target = (z + Z - (step - 1)) % Z, z_up
        else:
            origin, target = (z + step - 1) % Z, z_dn
        block = ring[it][t].at[origin]
        slot = ((step - 1) * 2 + way) * 2 + t
        return pltpu.make_async_remote_copy(
            src_ref=block, dst_ref=block, send_sem=zs.at[it, slot], recv_sem=zr.at[it, slot],
            device_id={"space": target}, device_id_type=MESH)

    def ring_arrival(it, step, way, t):
        if way == 0:
            origin, target = (z + Z - step) % Z, z_up
        else:
            origin, target = (z + step) % Z, z_dn
        block = ring[it][t].at[origin]
        slot = ((step - 1) * 2 + way) * 2 + t
        return pltpu.make_async_remote_copy(
            src_ref=block, dst_ref=block, send_sem=zs.at[it, slot], recv_sem=zr.at[it, slot],
            device_id={"space": target}, device_id_type=MESH)

    def column_copy(it, kind, t):
        origin, target = ((q, mate), (q, cross), ((q + 2) % Q, mate))[kind]
        block = cols[it][t].at[origin]
        slot = kind * 2 + t
        return pltpu.make_async_remote_copy(
            src_ref=block, dst_ref=block, send_sem=cs.at[it, slot], recv_sem=cr.at[it, slot],
            device_id={"space": target}, device_id_type=MESH)

    def column_arrival(it, kind, t):
        mate_q = q + 1 - 2 * (q % 2)
        origin, target = ((mate_q, mate), ((q + 2) % Q, cross), ((mate_q + 2) % Q, mate))[kind]
        block = cols[it][t].at[origin]
        slot = kind * 2 + t
        return pltpu.make_async_remote_copy(
            src_ref=block, dst_ref=block, send_sem=cs.at[it, slot], recv_sem=cr.at[it, slot],
            device_id={"space": target}, device_id_type=MESH)

    def pack_copy(it, way):
        target = (after, before)[way]
        return pltpu.make_async_remote_copy(
            src_ref=packs.at[it, way], dst_ref=packed.at[it, way], send_sem=ps.at[it, way], recv_sem=pr.at[it, way],
            device_id={"space": target}, device_id_type=MESH)

    def ring_steps(step):
        return ((0, 0), (1, 0), (0, 1), (1, 1)) if step < 4 else ((0, 0), (1, 1))

    def build_matrix():
        row = lax.broadcasted_iota(jnp.int32, (NODES, LANES), 0)
        lane = lax.broadcasted_iota(jnp.int32, (NODES, LANES), 1)
        first = lane < NODES
        on = row == jnp.bitwise_and(lane, NODES - 1)
        one, zero = jnp.float32(1.0), jnp.float32(0.0)
        lower = jnp.where(on & (row < 16), one, zero)
        upper = jnp.where(on & (row >= 48), one, zero)
        slide = jnp.where(on & (jnp.bitwise_and(row, 3) == 3), one, zero)
        scale = jnp.float32(0.5 * lift_scale)
        side[0] = vol_ref[0] + scale * (lower - upper)
        side[1] = vol_ref[1] - scale * slide
        side[2] = (scale * jnp.float32(dissipation)) * (lower + upper + slide)

        def row_block(v, carry):
            for j in range(VARS // 2):
                tile = jnp.zeros((NODES, LANES), jnp.float32)
                for d in range(2):
                    factor = jnp.where(first, flux_ref[d, v, 2 * j], flux_ref[d, v, 2 * j + 1])
                    tile = tile + factor * side[d]
                own = jnp.where(first, jnp.where(v == 2 * j, one, zero), jnp.where(v == 2 * j + 1, one, zero))
                tile = tile + own * side[2]
                high = tile.astype(jnp.bfloat16)
                where = (pl.ds(pl.multiple_of(v * NODES, NODES), NODES), pl.ds(j * LANES, LANES))
                a_hi[where] = high
                a_lo[where] = (tile - high.astype(jnp.float32)).astype(jnp.bfloat16)
            return carry

        lax.fori_loop(0, VARS, row_block, 0)

    def volume_part(it):
        u = jnp.concatenate(
            [ub[it, 0].reshape(VARS * NODES, LANES), ub[it, 1].reshape(VARS * NODES, LANES)], axis=1)
        high = u.astype(jnp.bfloat16)
        low = (u - high.astype(jnp.float32)).astype(jnp.bfloat16)
        for part in range(2):
            rows = pl.ds(part * 320, 320)
            out = jnp.dot(a_hi[rows, :], high, preferred_element_type=jnp.float32)
            out = out + jnp.dot(a_hi[rows, :], low, preferred_element_type=jnp.float32)
            out = out + jnp.dot(a_lo[rows, :], high, preferred_element_type=jnp.float32)
            for t in range(2):
                res_ref[t, pl.ds(part * 5, 5)] = out[:, t * LANES:(t + 1) * LANES].reshape(5, NODES, LANES)

    def iteration(it):
        for t in range(2):
            ring[it][t][z] = ub[it, t, :, pl.ds(3, 16, stride=4), :]
        for way, t in ring_steps(1):
            ring_copy(it, 1, way, t).start()
        for k in range(1, TM):
            forward_copy(it, k).start()
        up_pack = jnp.zeros((16, LANES), jnp.float32)
        lo_pack = jnp.zeros((16, LANES), jnp.float32)
        for i in range(2 * VARS):
            mine = (lane16 >= REACH * i) & (lane16 < REACH * (i + 1))
            u_face = ub[it, i // VARS, i % VARS, pl.ds(48, 16), :]
            l_face = ub[it, i // VARS, i % VARS, pl.ds(0, 16), :]
            up_pack = jnp.where(mine, pltpu.roll(u_face, (REACH * i + REACH) % LANES, 1), up_pack)
            lo_pack = jnp.where(mine, pltpu.roll(l_face, REACH * i, 1) if i else l_face, lo_pack)
        packs[it, 0] = up_pack
        packs[it, 1] = lo_pack
        for way in range(2):
            pack_copy(it, way).start()
        gat[it, tm] = ub[it, :, :, rows_of(tm), :]

        if it == 0:
            build_matrix()

        volume_part(it)

        for way, t in ring_steps(1):
            ring_arrival(it, 1, way, t).wait_recv()
            if (way, t) in ring_steps(2):
                ring_copy(it, 2, way, t).start()

        for way in range(2):
            pack_copy(it, way).wait_recv()
        from_before = packed[it, 0]
        from_after = packed[it, 1]
        behind = lane16 - back_gap
        ahead = lane16 + ahead_gap
        for i in range(2 * VARS):
            u_face = ub[it, i // VARS, i % VARS, pl.ds(48, 16), :]
            l_face = ub[it, i // VARS, i % VARS, pl.ds(0, 16), :]
            own = jnp.take_along_axis(u_face, jnp.bitwise_and(behind, LANES - 1), axis=1)
            far = jnp.take_along_axis(from_before, jnp.bitwise_and(behind + REACH * (i + 1), LANES - 1), axis=1)
            lo_b[i // VARS, i % VARS] = jnp.where(behind < 0, far, own)
            own = jnp.take_along_axis(l_face, jnp.bitwise_and(ahead, LANES - 1), axis=1)
            far = jnp.take_along_axis(from_after, jnp.bitwise_and(ahead + REACH * i, LANES - 1), axis=1)
            up_b[i // VARS, i % VARS] = jnp.where(ahead >= LANES, far, own)

        scale = jnp.float32(0.5 * lift_scale)
        loss = jnp.float32(0.5 * lift_scale * dissipation)

        def first_faces(v, c):
            low = -loss * lo_b[:, v]
            upp = -loss * up_b[:, v]
            for w in range(VARS):
                f = scale * flux_ref[0, v, w]
                low = low - f * lo_b[:, w]
                upp = upp + f * up_b[:, w]
            res_ref[:, v, pl.ds(0, 16), :] += low
            res_ref[:, v, pl.ds(48, 16), :] += upp
            return c

        lax.fori_loop(0, VARS, first_faces, 0)

        for way, t in ring_steps(2):
            ring_arrival(it, 2, way, t).wait_recv()
            if (way, t) in ring_steps(3):
                ring_copy(it, 3, way, t).start()

        for k in range(1, TM):
            forward_arrival(it, k).wait_recv()

        def derive(v, c):
            x = [gat[it, t // 2, t % 2, v] for t in range(SAMPLE_COUNT)]
            diff = {}
            for t in range(SAMPLE_COUNT // 2):
                for m in range(1, SAMPLE_COUNT // 2):
                    diff[t, m] = x[(t + m) % SAMPLE_COUNT] - x[(t - m) % SAMPLE_COUNT]
            for t in range(SAMPLE_COUNT // 2):
                near = jnp.float32(weights[0]) * diff[t, 1]
                opposite = jnp.float32(-weights[SAMPLE_COUNT // 2 - 2]) * diff[t, 1]
                for m in range(2, SAMPLE_COUNT // 2):
                    near = near + jnp.float32(weights[m - 1]) * diff[t, m]
                    opposite = opposite - jnp.float32(weights[SAMPLE_COUNT // 2 - m - 1]) * diff[t, m]
                der[it, t, v] = near
                der[it, t + SAMPLE_COUNT // 2, v] = opposite
            return c

        lax.fori_loop(0, VARS, derive, 0)
        for k in range(1, TM):
            back_copy(it, k).start()
        tem[it, :, :, rows_of(tm), :] = der[it, pl.ds(2 * tm, 2)]

        for way, t in ring_steps(3):
            ring_arrival(it, 3, way, t).wait_recv()
            if (way, t) in ring_steps(4):
                ring_copy(it, 4, way, t).start()
        for way, t in ring_steps(4):
            ring_arrival(it, 4, way, t).wait_recv()

        lane_b = lax.broadcasted_iota(jnp.int32, (VARS, 16, LANES), 2)
        for t in range(2):
            group, shift = group_ref[t], shift_ref[t]
            first_dst = jnp.bitwise_and(q - group, Q - 1)
            second_dst = jnp.bitwise_and(q - group - 1, Q - 1)
            first = jnp.bitwise_and(z + lax.shift_right_arithmetic(first_dst + group - q, 2), Z - 1)
            second = jnp.bitwise_and(z + lax.shift_right_arithmetic(second_dst + group + 1 - q, 2), Z - 1)
            cols[it][t][q] = jnp.where(lane_b >= shift, ring[it][t][first], ring[it][t][second])
            column_copy(it, 1, t).start()
            column_copy(it, 0, t).start()
        for t in range(2):
            column_arrival(it, 1, t).wait_recv()
            column_copy(it, 2, t).start()
        for t in range(2):
            group, shift = group_ref[t], shift_ref[t]
            column_arrival(it, 0, t).wait_recv()
            column_arrival(it, 2, t).wait_recv()
            first = cols[it][t][jnp.bitwise_and(q + group, Q - 1)]
            second = cols[it][t][jnp.bitwise_and(q + group + 1, Q - 1)]
            both = jnp.where(lane_b >= shift, first, second)
            both = pltpu.roll(both.reshape(VARS * 16, LANES), jnp.bitwise_and(LANES - shift, LANES - 1), 1)
            sl_b[t] = both.reshape(VARS, 16, LANES)
            cosine, sine = pick(2 * tm + t, cosines), pick(2 * tm + t, sines)
            one, two = sl_b[t, 1], sl_b[t, 2]
            sl_b[t, 1] = cosine * one - sine * two
            sl_b[t, 2] = sine * one + cosine * two

        for k in range(1, TM):
            back_arrival(it, k).wait_recv()

        def finish(v, c):
            for t in range(2):
                term = -loss * sl_b[t, v]
                for w in range(VARS):
                    term = term + (scale * flux_ref[1, v, w]) * sl_b[t, w]
                res_ref[t, v, pl.ds(3, 16, stride=4), :] += term
                total = res_ref[t, v] + tem[it, t, v]
                res_ref[t, v] = total
                following = ub[it, t, v] - jnp.float32(pseudo_step) * total
                ub[it + 1, t, v] = following
                new_ref[t, v] = following
            return c

        lax.fori_loop(0, VARS, finish, 0)

        for k in range(1, TM):
            forward_copy(it, k).wait_send()
            back_copy(it, k).wait_send()
        for step in range(1, 5):
            for way, t in ring_steps(step):
                ring_copy(it, step, way, t).wait_send()
        for kind in range(3):
            for t in range(2):
                column_copy(it, kind, t).wait_send()
        for way in range(2):
            pack_copy(it, way).wait_send()

    for it in range(ITERS):
        iteration(it)


def per_device(conserved_field, face_neighbours, counterpart_group, counterpart_shift, volume_operator, flux_matrix):
    wide = jnp.concatenate([volume_operator, volume_operator], axis=2)
    state = jax.ShapeDtypeStruct(conserved_field.shape, jnp.float32)
    vmem = pl.BlockSpec(memory_space=pltpu.VMEM)
    smem = pl.BlockSpec(memory_space=pltpu.SMEM)
    f32, bf16 = jnp.float32, jnp.bfloat16
    dma = pltpu.SemaphoreType.DMA
    return pl.pallas_call(
        kernel,
        out_shape=(state, state),
        in_specs=[pl.BlockSpec(memory_space=pl.ANY), vmem, smem, smem, vmem, smem],
        out_specs=(vmem, vmem),
        scratch_shapes=[
            pltpu.VMEM((ITERS + 1, 2, VARS, NODES, LANES), f32),
            pltpu.VMEM((VARS * NODES, VARS * NODES), bf16),
            pltpu.VMEM((VARS * NODES, VARS * NODES), bf16),
            pltpu.VMEM((ITERS, TM, 2, VARS, 8, LANES), f32),
            pltpu.VMEM((ITERS, SAMPLE_COUNT, VARS, 8, LANES), f32),
            pltpu.VMEM((ITERS, 2, VARS, NODES, LANES), f32),
            *[pltpu.VMEM((Z, VARS, 16, LANES), f32)] * 4,
            *[pltpu.VMEM((Q, VARS, 16, LANES), f32)] * 4,
            pltpu.VMEM((ITERS, 2, 16, LANES), f32),
            pltpu.VMEM((ITERS, 2, 16, LANES), f32),
            pltpu.VMEM((3, NODES, LANES), f32),
            pltpu.VMEM((2, VARS, 16, LANES), f32),
            pltpu.VMEM((2, VARS, 16, LANES), f32),
            pltpu.VMEM((2, VARS, 16, LANES), f32),
            dma,
            dma((ITERS, TM)), dma((ITERS, TM)),
            dma((ITERS, TM)), dma((ITERS, TM)),
            dma((ITERS, 16)), dma((ITERS, 16)),
            dma((ITERS, 6)), dma((ITERS, 6)),
            dma((ITERS, 2)), dma((ITERS, 2)),
        ],
        compiler_params=pltpu.CompilerParams(
            collective_id=0, has_side_effects=True, vmem_limit_bytes=48 * 1024 * 1024),
        name="iterations",
    )(conserved_field, face_neighbours, counterpart_group, counterpart_shift, wide, flux_matrix)


def solution(mesh):
    return jax.shard_map(
        per_device,
        mesh=mesh,
        in_specs=(P("tm", None, None, "space"), P(None, "space"), P("tm"), P("tm"), P(), P()),
        out_specs=(P("tm", None, None, "space"), P("tm", None, None, "space")),
        check_vma=False,
    )
```

```python
import math

import jax
import jax.numpy as jnp
from jax import lax
from jax.experimental import pallas as pl
from jax.experimental.pallas import tpu as pltpu
from jax.sharding import PartitionSpec as P

SAMPLE_COUNT = 16
REACH = 4
ITERS = 2
VARS = 10
NODES = 64
LANES = 128
PARTS = 2
PIECE = VARS // PARTS

lift_scale = 2.0
dissipation = 1.5
angular_speed = 0.5
damping_factor = 4.0
pseudo_step = 0.2

MESH = pl.DeviceIdType.MESH
TM = 8
SP = 32
Z = 8
Q = 4


def spectral_weights():
    half = SAMPLE_COUNT // 2
    weights = []
    for m in range(1, half):
        total = 0.0
        for k in range(1, half):
            gain = 2.0 * angular_speed * k * math.exp(-damping_factor * (k / half) ** 8) / SAMPLE_COUNT
            total += gain * math.sin(2.0 * math.pi * k * m / SAMPLE_COUNT)
        weights.append(total)
    return weights


def pick(index, values):
    out = jnp.float32(values[0])
    for k in range(1, len(values)):
        out = jnp.where(index == k, jnp.float32(values[k]), out)
    return out


def kernel(
    u_ref, fn_ref, group_ref, shift_ref, vol_ref, flux_ref,
    new_ref, res_ref,
    ub, a_hi, a_lo, gat, der, tem, ring_00, ring_01, ring_10, ring_11, cols_00, cols_01, cols_10, cols_11, cols_20, cols_21,
    packs, packed, side, lo_b, up_b, sl_b, tw_b, in_sem, fs, fr, bs, br, zs, zr, cs, cr, ps, pr,
):
    ring = ((ring_00, ring_01), (ring_10, ring_11))
    cols = ((cols_00, cols_01), (cols_10, cols_11), (cols_20, cols_21))
    tm = lax.axis_index("tm")
    sp = lax.axis_index("space")
    z = sp // Q
    q = sp % Q

    def space_of(zz, qq):
        return zz * Q + qq

    z_up = space_of((z + 1) % Z, q)
    z_dn = space_of((z + Z - 1) % Z, q)
    mate = space_of(z, q + 1 - 2 * (q % 2))
    cross = space_of(z, (q + 2) % Q)
    after = (sp + 1) % SP
    before = (sp + SP - 1) % SP

    load = pltpu.make_async_copy(u_ref, ub.at[0], in_sem)
    load.start()

    barrier = pltpu.get_barrier_semaphore()
    for k in range(1, TM):
        pl.semaphore_signal(barrier, inc=1, device_id={"tm": (tm + k) % TM}, device_id_type=MESH)
    for other in (z_up, z_dn, mate, cross, after, before):
        pl.semaphore_signal(barrier, inc=1, device_id={"space": other}, device_id_type=MESH)
    with jax.named_scope("entry"):
        load.wait()
        pl.semaphore_wait(barrier, TM - 1 + 6)

    lane16 = lax.broadcasted_iota(jnp.int32, (16, LANES), 1)
    gidx = sp * LANES + lane16
    back_gap = jnp.bitwise_and(gidx - fn_ref[0:1, :], SP * LANES - 1)
    ahead_gap = jnp.bitwise_and(fn_ref[1:2, :] - gidx, SP * LANES - 1)

    weights = spectral_weights()
    cosines = [math.cos(2.0 * math.pi * k / SAMPLE_COUNT) for k in range(SAMPLE_COUNT)]
    sines = [math.sin(2.0 * math.pi * k / SAMPLE_COUNT) for k in range(SAMPLE_COUNT)]

    def rows_of(index):
        return pl.ds(pl.multiple_of(index * 8, 8), 8)

    def forward_copy(it, k):
        peer = (tm + k) % TM
        return pltpu.make_async_remote_copy(
            src_ref=ub.at[it, :, :, rows_of(peer), :], dst_ref=gat.at[it, tm],
            send_sem=fs.at[it, k], recv_sem=fr.at[it, k], device_id={"tm": peer}, device_id_type=MESH)

    def forward_arrival(it, k):
        peer = (tm + TM - k) % TM
        return pltpu.make_async_remote_copy(
            src_ref=ub.at[it, :, :, rows_of(peer), :], dst_ref=gat.at[it, peer],
            send_sem=fs.at[it, k], recv_sem=fr.at[it, k], device_id={"tm": peer}, device_id_type=MESH)

    def back_copy(it, k):
        peer = (tm + k) % TM
        return pltpu.make_async_remote_copy(
            src_ref=der.at[it, pl.ds(2 * peer, 2)], dst_ref=tem.at[it, :, :, rows_of(tm), :],
            send_sem=bs.at[it, k], recv_sem=br.at[it, k], device_id={"tm": peer}, device_id_type=MESH)

    def back_arrival(it, k):
        peer = (tm + TM - k) % TM
        return pltpu.make_async_remote_copy(
            src_ref=der.at[it, pl.ds(2 * peer, 2)], dst_ref=tem.at[it, :, :, rows_of(peer), :],
            send_sem=bs.at[it, k], recv_sem=br.at[it, k], device_id={"tm": peer}, device_id_type=MESH)

    def ring_slot(step, way, t, part):
        return (((step - 1) * 2 + way) * 2 + t) * PARTS + part

    def ring_copy(it, step, way, t, part):
        if way == 0:
            origin, target = (z + Z - (step - 1)) % Z, z_up
        else:
            origin, target = (z + step - 1) % Z, z_dn
        block = ring[it][t].at[origin, pl.ds(part * PIECE, PIECE)]
        slot = ring_slot(step, way, t, part)
        return pltpu.make_async_remote_copy(
            src_ref=block, dst_ref=block, send_sem=zs.at[it, slot], recv_sem=zr.at[it, slot],
            device_id={"space": target}, device_id_type=MESH)

    def ring_arrival(it, step, way, t, part):
        if way == 0:
            origin, target = (z + Z - step) % Z, z_up
        else:
            origin, target = (z + step) % Z, z_dn
        block = ring[it][t].at[origin, pl.ds(part * PIECE, PIECE)]
        slot = ring_slot(step, way, t, part)
        return pltpu.make_async_remote_copy(
            src_ref=block, dst_ref=block, send_sem=zs.at[it, slot], recv_sem=zr.at[it, slot],
            device_id={"space": target}, device_id_type=MESH)

    def column_copy(kind, hop, t):
        origin, target = ((q, mate), (q, cross), ((q + 2) % Q, mate))[hop]
        block = cols[kind][t].at[origin]
        slot = hop * 2 + t
        return pltpu.make_async_remote_copy(
            src_ref=block, dst_ref=block, send_sem=cs.at[kind, slot], recv_sem=cr.at[kind, slot],
            device_id={"space": target}, device_id_type=MESH)

    def column_arrival(kind, hop, t):
        mate_q = q + 1 - 2 * (q % 2)
        origin, target = ((mate_q, mate), ((q + 2) % Q, cross), ((mate_q + 2) % Q, mate))[hop]
        block = cols[kind][t].at[origin]
        slot = hop * 2 + t
        return pltpu.make_async_remote_copy(
            src_ref=block, dst_ref=block, send_sem=cs.at[kind, slot], recv_sem=cr.at[kind, slot],
            device_id={"space": target}, device_id_type=MESH)

    def pack_copy(it, way):
        target = (after, before)[way]
        return pltpu.make_async_remote_copy(
            src_ref=packs.at[it, way], dst_ref=packed.at[it, way], send_sem=ps.at[it, way], recv_sem=pr.at[it, way],
            device_id={"space": target}, device_id_type=MESH)

    def build_matrix():
        row = lax.broadcasted_iota(jnp.int32, (NODES, LANES), 0)
        lane = lax.broadcasted_iota(jnp.int32, (NODES, LANES), 1)
        first = lane < NODES
        on = row == jnp.bitwise_and(lane, NODES - 1)
        one, zero = jnp.float32(1.0), jnp.float32(0.0)
        lower = jnp.where(on & (row < 16), one, zero)
        upper = jnp.where(on & (row >= 48), one, zero)
        slide = jnp.where(on & (jnp.bitwise_and(row, 3) == 3), one, zero)
        scale = jnp.float32(0.5 * lift_scale)
        side[0] = jnp.concatenate([vol_ref[0], vol_ref[0]], axis=1) + scale * (lower - upper)
        side[1] = jnp.concatenate([vol_ref[1], vol_ref[1]], axis=1) - scale * slide
        side[2] = (scale * jnp.float32(dissipation)) * (lower + upper + slide)

        def row_block(v, carry):
            for j in range(VARS // 2):
                tile = jnp.zeros((NODES, LANES), jnp.float32)
                for d in range(2):
                    factor = jnp.where(first, flux_ref[v, d, 2 * j], flux_ref[v, d, 2 * j + 1])
                    tile = tile + factor * side[d]
                own = jnp.where(first, jnp.where(v == 2 * j, one, zero), jnp.where(v == 2 * j + 1, one, zero))
                tile = tile + own * side[2]
                high = tile.astype(jnp.bfloat16)
                where = (pl.ds(pl.multiple_of(v * NODES, NODES), NODES), pl.ds(j * LANES, LANES))
                a_hi[where] = high
                a_lo[where] = (tile - high.astype(jnp.float32)).astype(jnp.bfloat16)
            return carry

        lax.fori_loop(0, VARS, row_block, 0)

    def volume_part(it):
        u = jnp.concatenate(
            [ub[it, 0].reshape(VARS * NODES, LANES), ub[it, 1].reshape(VARS * NODES, LANES)], axis=1)
        high = u.astype(jnp.bfloat16)
        low = (u - high.astype(jnp.float32)).astype(jnp.bfloat16)
        for part in range(2):
            rows = pl.ds(part * 320, 320)
            out = jnp.dot(a_hi[rows, :], high, preferred_element_type=jnp.float32)
            out = out + jnp.dot(a_hi[rows, :], low, preferred_element_type=jnp.float32)
            out = out + jnp.dot(a_lo[rows, :], high, preferred_element_type=jnp.float32)
            for t in range(2):
                res_ref[t, pl.ds(part * 5, 5)] = out[:, t * LANES:(t + 1) * LANES].reshape(5, NODES, LANES)

    def ring_chunks(step, t):
        ways = (0, 1) if step < 4 else (t,)
        return [(way, part) for part in range(PARTS) for way in ways]

    def ring_start(it, t):
        for way, part in ring_chunks(1, t):
            ring_copy(it, 1, way, t, part).start()

    def ring_relay(it, step, t):
        onward = ring_chunks(step + 1, t) if step < 4 else []
        for way, part in ring_chunks(step, t):
            ring_arrival(it, step, way, t, part).wait_recv()
            if (way, part) in onward:
                ring_copy(it, step + 1, way, t, part).start()

    def pack_traces(it):
        up_pack = jnp.zeros((16, LANES), jnp.float32)
        lo_pack = jnp.zeros((16, LANES), jnp.float32)
        for i in range(2 * VARS):
            mine = (lane16 >= REACH * i) & (lane16 < REACH * (i + 1))
            u_face = ub[it, i // VARS, i % VARS, pl.ds(48, 16), :]
            l_face = ub[it, i // VARS, i % VARS, pl.ds(0, 16), :]
            up_pack = jnp.where(mine, pltpu.roll(u_face, (REACH * i + REACH) % LANES, 1), up_pack)
            lo_pack = jnp.where(mine, pltpu.roll(l_face, REACH * i, 1) if i else l_face, lo_pack)
        packs[it, 0] = up_pack
        packs[it, 1] = lo_pack
        for way in range(2):
            pack_copy(it, way).start()

    scale = jnp.float32(0.5 * lift_scale)
    loss = jnp.float32(0.5 * lift_scale * dissipation)

    def first_direction(it):
        for way in range(2):
            pack_copy(it, way).wait_recv()
        from_before = packed[it, 0]
        from_after = packed[it, 1]
        behind = lane16 - back_gap
        ahead = lane16 + ahead_gap
        for i in range(2 * VARS):
            u_face = ub[it, i // VARS, i % VARS, pl.ds(48, 16), :]
            l_face = ub[it, i // VARS, i % VARS, pl.ds(0, 16), :]
            own = jnp.take_along_axis(u_face, jnp.bitwise_and(behind, LANES - 1), axis=1)
            far = jnp.take_along_axis(from_before, jnp.bitwise_and(behind + REACH * (i + 1), LANES - 1), axis=1)
            lo_b[i // VARS, i % VARS] = jnp.where(behind < 0, far, own)
            own = jnp.take_along_axis(l_face, jnp.bitwise_and(ahead, LANES - 1), axis=1)
            far = jnp.take_along_axis(from_after, jnp.bitwise_and(ahead + REACH * i, LANES - 1), axis=1)
            up_b[i // VARS, i % VARS] = jnp.where(ahead >= LANES, far, own)

        def first_faces(v, c):
            low = -loss * lo_b[:, v]
            upp = -loss * up_b[:, v]
            for w in range(VARS):
                f = scale * flux_ref[v, 0, w]
                low = low - f * lo_b[:, w]
                upp = upp + f * up_b[:, w]
            res_ref[:, v, pl.ds(0, 16), :] += low
            res_ref[:, v, pl.ds(48, 16), :] += upp
            return c

        lax.fori_loop(0, VARS, first_faces, 0)

    def time_derivative(it):
        for k in range(1, TM):
            forward_arrival(it, k).wait_recv()

        def derive(v, c):
            x = [gat[it, t // 2, t % 2, v] for t in range(SAMPLE_COUNT)]
            diff = {}
            for t in range(SAMPLE_COUNT // 2):
                for m in range(1, SAMPLE_COUNT // 2):
                    diff[t, m] = x[(t + m) % SAMPLE_COUNT] - x[(t - m) % SAMPLE_COUNT]
            for t in range(SAMPLE_COUNT // 2):
                near = jnp.float32(weights[0]) * diff[t, 1]
                opposite = jnp.float32(-weights[SAMPLE_COUNT // 2 - 2]) * diff[t, 1]
                for m in range(2, SAMPLE_COUNT // 2):
                    near = near + jnp.float32(weights[m - 1]) * diff[t, m]
                    opposite = opposite - jnp.float32(weights[SAMPLE_COUNT // 2 - m - 1]) * diff[t, m]
                der[it, t, v] = near
                der[it, t + SAMPLE_COUNT // 2, v] = opposite
            return c

        lax.fori_loop(0, VARS, derive, 0)
        for k in range(1, TM):
            back_copy(it, k).start()
        tem[it, :, :, rows_of(tm), :] = der[it, pl.ds(2 * tm, 2)]

    def offset_of(kind, t):
        group, shift = group_ref[t], shift_ref[t]
        if kind == 1:
            group = jnp.bitwise_and(2 * group + lax.shift_right_arithmetic(shift, 6), SP - 1)
            shift = jnp.bitwise_and(2 * shift, LANES - 1)
        return group, shift

    lane_b = lax.broadcasted_iota(jnp.int32, (VARS, 16, LANES), 2)

    def column_start(kind, t):
        it = kind // 2
        group, shift = offset_of(kind, t)
        first_dst = jnp.bitwise_and(q - group, Q - 1)
        second_dst = jnp.bitwise_and(q - group - 1, Q - 1)
        first = jnp.bitwise_and(z + lax.shift_right_arithmetic(first_dst + group - q, 2), Z - 1)
        second = jnp.bitwise_and(z + lax.shift_right_arithmetic(second_dst + group + 1 - q, 2), Z - 1)
        cols[kind][t][q] = jnp.where(lane_b >= shift, ring[it][t][first], ring[it][t][second])
        column_copy(kind, 1, t).start()
        column_copy(kind, 0, t).start()

    def column_relay(kind, t):
        column_arrival(kind, 1, t).wait_recv()
        column_copy(kind, 2, t).start()

    def column_finish(kind, t):
        column_arrival(kind, 0, t).wait_recv()
        column_arrival(kind, 2, t).wait_recv()
        group, shift = offset_of(kind, t)
        first = cols[kind][t][jnp.bitwise_and(q + group, Q - 1)]
        second = cols[kind][t][jnp.bitwise_and(q + group + 1, Q - 1)]
        both = jnp.where(lane_b >= shift, first, second)
        both = pltpu.roll(both.reshape(VARS * 16, LANES), jnp.bitwise_and(LANES - shift, LANES - 1), 1)
        return both.reshape(VARS, 16, LANES)

    def turn(t):
        cosine, sine = pick(2 * tm + t, cosines), pick(2 * tm + t, sines)
        one, two = sl_b[t, 1], sl_b[t, 2]
        sl_b[t, 1] = cosine * one - sine * two
        sl_b[t, 2] = sine * one + cosine * two

    def slide_term(t, v):
        term = -loss * sl_b[t, v]
        for w in range(VARS):
            term = term + (scale * flux_ref[v, 1, w]) * sl_b[t, w]
        return term

    step_size = jnp.float32(pseudo_step)
    scope = jax.named_scope

    with scope("start0"):
        for t in range(2):
            ring[0][t][z] = ub[0, t, :, pl.ds(3, 16, stride=4), :]
            ring_start(0, t)
        for k in range(1, TM):
            forward_copy(0, k).start()
        pack_traces(0)
        gat[0, tm] = ub[0, :, :, rows_of(tm), :]
    with scope("matrix"):
        build_matrix()
    with scope("volume0"):
        volume_part(0)
    with scope("ring0_1"):
        ring_relay(0, 1, 0)
        ring_relay(0, 1, 1)
    with scope("ring0_2a"):
        ring_relay(0, 2, 0)
    with scope("derive0"):
        time_derivative(0)
    with scope("ring0_2b"):
        ring_relay(0, 2, 1)
    with scope("first0"):
        first_direction(0)
    with scope("ring0_3"):
        ring_relay(0, 3, 0)
        ring_relay(0, 3, 1)
    with scope("ring0_4"):
        for t in range(2):
            ring_relay(0, 4, t)
            column_start(0, t)
    with scope("back0"):
        for k in range(1, TM):
            back_arrival(0, k).wait_recv()

    def partial_state(v, c):
        for t in range(2):
            ub[1, t, v] = ub[0, t, v] - step_size * (res_ref[t, v] + tem[0, t, v])
        return c

    with scope("w"):
        lax.fori_loop(0, VARS, partial_state, 0)
        for t in range(2):
            ring[1][t][z] = ub[1, t, :, pl.ds(3, 16, stride=4), :]
            ring_start(1, t)
    with scope("cols1_start"):
        for t in range(2):
            column_start(1, t)
    with scope("ring1_1a"):
        ring_relay(1, 1, 0)
    with scope("cols0_relay"):
        for t in range(2):
            column_relay(0, t)
    with scope("ring1_1b"):
        ring_relay(1, 1, 1)
    with scope("cols0_finish"):
        for t in range(2):
            sl_b[t] = column_finish(0, t)
            turn(t)

    def next_state(v, c):
        for t in range(2):
            ub[1, t, v, pl.ds(3, 16, stride=4), :] += -step_size * slide_term(t, v)
        return c

    with scope("u1"):
        lax.fori_loop(0, VARS, next_state, 0)
        for k in range(1, TM):
            forward_copy(1, k).start()
        pack_traces(1)
        gat[1, tm] = ub[1, :, :, rows_of(tm), :]
    with scope("volume1"):
        volume_part(1)
    with scope("ring1_2"):
        ring_relay(1, 2, 0)
    with scope("cols1_relay"):
        for t in range(2):
            column_relay(1, t)
    with scope("ring1_2b"):
        ring_relay(1, 2, 1)
    with scope("cols1_finish"):
        for t in range(2):
            sl_b[t] = column_finish(1, t)
            turn(t)

        def twice(v, c):
            for t in range(2):
                tw_b[t, v] = step_size * slide_term(t, v)
            return c

        lax.fori_loop(0, VARS, twice, 0)
    with scope("first1"):
        first_direction(1)
    with scope("ring1_3"):
        ring_relay(1, 3, 0)
        ring_relay(1, 3, 1)
    with scope("derive1"):
        time_derivative(1)
    with scope("ring1_4"):
        for t in range(2):
            ring_relay(1, 4, t)
            column_start(2, t)
    with scope("cols2_relay"):
        for t in range(2):
            column_relay(2, t)
    with scope("cols2_finish"):
        for t in range(2):
            sl_b[t] = column_finish(2, t) - tw_b[t]
            turn(t)
    with scope("back1"):
        for k in range(1, TM):
            back_arrival(1, k).wait_recv()

    def finish(v, c):
        for t in range(2):
            res_ref[t, v, pl.ds(3, 16, stride=4), :] += slide_term(t, v)
            total = res_ref[t, v] + tem[1, t, v]
            res_ref[t, v] = total
            new_ref[t, v] = ub[1, t, v] - step_size * total
        return c

    with scope("finish"):
        lax.fori_loop(0, VARS, finish, 0)
    with scope("sends"):
        for it in range(ITERS):
            for k in range(1, TM):
                forward_copy(it, k).wait_send()
                back_copy(it, k).wait_send()
            for step in range(1, 5):
                for t in range(2):
                    for way, part in ring_chunks(step, t):
                        ring_copy(it, step, way, t, part).wait_send()
            for way in range(2):
                pack_copy(it, way).wait_send()
        for kind in range(3):
            for hop in range(3):
                for t in range(2):
                    column_copy(kind, hop, t).wait_send()


def per_device(conserved_field, face_neighbours, counterpart_group, counterpart_shift, volume_operator, flux_matrix):
    state = jax.ShapeDtypeStruct(conserved_field.shape, jnp.float32)
    vmem = pl.BlockSpec(memory_space=pltpu.VMEM)
    smem = pl.BlockSpec(memory_space=pltpu.SMEM)
    f32, bf16 = jnp.float32, jnp.bfloat16
    dma = pltpu.SemaphoreType.DMA
    return pl.pallas_call(
        kernel,
        out_shape=(state, state),
        in_specs=[pl.BlockSpec(memory_space=pl.ANY), vmem, smem, smem, vmem, smem],
        out_specs=(vmem, vmem),
        scratch_shapes=[
            pltpu.VMEM((ITERS, 2, VARS, NODES, LANES), f32),
            pltpu.VMEM((VARS * NODES, VARS * NODES), bf16),
            pltpu.VMEM((VARS * NODES, VARS * NODES), bf16),
            pltpu.VMEM((ITERS, TM, 2, VARS, 8, LANES), f32),
            pltpu.VMEM((ITERS, SAMPLE_COUNT, VARS, 8, LANES), f32),
            pltpu.VMEM((ITERS, 2, VARS, NODES, LANES), f32),
            *[pltpu.VMEM((Z, VARS, 16, LANES), f32)] * 4,
            *[pltpu.VMEM((Q, VARS, 16, LANES), f32)] * 6,
            pltpu.VMEM((ITERS, 2, 16, LANES), f32),
            pltpu.VMEM((ITERS, 2, 16, LANES), f32),
            pltpu.VMEM((3, NODES, LANES), f32),
            pltpu.VMEM((2, VARS, 16, LANES), f32),
            pltpu.VMEM((2, VARS, 16, LANES), f32),
            pltpu.VMEM((2, VARS, 16, LANES), f32),
            pltpu.VMEM((2, VARS, 16, LANES), f32),
            dma,
            dma((ITERS, TM)), dma((ITERS, TM)),
            dma((ITERS, TM)), dma((ITERS, TM)),
            dma((ITERS, 16 * PARTS)), dma((ITERS, 16 * PARTS)),
            dma((3, 6)), dma((3, 6)),
            dma((ITERS, 2)), dma((ITERS, 2)),
        ],
        compiler_params=pltpu.CompilerParams(
            collective_id=0, has_side_effects=True, vmem_limit_bytes=48 * 1024 * 1024),
        name="iterations",
    )(conserved_field, face_neighbours, counterpart_group, counterpart_shift, volume_operator,
      jnp.transpose(flux_matrix, (1, 0, 2)))


def solution(mesh):
    return jax.shard_map(
        per_device,
        mesh=mesh,
        in_specs=(P("tm", None, None, "space"), P(None, "space"), P("tm"), P("tm"), P(), P()),
        out_specs=(P("tm", None, None, "space"), P("tm", None, None, "space")),
        check_vma=False,
    )
```

```python
import math

import jax
import jax.numpy as jnp
from jax import lax
from jax.experimental import pallas as pl
from jax.experimental.pallas import tpu as pltpu
from jax.sharding import PartitionSpec as P

SAMPLE_COUNT = 16
REACH = 4
ITERS = 2
VARS = 10
NODES = 64
LANES = 128
PARTS = 5
PIECE = VARS // PARTS

lift_scale = 2.0
dissipation = 1.5
angular_speed = 0.5
damping_factor = 4.0
pseudo_step = 0.2

MESH = pl.DeviceIdType.MESH
MOVES = ((2, 1), (1, 1), (3, 1), (0, 1), (2, 0), (1, 0), (3, 0))
TM = 8
SP = 32
Z = 8
Q = 4


def spectral_weights():
    half = SAMPLE_COUNT // 2
    weights = []
    for m in range(1, half):
        total = 0.0
        for k in range(1, half):
            gain = 2.0 * angular_speed * k * math.exp(-damping_factor * (k / half) ** 8) / SAMPLE_COUNT
            total += gain * math.sin(2.0 * math.pi * k * m / SAMPLE_COUNT)
        weights.append(total)
    return weights


def pick(index, values):
    out = jnp.float32(values[0])
    for k in range(1, len(values)):
        out = jnp.where(index == k, jnp.float32(values[k]), out)
    return out


def kernel(
    u_ref, fn_ref, group_ref, shift_ref, vol_ref, flux_ref,
    new_ref, res_ref,
    ub, a_hi, a_lo, gat, der, der2, tem, tem2, sig, sig_gat, sig_der, sig_tem, ring_00, ring_01, ring_10, ring_11, cols_00, cols_01, cols_10, cols_11, cols_20, cols_21,
    packs, packed, side, lo_b, up_b, sl_b, tw_b, in_sem, fs, fr, bs, br, zs, zr, cs, cr, ps, pr,
):
    ring = ((ring_00, ring_01), (ring_10, ring_11))
    cols = ((cols_00, cols_01), (cols_10, cols_11), (cols_20, cols_21))
    tm = lax.axis_index("tm")
    sp = lax.axis_index("space")
    z = sp // Q
    q = sp % Q

    def space_of(zz, qq):
        return zz * Q + qq

    z_up = space_of((z + 1) % Z, q)
    z_dn = space_of((z + Z - 1) % Z, q)
    mate = space_of(z, q + 1 - 2 * (q % 2))
    cross = space_of(z, (q + 2) % Q)
    after = (sp + 1) % SP
    before = (sp + SP - 1) % SP

    load = pltpu.make_async_copy(u_ref, ub.at[0], in_sem)
    load.start()

    barrier = pltpu.get_barrier_semaphore()
    for k in range(1, TM):
        pl.semaphore_signal(barrier, inc=1, device_id={"tm": (tm + k) % TM}, device_id_type=MESH)
    for other in (z_up, z_dn, mate, cross, after, before):
        pl.semaphore_signal(barrier, inc=1, device_id={"space": other}, device_id_type=MESH)
    with jax.named_scope("entry"):
        load.wait()
        pl.semaphore_wait(barrier, TM - 1 + 6)

    lane16 = lax.broadcasted_iota(jnp.int32, (16, LANES), 1)
    gidx = sp * LANES + lane16
    back_gap = jnp.bitwise_and(gidx - fn_ref[0:1, :], SP * LANES - 1)
    ahead_gap = jnp.bitwise_and(fn_ref[1:2, :] - gidx, SP * LANES - 1)

    weights = spectral_weights()
    cosines = [math.cos(2.0 * math.pi * k / SAMPLE_COUNT) for k in range(SAMPLE_COUNT)]
    sines = [math.sin(2.0 * math.pi * k / SAMPLE_COUNT) for k in range(SAMPLE_COUNT)]

    def rows_of(index):
        return pl.ds(pl.multiple_of(index * 8, 8), 8)

    def peer_at(k, sign):
        dy, dx = MOVES[k]
        return ((tm // 2 + sign * dy + 4) % 4) * 2 + (tm % 2 + dx) % 2

    def three(index):
        return pl.ds(3 * index, 3)

    def forward_copy(kind, k):
        peer = peer_at(k, 1)
        source = ub.at[0, :, :, rows_of(peer), :] if kind == 0 else sig.at[:, three(peer)]
        target = gat.at[tm] if kind == 0 else sig_gat.at[tm]
        return pltpu.make_async_remote_copy(
            src_ref=source, dst_ref=target, send_sem=fs.at[kind, k], recv_sem=fr.at[kind, k],
            device_id={"tm": peer}, device_id_type=MESH)

    def forward_arrival(kind, k):
        peer = peer_at(k, -1)
        source = ub.at[0, :, :, rows_of(peer), :] if kind == 0 else sig.at[:, three(peer)]
        target = gat.at[peer] if kind == 0 else sig_gat.at[peer]
        return pltpu.make_async_remote_copy(
            src_ref=source, dst_ref=target, send_sem=fs.at[kind, k], recv_sem=fr.at[kind, k],
            device_id={"tm": peer}, device_id_type=MESH)

    def back_refs(kind, peer, place):
        source = (der, sig_der, der2)[kind].at[pl.ds(2 * peer, 2)]
        if kind == 1:
            return source, sig_tem.at[:, three(place)]
        return source, (tem, None, tem2)[kind].at[:, :, rows_of(place), :]

    def back_copy(kind, k):
        peer = peer_at(k, 1)
        source, target = back_refs(kind, peer, tm)
        return pltpu.make_async_remote_copy(
            src_ref=source, dst_ref=target, send_sem=bs.at[kind, k], recv_sem=br.at[kind, k],
            device_id={"tm": peer}, device_id_type=MESH)

    def back_arrival(kind, k):
        peer = peer_at(k, -1)
        source, target = back_refs(kind, peer, peer)
        return pltpu.make_async_remote_copy(
            src_ref=source, dst_ref=target, send_sem=bs.at[kind, k], recv_sem=br.at[kind, k],
            device_id={"tm": peer}, device_id_type=MESH)

    def ring_slot(step, way, t, part):
        return (((step - 1) * 2 + way) * 2 + t) * PARTS + part

    def ring_copy(it, step, way, t, part):
        if way == 0:
            origin, target = (z + Z - (step - 1)) % Z, z_up
        else:
            origin, target = (z + step - 1) % Z, z_dn
        block = ring[it][t].at[origin, pl.ds(part * PIECE, PIECE)]
        slot = ring_slot(step, way, t, part)
        return pltpu.make_async_remote_copy(
            src_ref=block, dst_ref=block, send_sem=zs.at[it, slot], recv_sem=zr.at[it, slot],
            device_id={"space": target}, device_id_type=MESH)

    def ring_arrival(it, step, way, t, part):
        if way == 0:
            origin, target = (z + Z - step) % Z, z_up
        else:
            origin, target = (z + step) % Z, z_dn
        block = ring[it][t].at[origin, pl.ds(part * PIECE, PIECE)]
        slot = ring_slot(step, way, t, part)
        return pltpu.make_async_remote_copy(
            src_ref=block, dst_ref=block, send_sem=zs.at[it, slot], recv_sem=zr.at[it, slot],
            device_id={"space": target}, device_id_type=MESH)

    def column_copy(kind, hop, t):
        origin, target = ((q, mate), (q, cross), ((q + 2) % Q, mate))[hop]
        block = cols[kind][t].at[origin]
        slot = hop * 2 + t
        return pltpu.make_async_remote_copy(
            src_ref=block, dst_ref=block, send_sem=cs.at[kind, slot], recv_sem=cr.at[kind, slot],
            device_id={"space": target}, device_id_type=MESH)

    def column_arrival(kind, hop, t):
        mate_q = q + 1 - 2 * (q % 2)
        origin, target = ((mate_q, mate), ((q + 2) % Q, cross), ((mate_q + 2) % Q, mate))[hop]
        block = cols[kind][t].at[origin]
        slot = hop * 2 + t
        return pltpu.make_async_remote_copy(
            src_ref=block, dst_ref=block, send_sem=cs.at[kind, slot], recv_sem=cr.at[kind, slot],
            device_id={"space": target}, device_id_type=MESH)

    def pack_copy(it, way):
        target = (after, before)[way]
        return pltpu.make_async_remote_copy(
            src_ref=packs.at[it, way], dst_ref=packed.at[it, way], send_sem=ps.at[it, way], recv_sem=pr.at[it, way],
            device_id={"space": target}, device_id_type=MESH)

    def build_matrix():
        row = lax.broadcasted_iota(jnp.int32, (NODES, LANES), 0)
        lane = lax.broadcasted_iota(jnp.int32, (NODES, LANES), 1)
        first = lane < NODES
        on = row == jnp.bitwise_and(lane, NODES - 1)
        one, zero = jnp.float32(1.0), jnp.float32(0.0)
        lower = jnp.where(on & (row < 16), one, zero)
        upper = jnp.where(on & (row >= 48), one, zero)
        slide = jnp.where(on & (jnp.bitwise_and(row, 3) == 3), one, zero)
        scale = jnp.float32(0.5 * lift_scale)
        side[0] = jnp.concatenate([vol_ref[0], vol_ref[0]], axis=1) + scale * (lower - upper)
        side[1] = jnp.concatenate([vol_ref[1], vol_ref[1]], axis=1) - scale * slide
        side[2] = (scale * jnp.float32(dissipation)) * (lower + upper + slide)

        def row_block(v, carry):
            for j in range(VARS // 2):
                tile = jnp.zeros((NODES, LANES), jnp.float32)
                for d in range(2):
                    factor = jnp.where(first, flux_ref[v, d, 2 * j], flux_ref[v, d, 2 * j + 1])
                    tile = tile + factor * side[d]
                own = jnp.where(first, jnp.where(v == 2 * j, one, zero), jnp.where(v == 2 * j + 1, one, zero))
                tile = tile + own * side[2]
                high = tile.astype(jnp.bfloat16)
                where = (pl.ds(pl.multiple_of(v * NODES, NODES), NODES), pl.ds(j * LANES, LANES))
                a_hi[where] = high
                a_lo[where] = (tile - high.astype(jnp.float32)).astype(jnp.bfloat16)
            return carry

        lax.fori_loop(0, VARS, row_block, 0)

    def volume_part(it):
        u = jnp.concatenate(
            [ub[it, 0].reshape(VARS * NODES, LANES), ub[it, 1].reshape(VARS * NODES, LANES)], axis=1)
        high = u.astype(jnp.bfloat16)
        low = (u - high.astype(jnp.float32)).astype(jnp.bfloat16)
        for part in range(2):
            rows = pl.ds(part * 320, 320)
            out = jnp.dot(a_hi[rows, :], high, preferred_element_type=jnp.float32)
            out = out + jnp.dot(a_hi[rows, :], low, preferred_element_type=jnp.float32)
            out = out + jnp.dot(a_lo[rows, :], high, preferred_element_type=jnp.float32)
            for t in range(2):
                res_ref[t, pl.ds(part * 5, 5)] = out[:, t * LANES:(t + 1) * LANES].reshape(5, NODES, LANES)

    def ring_chunks(step, t):
        ways = (0, 1) if step < 4 else (t,)
        return [(way, part) for part in range(PARTS) for way in ways]

    def ring_start(it, t):
        for way, part in ring_chunks(1, t):
            ring_copy(it, 1, way, t, part).start()

    def ring_relay(it, step, t):
        onward = ring_chunks(step + 1, t) if step < 4 else []
        for way, part in ring_chunks(step, t):
            ring_arrival(it, step, way, t, part).wait_recv()
            if (way, part) in onward:
                ring_copy(it, step + 1, way, t, part).start()

    def pack_traces(it):
        up_pack = jnp.zeros((16, LANES), jnp.float32)
        lo_pack = jnp.zeros((16, LANES), jnp.float32)
        for i in range(2 * VARS):
            mine = (lane16 >= REACH * i) & (lane16 < REACH * (i + 1))
            u_face = ub[it, i // VARS, i % VARS, pl.ds(48, 16), :]
            l_face = ub[it, i // VARS, i % VARS, pl.ds(0, 16), :]
            up_pack = jnp.where(mine, pltpu.roll(u_face, (REACH * i + REACH) % LANES, 1), up_pack)
            lo_pack = jnp.where(mine, pltpu.roll(l_face, REACH * i, 1) if i else l_face, lo_pack)
        packs[it // 2, 0] = up_pack
        packs[it // 2, 1] = lo_pack
        for way in range(2):
            pack_copy(it // 2, way).start()

    scale = jnp.float32(0.5 * lift_scale)
    loss = jnp.float32(0.5 * lift_scale * dissipation)

    def first_direction(it):
        for way in range(2):
            pack_copy(it // 2, way).wait_recv()
        from_before = packed[it // 2, 0]
        from_after = packed[it // 2, 1]
        behind = lane16 - back_gap
        ahead = lane16 + ahead_gap
        for i in range(2 * VARS):
            u_face = ub[it, i // VARS, i % VARS, pl.ds(48, 16), :]
            l_face = ub[it, i // VARS, i % VARS, pl.ds(0, 16), :]
            own = jnp.take_along_axis(u_face, jnp.bitwise_and(behind, LANES - 1), axis=1)
            far = jnp.take_along_axis(from_before, jnp.bitwise_and(behind + REACH * (i + 1), LANES - 1), axis=1)
            lo_b[i // VARS, i % VARS] = jnp.where(behind < 0, far, own)
            own = jnp.take_along_axis(l_face, jnp.bitwise_and(ahead, LANES - 1), axis=1)
            far = jnp.take_along_axis(from_after, jnp.bitwise_and(ahead + REACH * i, LANES - 1), axis=1)
            up_b[i // VARS, i % VARS] = jnp.where(ahead >= LANES, far, own)

        def first_faces(v, c):
            low = -loss * lo_b[:, v]
            upp = -loss * up_b[:, v]
            for w in range(VARS):
                f = scale * flux_ref[v, 0, w]
                low = low - f * lo_b[:, w]
                upp = upp + f * up_b[:, w]
            res_ref[:, v, pl.ds(0, 16), :] += low
            res_ref[:, v, pl.ds(48, 16), :] += upp
            return c

        lax.fori_loop(0, VARS, first_faces, 0)

    def spectral(load_at, store_at):
        x = [load_at(t) for t in range(SAMPLE_COUNT)]
        half = SAMPLE_COUNT // 2
        for t in range(half):
            near = opposite = None
            for m in range(1, half):
                diff = x[(t + m) % SAMPLE_COUNT] - x[(t - m) % SAMPLE_COUNT]
                one, two = jnp.float32(weights[m - 1]) * diff, jnp.float32(-weights[half - m - 1]) * diff
                near = one if near is None else near + one
                opposite = two if opposite is None else opposite + two
            store_at(t, near)
            store_at(t + half, opposite)

    def first_derivative(v, c):
        spectral(lambda t: gat[t // 2, t % 2, v], lambda t, value: der.__setitem__((t, v), value))
        return c

    def second_derivative(v, c):
        spectral(lambda t: der[t, v], lambda t, value: der2.__setitem__((t, v), value))
        return c

    def sliding_derivative(i, c):
        spectral(lambda t: sig_gat[t // 2, t % 2, i], lambda t, value: sig_der.__setitem__((t, i), value))
        return c

    def exchange_all(make, kind, method):
        for k in range(len(MOVES)):
            getattr(make(kind, k), method)()

    def offset_of(kind, t):
        group, shift = group_ref[t], shift_ref[t]
        if kind == 1:
            group = jnp.bitwise_and(2 * group + lax.shift_right_arithmetic(shift, 6), SP - 1)
            shift = jnp.bitwise_and(2 * shift, LANES - 1)
        return group, shift

    lane_b = lax.broadcasted_iota(jnp.int32, (VARS, 16, LANES), 2)

    def column_start(kind, t):
        it = kind // 2
        group, shift = offset_of(kind, t)
        first_dst = jnp.bitwise_and(q - group, Q - 1)
        second_dst = jnp.bitwise_and(q - group - 1, Q - 1)
        first = jnp.bitwise_and(z + lax.shift_right_arithmetic(first_dst + group - q, 2), Z - 1)
        second = jnp.bitwise_and(z + lax.shift_right_arithmetic(second_dst + group + 1 - q, 2), Z - 1)
        cols[kind][t][q] = jnp.where(lane_b >= shift, ring[it][t][first], ring[it][t][second])
        column_copy(kind, 1, t).start()
        column_copy(kind, 0, t).start()

    def column_relay(kind, t):
        column_arrival(kind, 1, t).wait_recv()
        column_copy(kind, 2, t).start()

    def column_finish(kind, t):
        column_arrival(kind, 0, t).wait_recv()
        column_arrival(kind, 2, t).wait_recv()
        group, shift = offset_of(kind, t)
        first = cols[kind][t][jnp.bitwise_and(q + group, Q - 1)]
        second = cols[kind][t][jnp.bitwise_and(q + group + 1, Q - 1)]
        both = jnp.where(lane_b >= shift, first, second)
        both = pltpu.roll(both.reshape(VARS * 16, LANES), jnp.bitwise_and(LANES - shift, LANES - 1), 1)
        return both.reshape(VARS, 16, LANES)

    def turn(t):
        cosine, sine = pick(2 * tm + t, cosines), pick(2 * tm + t, sines)
        one, two = sl_b[t, 1], sl_b[t, 2]
        sl_b[t, 1] = cosine * one - sine * two
        sl_b[t, 2] = sine * one + cosine * two

    def slide_term(t, v):
        term = -loss * sl_b[t, v]
        for w in range(VARS):
            term = term + (scale * flux_ref[v, 1, w]) * sl_b[t, w]
        return term

    step_size = jnp.float32(pseudo_step)
    scope = jax.named_scope

    with scope("start0"):
        for t in range(2):
            ring[0][t][z] = ub[0, t, :, pl.ds(3, 16, stride=4), :]
            ring_start(0, t)
        pack_traces(0)
        exchange_all(forward_copy, 0, "start")
        gat[tm] = ub[0, :, :, rows_of(tm), :]
        sig[:, pl.ds(2 * VARS, 4)] = jnp.zeros((2, 4, 8, LANES), jnp.float32)
    with scope("matrix"):
        build_matrix()
    with scope("volume0"):
        volume_part(0)
    with scope("ring0_1"):
        ring_relay(0, 1, 0)
        ring_relay(0, 1, 1)
    with scope("ring0_2a"):
        ring_relay(0, 2, 0)
    with scope("fwd0"):
        exchange_all(forward_arrival, 0, "wait_recv")
    with scope("derive0"):
        lax.fori_loop(0, VARS, first_derivative, 0)
        exchange_all(back_copy, 0, "start")
        tem[:, :, rows_of(tm), :] = der[pl.ds(2 * tm, 2)]
    with scope("ring0_2b"):
        ring_relay(0, 2, 1)
    with scope("first0"):
        first_direction(0)
    with scope("ring0_3"):
        ring_relay(0, 3, 0)
    with scope("derive2"):
        lax.fori_loop(0, VARS, second_derivative, 0)
        tem2[:, :, rows_of(tm), :] = der2[pl.ds(2 * tm, 2)]
    with scope("ring0_3b"):
        ring_relay(0, 3, 1)
    with scope("ring0_4"):
        for t in range(2):
            ring_relay(0, 4, t)
            column_start(0, t)
    with scope("back0"):
        exchange_all(back_arrival, 0, "wait_recv")

    def partial_state(v, c):
        for t in range(2):
            ub[1, t, v] = ub[0, t, v] - step_size * (res_ref[t, v] + tem[t, v])
        return c

    with scope("w"):
        lax.fori_loop(0, VARS, partial_state, 0)
        for t in range(2):
            ring[1][t][z] = ub[1, t, :, pl.ds(3, 16, stride=4), :]
            ring_start(1, t)
    with scope("cols1_start"):
        for t in range(2):
            column_start(1, t)
        exchange_all(back_copy, 2, "start")
    with scope("ring1_1a"):
        ring_relay(1, 1, 0)
    with scope("cols0_relay"):
        for t in range(2):
            column_relay(0, t)
    with scope("ring1_1b"):
        ring_relay(1, 1, 1)
    with scope("cols0_finish"):
        for t in range(2):
            sl_b[t] = column_finish(0, t)
            turn(t)

    def next_state(v, c):
        for t in range(2):
            term = slide_term(t, v)
            sig[t, 2 * v] = term[0:8]
            sig[t, 2 * v + 1] = term[8:16]
            ub[1, t, v, pl.ds(3, 16, stride=4), :] += -step_size * term
            ub[2, t, v] = ub[1, t, v] - step_size * tem[t, v]
        return c

    with scope("u1"):
        lax.fori_loop(0, VARS, next_state, 0)
        exchange_all(forward_copy, 1, "start")
        pack_traces(2)
        sig_gat[tm] = sig[:, three(tm)]
    with scope("volume1"):
        volume_part(2)
    with scope("ring1_2"):
        ring_relay(1, 2, 0)
    with scope("cols1_relay"):
        for t in range(2):
            column_relay(1, t)
    with scope("ring1_2b"):
        ring_relay(1, 2, 1)
    with scope("first1"):
        first_direction(2)
    with scope("cols1_finish"):
        for t in range(2):
            sl_b[t] = column_finish(1, t)
            turn(t)

        def twice(v, c):
            for t in range(2):
                tw_b[t, v] = step_size * slide_term(t, v)
            return c

        lax.fori_loop(0, VARS, twice, 0)
    with scope("ring1_3"):
        ring_relay(1, 3, 0)
        ring_relay(1, 3, 1)
    with scope("fwd1"):
        exchange_all(forward_arrival, 1, "wait_recv")
    with scope("derive1"):
        lax.fori_loop(0, 3, sliding_derivative, 0)
        exchange_all(back_copy, 1, "start")
        sig_tem[:, three(tm)] = sig_der[pl.ds(2 * tm, 2)]
    with scope("ring1_4"):
        for t in range(2):
            ring_relay(1, 4, t)
            column_start(2, t)
    with scope("back2"):
        exchange_all(back_arrival, 2, "wait_recv")

    def without_slide(v, c):
        for t in range(2):
            res_ref[t, v] += tem[t, v] - step_size * tem2[t, v]
        return c

    with scope("without_slide"):
        lax.fori_loop(0, VARS, without_slide, 0)
    with scope("cols2_relay"):
        for t in range(2):
            column_relay(2, t)
    with scope("back1"):
        exchange_all(back_arrival, 1, "wait_recv")
    with scope("cols2_finish"):
        for t in range(2):
            sl_b[t] = column_finish(2, t) - tw_b[t]
            turn(t)

    def finish(v, c):
        for t in range(2):
            late = jnp.concatenate([sig_tem[t, 2 * v], sig_tem[t, 2 * v + 1]], axis=0)
            res_ref[t, v, pl.ds(3, 16, stride=4), :] += slide_term(t, v) - step_size * late
            new_ref[t, v] = ub[1, t, v] - step_size * res_ref[t, v]
        return c

    with scope("finish"):
        lax.fori_loop(0, VARS, finish, 0)
    with scope("sends"):
        for kind in range(3):
            if kind < 2:
                exchange_all(forward_copy, kind, "wait_send")
            exchange_all(back_copy, kind, "wait_send")
            for hop in range(3):
                for t in range(2):
                    column_copy(kind, hop, t).wait_send()
        for it in range(ITERS):
            for step in range(1, 5):
                for t in range(2):
                    for way, part in ring_chunks(step, t):
                        ring_copy(it, step, way, t, part).wait_send()
            for way in range(2):
                pack_copy(it, way).wait_send()


def per_device(conserved_field, face_neighbours, counterpart_group, counterpart_shift, volume_operator, flux_matrix):
    state = jax.ShapeDtypeStruct(conserved_field.shape, jnp.float32)
    vmem = pl.BlockSpec(memory_space=pltpu.VMEM)
    smem = pl.BlockSpec(memory_space=pltpu.SMEM)
    f32, bf16 = jnp.float32, jnp.bfloat16
    dma = pltpu.SemaphoreType.DMA
    return pl.pallas_call(
        kernel,
        out_shape=(state, state),
        in_specs=[pl.BlockSpec(memory_space=pl.ANY), vmem, smem, smem, vmem, smem],
        out_specs=(vmem, vmem),
        scratch_shapes=[
            pltpu.VMEM((3, 2, VARS, NODES, LANES), f32),
            pltpu.VMEM((VARS * NODES, VARS * NODES), bf16),
            pltpu.VMEM((VARS * NODES, VARS * NODES), bf16),
            pltpu.VMEM((TM, 2, VARS, 8, LANES), f32),
            pltpu.VMEM((SAMPLE_COUNT, VARS, 8, LANES), f32),
            pltpu.VMEM((SAMPLE_COUNT, VARS, 8, LANES), f32),
            pltpu.VMEM((2, VARS, NODES, LANES), f32),
            pltpu.VMEM((2, VARS, NODES, LANES), f32),
            pltpu.VMEM((2, 3 * TM, 8, LANES), f32),
            pltpu.VMEM((TM, 2, 3, 8, LANES), f32),
            pltpu.VMEM((SAMPLE_COUNT, 3, 8, LANES), f32),
            pltpu.VMEM((2, 3 * TM, 8, LANES), f32),
            *[pltpu.VMEM((Z, VARS, 16, LANES), f32)] * 4,
            *[pltpu.VMEM((Q, VARS, 16, LANES), f32)] * 6,
            pltpu.VMEM((ITERS, 2, 16, LANES), f32),
            pltpu.VMEM((ITERS, 2, 16, LANES), f32),
            pltpu.VMEM((3, NODES, LANES), f32),
            pltpu.VMEM((2, VARS, 16, LANES), f32),
            pltpu.VMEM((2, VARS, 16, LANES), f32),
            pltpu.VMEM((2, VARS, 16, LANES), f32),
            pltpu.VMEM((2, VARS, 16, LANES), f32),
            dma,
            dma((2, 7)), dma((2, 7)),
            dma((3, 7)), dma((3, 7)),
            dma((ITERS, 16 * PARTS)), dma((ITERS, 16 * PARTS)),
            dma((3, 6)), dma((3, 6)),
            dma((ITERS, 2)), dma((ITERS, 2)),
        ],
        compiler_params=pltpu.CompilerParams(
            collective_id=0, has_side_effects=True, vmem_limit_bytes=48 * 1024 * 1024),
        name="iterations",
    )(conserved_field, face_neighbours, counterpart_group, counterpart_shift, volume_operator,
      jnp.transpose(flux_matrix, (1, 0, 2)))


def solution(mesh):
    return jax.shard_map(
        per_device,
        mesh=mesh,
        in_specs=(P("tm", None, None, "space"), P(None, "space"), P("tm"), P("tm"), P(), P()),
        out_specs=(P("tm", None, None, "space"), P("tm", None, None, "space")),
        check_vma=False,
    )
```

```python
import math

import jax
import jax.numpy as jnp
from jax import lax
from jax.experimental import pallas as pl
from jax.experimental.pallas import tpu as pltpu
from jax.sharding import PartitionSpec as P

SAMPLE_COUNT = 16
REACH = 4
ITERS = 2
VARS = 10
NODES = 64
LANES = 128
PARTS = 5
PIECE = VARS // PARTS

lift_scale = 2.0
dissipation = 1.5
angular_speed = 0.5
damping_factor = 4.0
pseudo_step = 0.2

MESH = pl.DeviceIdType.MESH
MOVES = ((2, 1), (1, 1), (3, 1), (0, 1), (2, 0), (1, 0), (3, 0))
TM = 8
SP = 32
Z = 8
Q = 4


def spectral_weights():
    half = SAMPLE_COUNT // 2
    weights = []
    for m in range(1, half):
        total = 0.0
        for k in range(1, half):
            gain = 2.0 * angular_speed * k * math.exp(-damping_factor * (k / half) ** 8) / SAMPLE_COUNT
            total += gain * math.sin(2.0 * math.pi * k * m / SAMPLE_COUNT)
        weights.append(total)
    return weights


def spectral_squares():
    first = [0.0] + spectral_weights() + [0.0]
    full = first + [-first[SAMPLE_COUNT - m] for m in range(SAMPLE_COUNT // 2 + 1, SAMPLE_COUNT)]
    return [
        sum(full[j] * full[(m - j) % SAMPLE_COUNT] for j in range(SAMPLE_COUNT))
        for m in range(SAMPLE_COUNT // 2 + 1)
    ]


def slide_place(v, h):
    index = 2 * v + h
    return index // 5, index % 5


def other_place(v, c, h):
    index = 6 * v + 2 * c + h
    return index // 15, 5 + index % 15


def pick(index, values):
    out = jnp.float32(values[0])
    for k in range(1, len(values)):
        out = jnp.where(index == k, jnp.float32(values[k]), out)
    return out


def kernel(
    u_hbm, fn_hbm, group_hbm, shift_hbm, vol_hbm, flux_hbm,
    new_ref, res_ref, fn_ref, group_ref, shift_ref, vol_ref, flux_ref,
    ub, a_hi, a_lo, up, gat, dt, dt2, tem, tem2, sig, sig_gat, sig_dt, sig_tem, ring_00, ring_01, ring_10, ring_11, cols_00, cols_01, cols_10, cols_11, cols_20, cols_21,
    packs, packed, side, lo_b, up_b, sl_b, tw_b, in_sem, fs, fr, bs, br, zs, zr, cs, cr, ps, pr,
):
    ring = ((ring_00, ring_01), (ring_10, ring_11))
    cols = ((cols_00, cols_01), (cols_10, cols_11), (cols_20, cols_21))
    tm = lax.axis_index("tm")
    sp = lax.axis_index("space")
    z = sp // Q
    q = sp % Q
    y = tm // 2
    side_x = tm % 2

    def space_of(zz, qq):
        return zz * Q + qq

    z_up = space_of((z + 1) % Z, q)
    z_dn = space_of((z + Z - 1) % Z, q)
    mate = space_of(z, q + 1 - 2 * (q % 2))
    cross = space_of(z, (q + 2) % Q)
    after = (sp + 1) % SP
    before = (sp + SP - 1) % SP

    loads = [
        pltpu.make_async_copy(source, target, in_sem.at[k])
        for k, (source, target) in enumerate((
            (u_hbm, ub.at[0]), (flux_hbm, flux_ref), (vol_hbm, vol_ref),
            (fn_hbm, fn_ref), (group_hbm, group_ref), (shift_hbm, shift_ref)))
    ]
    for load in loads:
        load.start()

    barrier = pltpu.get_barrier_semaphore()
    for k in range(1, TM):
        pl.semaphore_signal(barrier, inc=1, device_id={"tm": (tm + k) % TM}, device_id_type=MESH)
    for other in (z_up, z_dn, mate, cross, after, before):
        pl.semaphore_signal(barrier, inc=1, device_id={"space": other}, device_id_type=MESH)
    with jax.named_scope("entry"):
        for load in loads:
            load.wait()
        pl.semaphore_wait(barrier, TM - 1 + 6)

    lane16 = lax.broadcasted_iota(jnp.int32, (16, LANES), 1)
    gidx = sp * LANES + lane16
    back_gap = jnp.bitwise_and(gidx - fn_ref[0:1, :], SP * LANES - 1)
    ahead_gap = jnp.bitwise_and(fn_ref[1:2, :] - gidx, SP * LANES - 1)

    weights = spectral_weights()
    squares = spectral_squares()
    cosines = [math.cos(2.0 * math.pi * k / SAMPLE_COUNT) for k in range(SAMPLE_COUNT)]
    sines = [math.sin(2.0 * math.pi * k / SAMPLE_COUNT) for k in range(SAMPLE_COUNT)]

    OUT = ((0, 5), (5, 5), (10, 10))
    BACK = ((0, 5), (5, 15), (0, 20))

    def peer_at(k, sign):
        dy, dx = MOVES[k]
        row = (y + sign * dy + 4) % 4
        return row, row * 2 + (side_x + dx) % 2

    def out_refs(kind, row, place):
        if kind == 3:
            return sig.at[:, pl.ds(5 * row, 5)], sig_gat.at[place]
        tiles = pl.ds(*OUT[kind])
        return up.at[:, row, tiles], gat.at[place, :, tiles]

    def back_refs(kind, row, place):
        if kind == 3:
            return sig_dt.at[row], sig_tem.at[:, pl.ds(5 * place, 5)]
        tiles = pl.ds(*BACK[kind])
        source, target = ((dt, tem), (dt, tem), (dt2, tem2))[kind]
        return source.at[row, :, tiles], target.at[:, place, tiles]

    def out_copy(kind, k):
        row, peer = peer_at(k, 1)
        source, target = out_refs(kind, row, tm)
        return pltpu.make_async_remote_copy(
            src_ref=source, dst_ref=target, send_sem=fs.at[kind, k], recv_sem=fr.at[kind, k],
            device_id={"tm": peer}, device_id_type=MESH)

    def out_arrival(kind, k):
        row, peer = peer_at(k, -1)
        source, target = out_refs(kind, row, peer)
        return pltpu.make_async_remote_copy(
            src_ref=source, dst_ref=target, send_sem=fs.at[kind, k], recv_sem=fr.at[kind, k],
            device_id={"tm": peer}, device_id_type=MESH)

    def back_copy(kind, k):
        row, peer = peer_at(k, 1)
        source, target = back_refs(kind, row, y)
        return pltpu.make_async_remote_copy(
            src_ref=source, dst_ref=target, send_sem=bs.at[kind, k - 4], recv_sem=br.at[kind, k - 4],
            device_id={"tm": peer}, device_id_type=MESH)

    def back_arrival(kind, k):
        row, peer = peer_at(k, -1)
        source, target = back_refs(kind, row, row)
        return pltpu.make_async_remote_copy(
            src_ref=source, dst_ref=target, send_sem=bs.at[kind, k - 4], recv_sem=br.at[kind, k - 4],
            device_id={"tm": peer}, device_id_type=MESH)

    def out_all(make, kind, method):
        for k in range(7):
            getattr(make(kind, k), method)()

    def back_all(make, kind, method):
        for k in range(4, 7):
            getattr(make(kind, k), method)()

    def ring_slot(step, way, t, part):
        return (((step - 1) * 2 + way) * 2 + t) * PARTS + part

    def ring_copy(it, step, way, t, part):
        if way == 0:
            origin, target = (z + Z - (step - 1)) % Z, z_up
        else:
            origin, target = (z + step - 1) % Z, z_dn
        block = ring[it][t].at[origin, pl.ds(part * PIECE, PIECE)]
        slot = ring_slot(step, way, t, part)
        return pltpu.make_async_remote_copy(
            src_ref=block, dst_ref=block, send_sem=zs.at[it, slot], recv_sem=zr.at[it, slot],
            device_id={"space": target}, device_id_type=MESH)

    def ring_arrival(it, step, way, t, part):
        if way == 0:
            origin, target = (z + Z - step) % Z, z_up
        else:
            origin, target = (z + step) % Z, z_dn
        block = ring[it][t].at[origin, pl.ds(part * PIECE, PIECE)]
        slot = ring_slot(step, way, t, part)
        return pltpu.make_async_remote_copy(
            src_ref=block, dst_ref=block, send_sem=zs.at[it, slot], recv_sem=zr.at[it, slot],
            device_id={"space": target}, device_id_type=MESH)

    def column_copy(kind, hop, t):
        origin, target = ((q, mate), (q, cross), ((q + 2) % Q, mate))[hop]
        block = cols[kind][t].at[origin]
        slot = hop * 2 + t
        return pltpu.make_async_remote_copy(
            src_ref=block, dst_ref=block, send_sem=cs.at[kind, slot], recv_sem=cr.at[kind, slot],
            device_id={"space": target}, device_id_type=MESH)

    def column_arrival(kind, hop, t):
        mate_q = q + 1 - 2 * (q % 2)
        origin, target = ((mate_q, mate), ((q + 2) % Q, cross), ((mate_q + 2) % Q, mate))[hop]
        block = cols[kind][t].at[origin]
        slot = hop * 2 + t
        return pltpu.make_async_remote_copy(
            src_ref=block, dst_ref=block, send_sem=cs.at[kind, slot], recv_sem=cr.at[kind, slot],
            device_id={"space": target}, device_id_type=MESH)

    def pack_copy(it, way):
        target = (after, before)[way]
        return pltpu.make_async_remote_copy(
            src_ref=packs.at[it, way], dst_ref=packed.at[it, way], send_sem=ps.at[it, way], recv_sem=pr.at[it, way],
            device_id={"space": target}, device_id_type=MESH)

    def build_matrix():
        row = lax.broadcasted_iota(jnp.int32, (NODES, LANES), 0)
        lane = lax.broadcasted_iota(jnp.int32, (NODES, LANES), 1)
        first = lane < NODES
        on = row == jnp.bitwise_and(lane, NODES - 1)
        one, zero = jnp.float32(1.0), jnp.float32(0.0)
        lower = jnp.where(on & (row < 16), one, zero)
        upper = jnp.where(on & (row >= 48), one, zero)
        slide = jnp.where(on & (jnp.bitwise_and(row, 3) == 3), one, zero)
        scale = jnp.float32(0.5 * lift_scale)
        side[0] = jnp.concatenate([vol_ref[0], vol_ref[0]], axis=1) + scale * (lower - upper)
        side[1] = jnp.concatenate([vol_ref[1], vol_ref[1]], axis=1) - scale * slide
        side[2] = (scale * jnp.float32(dissipation)) * (lower + upper + slide)

        def row_block(v, carry):
            for j in range(VARS // 2):
                tile = jnp.zeros((NODES, LANES), jnp.float32)
                for d in range(2):
                    factor = jnp.where(first, flux_ref[v, d, 2 * j], flux_ref[v, d, 2 * j + 1])
                    tile = tile + factor * side[d]
                own = jnp.where(first, jnp.where(v == 2 * j, one, zero), jnp.where(v == 2 * j + 1, one, zero))
                tile = tile + own * side[2]
                high = tile.astype(jnp.bfloat16)
                where = (pl.ds(pl.multiple_of(v * NODES, NODES), NODES), pl.ds(j * LANES, LANES))
                a_hi[where] = high
                a_lo[where] = (tile - high.astype(jnp.float32)).astype(jnp.bfloat16)
            return carry

        lax.fori_loop(0, VARS, row_block, 0)

    def volume_part(it):
        u = jnp.concatenate(
            [ub[it, 0].reshape(VARS * NODES, LANES), ub[it, 1].reshape(VARS * NODES, LANES)], axis=1)
        high = u.astype(jnp.bfloat16)
        low = (u - high.astype(jnp.float32)).astype(jnp.bfloat16)
        for part in range(2):
            rows = pl.ds(part * 320, 320)
            out = jnp.dot(a_hi[rows, :], high, preferred_element_type=jnp.float32)
            out = out + jnp.dot(a_hi[rows, :], low, preferred_element_type=jnp.float32)
            out = out + jnp.dot(a_lo[rows, :], high, preferred_element_type=jnp.float32)
            for t in range(2):
                res_ref[t, pl.ds(part * 5, 5)] = out[:, t * LANES:(t + 1) * LANES].reshape(5, NODES, LANES)

    def ring_chunks(step, t):
        ways = (0, 1) if step < 4 else (t,)
        return [(way, part) for part in range(PARTS) for way in ways]

    def ring_start(it, t):
        for way, part in ring_chunks(1, t):
            ring_copy(it, 1, way, t, part).start()

    def ring_relay(it, step, t):
        onward = ring_chunks(step + 1, t) if step < 4 else []
        for way, part in ring_chunks(step, t):
            ring_arrival(it, step, way, t, part).wait_recv()
            if (way, part) in onward:
                ring_copy(it, step + 1, way, t, part).start()

    def pack_traces(it):
        up_pack = jnp.zeros((16, LANES), jnp.float32)
        lo_pack = jnp.zeros((16, LANES), jnp.float32)
        for i in range(2 * VARS):
            mine = (lane16 >= REACH * i) & (lane16 < REACH * (i + 1))
            u_face = ub[it, i // VARS, i % VARS, pl.ds(48, 16), :]
            l_face = ub[it, i // VARS, i % VARS, pl.ds(0, 16), :]
            up_pack = jnp.where(mine, pltpu.roll(u_face, (REACH * i + REACH) % LANES, 1), up_pack)
            lo_pack = jnp.where(mine, pltpu.roll(l_face, REACH * i, 1) if i else l_face, lo_pack)
        packs[it // 2, 0] = up_pack
        packs[it // 2, 1] = lo_pack
        for way in range(2):
            pack_copy(it // 2, way).start()

    scale = jnp.float32(0.5 * lift_scale)
    loss = jnp.float32(0.5 * lift_scale * dissipation)

    def first_direction(it):
        for way in range(2):
            pack_copy(it // 2, way).wait_recv()
        from_before = packed[it // 2, 0]
        from_after = packed[it // 2, 1]
        behind = lane16 - back_gap
        ahead = lane16 + ahead_gap
        for i in range(2 * VARS):
            u_face = ub[it, i // VARS, i % VARS, pl.ds(48, 16), :]
            l_face = ub[it, i // VARS, i % VARS, pl.ds(0, 16), :]
            own = jnp.take_along_axis(u_face, jnp.bitwise_and(behind, LANES - 1), axis=1)
            far = jnp.take_along_axis(from_before, jnp.bitwise_and(behind + REACH * (i + 1), LANES - 1), axis=1)
            lo_b[i // VARS, i % VARS] = jnp.where(behind < 0, far, own)
            own = jnp.take_along_axis(l_face, jnp.bitwise_and(ahead, LANES - 1), axis=1)
            far = jnp.take_along_axis(from_after, jnp.bitwise_and(ahead + REACH * i, LANES - 1), axis=1)
            up_b[i // VARS, i % VARS] = jnp.where(ahead >= LANES, far, own)

        def first_faces(v, c):
            low = -loss * lo_b[:, v]
            upp = -loss * up_b[:, v]
            for w in range(VARS):
                f = scale * flux_ref[v, 0, w]
                low = low - f * lo_b[:, w]
                upp = upp + f * up_b[:, w]
            res_ref[:, v, pl.ds(0, 16), :] += low
            res_ref[:, v, pl.ds(48, 16), :] += upp
            return c

        lax.fori_loop(0, VARS, first_faces, 0)

    half = SAMPLE_COUNT // 2

    def spectral(source, first, second, i):
        x = [source[(side_x + r // 2) % TM, r % 2, i] for r in range(SAMPLE_COUNT)]
        for r in (0, 1, 4, 5):
            near = opposite = None
            for m in range(1, half):
                diff = x[(r + m) % SAMPLE_COUNT] - x[(r - m) % SAMPLE_COUNT]
                one, two = jnp.float32(weights[m - 1]) * diff, jnp.float32(-weights[half - m - 1]) * diff
                near = one if near is None else near + one
                opposite = two if opposite is None else opposite + two
            first[r // 4, r % 2, i] = near
            first[r // 4 + 2, r % 2, i] = opposite
            if second is None:
                continue
            zero, eight = jnp.float32(squares[0]), jnp.float32(squares[half])
            near = zero * x[r] + eight * x[r + half]
            opposite = eight * x[r] + zero * x[r + half]
            for m in range(1, half):
                both = x[(r + m) % SAMPLE_COUNT] + x[(r - m) % SAMPLE_COUNT]
                near = near + jnp.float32(squares[m]) * both
                opposite = opposite + jnp.float32(squares[half - m]) * both
            second[r // 4, r % 2, i] = near
            second[r // 4 + 2, r % 2, i] = opposite

    def derive_state(i, c):
        spectral(gat, dt, dt2, i)
        return c

    def derive_term(i, c):
        spectral(sig_gat, sig_dt, None, i)
        return c

    def rows(c):
        return pl.ds(c, 16, stride=4)

    def tiles_of(buffer, t, v, c):
        places = [slide_place(v, h) if c == 3 else other_place(v, c, h) for h in range(2)]
        return jnp.concatenate([buffer[t, j, i] for j, i in places], axis=0)

    def term_tiles(t, v):
        return jnp.concatenate([sig_tem[t, 2 * v], sig_tem[t, 2 * v + 1]], axis=0)

    def offset_of(kind, t):
        group, shift = group_ref[t], shift_ref[t]
        if kind == 1:
            group = jnp.bitwise_and(2 * group + lax.shift_right_arithmetic(shift, 6), SP - 1)
            shift = jnp.bitwise_and(2 * shift, LANES - 1)
        return group, shift

    lane_b = lax.broadcasted_iota(jnp.int32, (VARS, 16, LANES), 2)

    def column_start(kind, t):
        it = kind // 2
        group, shift = offset_of(kind, t)
        first_dst = jnp.bitwise_and(q - group, Q - 1)
        second_dst = jnp.bitwise_and(q - group - 1, Q - 1)
        first = jnp.bitwise_and(z + lax.shift_right_arithmetic(first_dst + group - q, 2), Z - 1)
        second = jnp.bitwise_and(z + lax.shift_right_arithmetic(second_dst + group + 1 - q, 2), Z - 1)
        cols[kind][t][q] = jnp.where(lane_b >= shift, ring[it][t][first], ring[it][t][second])
        column_copy(kind, 1, t).start()
        column_copy(kind, 0, t).start()

    def column_relay(kind, t):
        column_arrival(kind, 1, t).wait_recv()
        column_copy(kind, 2, t).start()

    def column_finish(kind, t):
        column_arrival(kind, 0, t).wait_recv()
        column_arrival(kind, 2, t).wait_recv()
        group, shift = offset_of(kind, t)
        first = cols[kind][t][jnp.bitwise_and(q + group, Q - 1)]
        second = cols[kind][t][jnp.bitwise_and(q + group + 1, Q - 1)]
        both = jnp.where(lane_b >= shift, first, second)
        both = pltpu.roll(both.reshape(VARS * 16, LANES), jnp.bitwise_and(LANES - shift, LANES - 1), 1)
        return both.reshape(VARS, 16, LANES)

    def turn(t):
        cosine, sine = pick(2 * tm + t, cosines), pick(2 * tm + t, sines)
        one, two = sl_b[t, 1], sl_b[t, 2]
        sl_b[t, 1] = cosine * one - sine * two
        sl_b[t, 2] = sine * one + cosine * two

    def slide_term(t, v):
        term = -loss * sl_b[t, v]
        for w in range(VARS):
            term = term + (scale * flux_ref[v, 1, w]) * sl_b[t, w]
        return term

    step_size = jnp.float32(pseudo_step)
    scope = jax.named_scope

    with scope("start0"):
        for t in range(2):
            for v in range(VARS):
                points = ub[0, t, v, rows(3), :]
                ring[0][t][z, v] = points
                for h in range(2):
                    j, i = slide_place(v, h)
                    up[t, j, i] = points[8 * h:8 * h + 8]
            ring_start(0, t)
        out_all(out_copy, 0, "start")
        pack_traces(0)
        for t in range(2):
            for v in range(VARS):
                for c in range(3):
                    points = ub[0, t, v, rows(c), :]
                    for h in range(2):
                        j, i = other_place(v, c, h)
                        up[t, j, i] = points[8 * h:8 * h + 8]
        out_all(out_copy, 1, "start")
        gat[tm] = up[:, y]
    with scope("matrix"):
        build_matrix()
    with scope("volume0"):
        volume_part(0)
    with scope("ring0_1"):
        ring_relay(0, 1, 0)
        ring_relay(0, 1, 1)
    with scope("out_slide"):
        out_all(out_arrival, 0, "wait_recv")
    with scope("derive_slide"):
        lax.fori_loop(0, 5, derive_state, 0)
        back_all(back_copy, 0, "start")
        out_all(out_copy, 2, "start")
        tem[:, y, pl.ds(0, 5)] = dt[y, :, pl.ds(0, 5)]
    with scope("ring0_2"):
        ring_relay(0, 2, 0)
        ring_relay(0, 2, 1)
    with scope("first0"):
        first_direction(0)
    with scope("ring0_3"):
        ring_relay(0, 3, 0)
    with scope("back_slide"):
        back_all(back_arrival, 0, "wait_recv")
    with scope("w"):
        for t in range(2):
            for v in range(VARS):
                rest = res_ref[t, v, rows(3), :] + tiles_of(tem, t, v, 3)
                ring[1][t][z, v] = ub[0, t, v, rows(3), :] - step_size * rest
    with scope("ring0_3b"):
        ring_relay(0, 3, 1)
        for t in range(2):
            ring_start(1, t)
    with scope("ring0_4"):
        for t in range(2):
            ring_relay(0, 4, t)
            column_start(0, t)
    with scope("cols1_start"):
        for t in range(2):
            column_start(1, t)
    with scope("ring1_1a"):
        ring_relay(1, 1, 0)
    with scope("out_rest"):
        out_all(out_arrival, 1, "wait_recv")
        out_all(out_arrival, 2, "wait_recv")
    with scope("derive_rest"):
        lax.fori_loop(5, 20, derive_state, 0)
        back_all(back_copy, 1, "start")
        back_all(back_copy, 2, "start")
        tem[:, y, pl.ds(5, 15)] = dt[y, :, pl.ds(5, 15)]
        tem2[:, y] = dt2[y]
    with scope("ring1_1b"):
        ring_relay(1, 1, 1)
    with scope("cols0_relay"):
        for t in range(2):
            column_relay(0, t)
    with scope("ring1_2a"):
        ring_relay(1, 2, 0)
    with scope("cols0_finish"):
        for t in range(2):
            sl_b[t] = column_finish(0, t)
            turn(t)

    def sliding_term(v, c):
        for t in range(2):
            term = slide_term(t, v)
            sig[t, 2 * v] = term[0:8]
            sig[t, 2 * v + 1] = term[8:16]
        return c

    with scope("sigma"):
        lax.fori_loop(0, VARS, sliding_term, 0)
        out_all(out_copy, 3, "start")
        sig_gat[tm] = sig[:, pl.ds(5 * y, 5)]
    with scope("ring1_2b"):
        ring_relay(1, 2, 1)
    with scope("cols1_relay"):
        for t in range(2):
            column_relay(1, t)
    with scope("back_rest"):
        back_all(back_arrival, 1, "wait_recv")
    with scope("u1"):
        for t in range(2):
            for v in range(VARS):
                for c in range(4):
                    late = tiles_of(tem, t, v, c)
                    rest = res_ref[t, v, rows(c), :] + late
                    if c == 3:
                        rest = rest + jnp.concatenate([sig[t, 2 * v], sig[t, 2 * v + 1]], axis=0)
                    state = ub[0, t, v, rows(c), :] - step_size * rest
                    ub[1, t, v, rows(c), :] = state
                    ub[2, t, v, rows(c), :] = state - step_size * late
        pack_traces(2)
    with scope("ring1_3a"):
        ring_relay(1, 3, 0)
    with scope("volume1"):
        volume_part(2)
    with scope("ring1_3b"):
        ring_relay(1, 3, 1)
    with scope("out_term"):
        out_all(out_arrival, 3, "wait_recv")
    with scope("derive_term"):
        lax.fori_loop(0, 5, derive_term, 0)
        back_all(back_copy, 3, "start")
        sig_tem[:, pl.ds(5 * y, 5)] = sig_dt[y]
    with scope("ring1_4"):
        for t in range(2):
            ring_relay(1, 4, t)
            column_start(2, t)
    with scope("cols1_finish"):
        for t in range(2):
            sl_b[t] = column_finish(1, t)
            turn(t)

        def twice(v, c):
            for t in range(2):
                tw_b[t, v] = step_size * slide_term(t, v)
            return c

        lax.fori_loop(0, VARS, twice, 0)
    with scope("first1"):
        first_direction(2)
    with scope("back_late"):
        back_all(back_arrival, 2, "wait_recv")
        back_all(back_arrival, 3, "wait_recv")
    with scope("without_slide"):
        for t in range(2):
            for v in range(VARS):
                for c in range(4):
                    late = tiles_of(tem2, t, v, c)
                    if c == 3:
                        late = late + term_tiles(t, v)
                    total = res_ref[t, v, rows(c), :] + (tiles_of(tem, t, v, c) - step_size * late)
                    res_ref[t, v, rows(c), :] = total
                    if c < 3:
                        new_ref[t, v, rows(c), :] = ub[1, t, v, rows(c), :] - step_size * total
    with scope("cols2_relay"):
        for t in range(2):
            column_relay(2, t)
    with scope("cols2_finish"):
        for t in range(2):
            sl_b[t] = column_finish(2, t) - tw_b[t]
            turn(t)

    def finish(v, c):
        for t in range(2):
            total = res_ref[t, v, rows(3), :] + slide_term(t, v)
            res_ref[t, v, rows(3), :] = total
            new_ref[t, v, rows(3), :] = ub[1, t, v, rows(3), :] - step_size * total
        return c

    with scope("finish"):
        lax.fori_loop(0, VARS, finish, 0)
    with scope("sends"):
        for kind in range(4):
            out_all(out_copy, kind, "wait_send")
            back_all(back_copy, kind, "wait_send")
        for kind in range(3):
            for hop in range(3):
                for t in range(2):
                    column_copy(kind, hop, t).wait_send()
        for it in range(ITERS):
            for step in range(1, 5):
                for t in range(2):
                    for way, part in ring_chunks(step, t):
                        ring_copy(it, step, way, t, part).wait_send()
            for way in range(2):
                pack_copy(it, way).wait_send()


def per_device(conserved_field, face_neighbours, counterpart_group, counterpart_shift, volume_operator, flux_matrix):
    state = jax.ShapeDtypeStruct(conserved_field.shape, jnp.float32)
    vmem = pl.BlockSpec(memory_space=pltpu.VMEM)
    f32, bf16 = jnp.float32, jnp.bfloat16
    dma = pltpu.SemaphoreType.DMA
    return pl.pallas_call(
        kernel,
        out_shape=(state, state),
        in_specs=[pl.BlockSpec(memory_space=pltpu.HBM)] * 6,
        out_specs=(vmem, vmem),
        scratch_shapes=[
            pltpu.VMEM((2, LANES), jnp.int32),
            pltpu.SMEM((2,), jnp.int32),
            pltpu.SMEM((2,), jnp.int32),
            pltpu.VMEM((2, NODES, NODES), f32),
            pltpu.SMEM((VARS, 2, VARS), f32),
            pltpu.VMEM((3, 2, VARS, NODES, LANES), f32),
            pltpu.VMEM((VARS * NODES, VARS * NODES), bf16),
            pltpu.VMEM((VARS * NODES, VARS * NODES), bf16),
            pltpu.VMEM((2, 4, 20, 8, LANES), f32),
            pltpu.VMEM((TM, 2, 20, 8, LANES), f32),
            pltpu.VMEM((4, 2, 20, 8, LANES), f32),
            pltpu.VMEM((4, 2, 20, 8, LANES), f32),
            pltpu.VMEM((2, 4, 20, 8, LANES), f32),
            pltpu.VMEM((2, 4, 20, 8, LANES), f32),
            pltpu.VMEM((2, 20, 8, LANES), f32),
            pltpu.VMEM((TM, 2, 5, 8, LANES), f32),
            pltpu.VMEM((4, 2, 5, 8, LANES), f32),
            pltpu.VMEM((2, 20, 8, LANES), f32),
            *[pltpu.VMEM((Z, VARS, 16, LANES), f32)] * 4,
            *[pltpu.VMEM((Q, VARS, 16, LANES), f32)] * 6,
            pltpu.VMEM((ITERS, 2, 16, LANES), f32),
            pltpu.VMEM((ITERS, 2, 16, LANES), f32),
            pltpu.VMEM((3, NODES, LANES), f32),
            pltpu.VMEM((2, VARS, 16, LANES), f32),
            pltpu.VMEM((2, VARS, 16, LANES), f32),
            pltpu.VMEM((2, VARS, 16, LANES), f32),
            pltpu.VMEM((2, VARS, 16, LANES), f32),
            dma((6,)),
            dma((4, 7)), dma((4, 7)),
            dma((4, 3)), dma((4, 3)),
            dma((ITERS, 16 * PARTS)), dma((ITERS, 16 * PARTS)),
            dma((3, 6)), dma((3, 6)),
            dma((ITERS, 2)), dma((ITERS, 2)),
        ],
        compiler_params=pltpu.CompilerParams(
            collective_id=0, has_side_effects=True, vmem_limit_bytes=48 * 1024 * 1024),
        name="iterations",
    )(conserved_field, face_neighbours, counterpart_group, counterpart_shift, volume_operator,
      jnp.transpose(flux_matrix, (1, 0, 2)))


def solution(mesh):
    return jax.shard_map(
        per_device,
        mesh=mesh,
        in_specs=(P("tm", None, None, "space"), P(None, "space"), P("tm"), P("tm"), P(), P()),
        out_specs=(P("tm", None, None, "space"), P("tm", None, None, "space")),
        check_vma=False,
    )
```

```python
import math

import jax
import jax.numpy as jnp
from jax import lax
from jax.experimental import pallas as pl
from jax.experimental.pallas import tpu as pltpu
from jax.sharding import PartitionSpec as P

SAMPLE_COUNT = 16
REACH = 4
ITERS = 2
VARS = 10
NODES = 64
LANES = 128
PARTS = 5
PIECE = VARS // PARTS

lift_scale = 2.0
dissipation = 1.5
angular_speed = 0.5
damping_factor = 4.0
pseudo_step = 0.2

MESH = pl.DeviceIdType.MESH
MOVES = ((2, 1), (1, 1), (3, 1), (0, 1), (2, 0), (1, 0), (3, 0))
TM = 8
SP = 32
Z = 8
Q = 4


def spectral_weights():
    half = SAMPLE_COUNT // 2
    weights = []
    for m in range(1, half):
        total = 0.0
        for k in range(1, half):
            gain = 2.0 * angular_speed * k * math.exp(-damping_factor * (k / half) ** 8) / SAMPLE_COUNT
            total += gain * math.sin(2.0 * math.pi * k * m / SAMPLE_COUNT)
        weights.append(total)
    return weights


def spectral_squares():
    first = [0.0] + spectral_weights() + [0.0]
    full = first + [-first[SAMPLE_COUNT - m] for m in range(SAMPLE_COUNT // 2 + 1, SAMPLE_COUNT)]
    return [
        sum(full[j] * full[(m - j) % SAMPLE_COUNT] for j in range(SAMPLE_COUNT))
        for m in range(SAMPLE_COUNT // 2 + 1)
    ]


def slide_place(v, h):
    index = 2 * v + h
    return index // 5, index % 5


def other_place(v, c, h):
    index = 6 * v + 2 * c + h
    return index // 15, 5 + index % 15


def pick(index, values):
    out = jnp.float32(values[0])
    for k in range(1, len(values)):
        out = jnp.where(index == k, jnp.float32(values[k]), out)
    return out


def kernel(
    u_hbm, fn_hbm, group_hbm, shift_hbm, vol_hbm, flux_hbm,
    new_ref, res_ref, fn_ref, group_ref, shift_ref, vol_ref, flux_ref,
    ub, a_hi, a_lo, up, gat, dt, dt2, tem, tem2, sig, sig_gat, sig_dt, sig_tem, ring_00, ring_01, ring_10, ring_11, cols_00, cols_01, cols_10, cols_11, cols_20, cols_21,
    packs, packed, side, lo_b, up_b, sl_b, tw_b, in_sem, fs, fr, bs, br, zs, zr, cs, cr, ps, pr, xs, xr,
):
    ring = ((ring_00, ring_01), (ring_10, ring_11))
    cols = ((cols_00, cols_01), (cols_10, cols_11), (cols_20, cols_21))
    tm = lax.axis_index("tm")
    sp = lax.axis_index("space")
    z = sp // Q
    q = sp % Q
    y = tm // 2
    side_x = tm % 2

    def space_of(zz, qq):
        return zz * Q + qq

    z_up = space_of((z + 1) % Z, q)
    z_dn = space_of((z + Z - 1) % Z, q)
    mate = space_of(z, q + 1 - 2 * (q % 2))
    cross = space_of(z, (q + 2) % Q)
    after = (sp + 1) % SP
    before = (sp + SP - 1) % SP

    loads = [
        pltpu.make_async_copy(source, target, in_sem.at[k])
        for k, (source, target) in enumerate((
            (u_hbm, ub.at[0]), (flux_hbm, flux_ref), (vol_hbm, vol_ref),
            (fn_hbm, fn_ref), (group_hbm, group_ref), (shift_hbm, shift_ref)))
    ]
    for load in loads:
        load.start()

    barrier = pltpu.get_barrier_semaphore()
    for k in range(1, TM):
        pl.semaphore_signal(barrier, inc=1, device_id={"tm": (tm + k) % TM}, device_id_type=MESH)
    for other in (z_up, z_dn, mate, cross, after, before):
        pl.semaphore_signal(barrier, inc=1, device_id={"space": other}, device_id_type=MESH)
    with jax.named_scope("entry"):
        for load in loads:
            load.wait()
        pl.semaphore_wait(barrier, TM - 1 + 6)

    lane16 = lax.broadcasted_iota(jnp.int32, (16, LANES), 1)
    gidx = sp * LANES + lane16
    back_gap = jnp.bitwise_and(gidx - fn_ref[0:1, :], SP * LANES - 1)
    ahead_gap = jnp.bitwise_and(fn_ref[1:2, :] - gidx, SP * LANES - 1)

    weights = spectral_weights()
    squares = spectral_squares()
    cosines = [math.cos(2.0 * math.pi * k / SAMPLE_COUNT) for k in range(SAMPLE_COUNT)]
    sines = [math.sin(2.0 * math.pi * k / SAMPLE_COUNT) for k in range(SAMPLE_COUNT)]

    OUT = ((0, 5), (5, 5), (10, 10))
    BACK = ((0, 5), (5, 5), (10, 10), None, (0, 5), (5, 5), (10, 10))

    def peer_at(k, sign):
        dy, dx = MOVES[k]
        row = (y + sign * dy + 4) % 4
        return row, row * 2 + (side_x + dx) % 2

    def out_refs(kind, row, place):
        if kind == 3:
            return sig.at[:, pl.ds(5 * row, 5)], sig_gat.at[place]
        tiles = pl.ds(*OUT[kind])
        return up.at[:, row, tiles], gat.at[place, :, tiles]

    def back_refs(kind, row, place):
        if kind == 3:
            return sig_dt.at[row], sig_tem.at[:, pl.ds(5 * place, 5)]
        tiles = pl.ds(*BACK[kind])
        source, target = (dt2, tem2) if kind > 3 else (dt, tem)
        return source.at[row, :, tiles], target.at[:, place, tiles]

    def out_copy(kind, k):
        row, peer = peer_at(k, 1)
        source, target = out_refs(kind, row, tm)
        return pltpu.make_async_remote_copy(
            src_ref=source, dst_ref=target, send_sem=fs.at[kind, k], recv_sem=fr.at[kind, k],
            device_id={"tm": peer}, device_id_type=MESH)

    def out_arrival(kind, k):
        row, peer = peer_at(k, -1)
        source, target = out_refs(kind, row, peer)
        return pltpu.make_async_remote_copy(
            src_ref=source, dst_ref=target, send_sem=fs.at[kind, k], recv_sem=fr.at[kind, k],
            device_id={"tm": peer}, device_id_type=MESH)

    def back_copy(kind, k):
        row, peer = peer_at(k, 1)
        source, target = back_refs(kind, row, y)
        return pltpu.make_async_remote_copy(
            src_ref=source, dst_ref=target, send_sem=bs.at[kind, k - 4], recv_sem=br.at[kind, k - 4],
            device_id={"tm": peer}, device_id_type=MESH)

    def back_arrival(kind, k):
        row, peer = peer_at(k, -1)
        source, target = back_refs(kind, row, row)
        return pltpu.make_async_remote_copy(
            src_ref=source, dst_ref=target, send_sem=bs.at[kind, k - 4], recv_sem=br.at[kind, k - 4],
            device_id={"tm": peer}, device_id_type=MESH)

    def out_all(make, kind, method):
        for k in range(7) if kind in (0, 3) else range(4, 7):
            getattr(make(kind, k), method)()

    def pass_on(kind, k, side):
        row = (y if k == 7 else peer_at(k, -1)[0])
        place = row * 2 + (side_x if side == 0 else 1 - side_x)
        block = gat.at[place, :, pl.ds(*OUT[kind])]
        slot = (kind - 1) * 4 + k - 4
        return pltpu.make_async_remote_copy(
            src_ref=block, dst_ref=block, send_sem=xs.at[slot], recv_sem=xr.at[slot],
            device_id={"tm": y * 2 + 1 - side_x}, device_id_type=MESH)

    def relay_points(kind):
        for k in (5, 6, 4):
            out_arrival(kind, k).wait_recv()
            pass_on(kind, k, 0).start()

    def wait_points(kind):
        for k in (7, 5, 6, 4):
            pass_on(kind, k, 1).wait_recv()

    def back_all(make, kind, method):
        for k in range(4, 7):
            getattr(make(kind, k), method)()

    def ring_slot(step, way, t, part):
        return (((step - 1) * 2 + way) * 2 + t) * PARTS + part

    def ring_copy(it, step, way, t, part):
        if way == 0:
            origin, target = (z + Z - (step - 1)) % Z, z_up
        else:
            origin, target = (z + step - 1) % Z, z_dn
        block = ring[it][t].at[origin, pl.ds(part * PIECE, PIECE)]
        slot = ring_slot(step, way, t, part)
        return pltpu.make_async_remote_copy(
            src_ref=block, dst_ref=block, send_sem=zs.at[it, slot], recv_sem=zr.at[it, slot],
            device_id={"space": target}, device_id_type=MESH)

    def ring_arrival(it, step, way, t, part):
        if way == 0:
            origin, target = (z + Z - step) % Z, z_up
        else:
            origin, target = (z + step) % Z, z_dn
        block = ring[it][t].at[origin, pl.ds(part * PIECE, PIECE)]
        slot = ring_slot(step, way, t, part)
        return pltpu.make_async_remote_copy(
            src_ref=block, dst_ref=block, send_sem=zs.at[it, slot], recv_sem=zr.at[it, slot],
            device_id={"space": target}, device_id_type=MESH)

    def column_copy(kind, hop, t):
        origin, target = ((q, mate), (q, cross), ((q + 2) % Q, mate))[hop]
        block = cols[kind][t].at[origin]
        slot = hop * 2 + t
        return pltpu.make_async_remote_copy(
            src_ref=block, dst_ref=block, send_sem=cs.at[kind, slot], recv_sem=cr.at[kind, slot],
            device_id={"space": target}, device_id_type=MESH)

    def column_arrival(kind, hop, t):
        mate_q = q + 1 - 2 * (q % 2)
        origin, target = ((mate_q, mate), ((q + 2) % Q, cross), ((mate_q + 2) % Q, mate))[hop]
        block = cols[kind][t].at[origin]
        slot = hop * 2 + t
        return pltpu.make_async_remote_copy(
            src_ref=block, dst_ref=block, send_sem=cs.at[kind, slot], recv_sem=cr.at[kind, slot],
            device_id={"space": target}, device_id_type=MESH)

    def pack_copy(it, way):
        target = (after, before)[way]
        return pltpu.make_async_remote_copy(
            src_ref=packs.at[it, way], dst_ref=packed.at[it, way], send_sem=ps.at[it, way], recv_sem=pr.at[it, way],
            device_id={"space": target}, device_id_type=MESH)

    def build_matrix():
        row = lax.broadcasted_iota(jnp.int32, (NODES, LANES), 0)
        lane = lax.broadcasted_iota(jnp.int32, (NODES, LANES), 1)
        first = lane < NODES
        on = row == jnp.bitwise_and(lane, NODES - 1)
        one, zero = jnp.float32(1.0), jnp.float32(0.0)
        lower = jnp.where(on & (row < 16), one, zero)
        upper = jnp.where(on & (row >= 48), one, zero)
        slide = jnp.where(on & (jnp.bitwise_and(row, 3) == 3), one, zero)
        scale = jnp.float32(0.5 * lift_scale)
        side[0] = jnp.concatenate([vol_ref[0], vol_ref[0]], axis=1) + scale * (lower - upper)
        side[1] = jnp.concatenate([vol_ref[1], vol_ref[1]], axis=1) - scale * slide
        side[2] = (scale * jnp.float32(dissipation)) * (lower + upper + slide)

        def row_block(v, carry):
            for j in range(VARS // 2):
                tile = jnp.zeros((NODES, LANES), jnp.float32)
                for d in range(2):
                    factor = jnp.where(first, flux_ref[v, d, 2 * j], flux_ref[v, d, 2 * j + 1])
                    tile = tile + factor * side[d]
                own = jnp.where(first, jnp.where(v == 2 * j, one, zero), jnp.where(v == 2 * j + 1, one, zero))
                tile = tile + own * side[2]
                high = tile.astype(jnp.bfloat16)
                where = (pl.ds(pl.multiple_of(v * NODES, NODES), NODES), pl.ds(j * LANES, LANES))
                a_hi[where] = high
                a_lo[where] = (tile - high.astype(jnp.float32)).astype(jnp.bfloat16)
            return carry

        lax.fori_loop(0, VARS, row_block, 0)

    def volume_part(it):
        u = jnp.concatenate(
            [ub[it, 0].reshape(VARS * NODES, LANES), ub[it, 1].reshape(VARS * NODES, LANES)], axis=1)
        high = u.astype(jnp.bfloat16)
        low = (u - high.astype(jnp.float32)).astype(jnp.bfloat16)
        for part in range(2):
            rows = pl.ds(part * 320, 320)
            out = jnp.dot(a_hi[rows, :], high, preferred_element_type=jnp.float32)
            out = out + jnp.dot(a_hi[rows, :], low, preferred_element_type=jnp.float32)
            out = out + jnp.dot(a_lo[rows, :], high, preferred_element_type=jnp.float32)
            for t in range(2):
                res_ref[t, pl.ds(part * 5, 5)] = out[:, t * LANES:(t + 1) * LANES].reshape(5, NODES, LANES)

    def ring_chunks(step, t):
        ways = (0, 1) if step < 4 else (t,)
        return [(way, part) for part in range(PARTS) for way in ways]

    def ring_start(it, t):
        for way, part in ring_chunks(1, t):
            ring_copy(it, 1, way, t, part).start()

    def ring_relay(it, step, t):
        onward = ring_chunks(step + 1, t) if step < 4 else []
        for way, part in ring_chunks(step, t):
            ring_arrival(it, step, way, t, part).wait_recv()
            if (way, part) in onward:
                ring_copy(it, step + 1, way, t, part).start()

    def pack_traces(it):
        up_pack = jnp.zeros((16, LANES), jnp.float32)
        lo_pack = jnp.zeros((16, LANES), jnp.float32)
        for i in range(2 * VARS):
            mine = (lane16 >= REACH * i) & (lane16 < REACH * (i + 1))
            u_face = ub[it, i // VARS, i % VARS, pl.ds(48, 16), :]
            l_face = ub[it, i // VARS, i % VARS, pl.ds(0, 16), :]
            up_pack = jnp.where(mine, pltpu.roll(u_face, (REACH * i + REACH) % LANES, 1), up_pack)
            lo_pack = jnp.where(mine, pltpu.roll(l_face, REACH * i, 1) if i else l_face, lo_pack)
        packs[it // 2, 0] = up_pack
        packs[it // 2, 1] = lo_pack
        for way in range(2):
            pack_copy(it // 2, way).start()

    scale = jnp.float32(0.5 * lift_scale)
    loss = jnp.float32(0.5 * lift_scale * dissipation)

    def first_direction(it):
        for way in range(2):
            pack_copy(it // 2, way).wait_recv()
        from_before = packed[it // 2, 0]
        from_after = packed[it // 2, 1]
        behind = lane16 - back_gap
        ahead = lane16 + ahead_gap
        for i in range(2 * VARS):
            u_face = ub[it, i // VARS, i % VARS, pl.ds(48, 16), :]
            l_face = ub[it, i // VARS, i % VARS, pl.ds(0, 16), :]
            own = jnp.take_along_axis(u_face, jnp.bitwise_and(behind, LANES - 1), axis=1)
            far = jnp.take_along_axis(from_before, jnp.bitwise_and(behind + REACH * (i + 1), LANES - 1), axis=1)
            lo_b[i // VARS, i % VARS] = jnp.where(behind < 0, far, own)
            own = jnp.take_along_axis(l_face, jnp.bitwise_and(ahead, LANES - 1), axis=1)
            far = jnp.take_along_axis(from_after, jnp.bitwise_and(ahead + REACH * i, LANES - 1), axis=1)
            up_b[i // VARS, i % VARS] = jnp.where(ahead >= LANES, far, own)

        def first_faces(v, c):
            low = -loss * lo_b[:, v]
            upp = -loss * up_b[:, v]
            for w in range(VARS):
                f = scale * flux_ref[v, 0, w]
                low = low - f * lo_b[:, w]
                upp = upp + f * up_b[:, w]
            res_ref[:, v, pl.ds(0, 16), :] += low
            res_ref[:, v, pl.ds(48, 16), :] += upp
            return c

        lax.fori_loop(0, VARS, first_faces, 0)

    half = SAMPLE_COUNT // 2

    def spectral(source, first, second, i):
        x = [source[(side_x + r // 2) % TM, r % 2, i] for r in range(SAMPLE_COUNT)]
        for r in (0, 1, 4, 5):
            near = opposite = None
            for m in range(1, half):
                diff = x[(r + m) % SAMPLE_COUNT] - x[(r - m) % SAMPLE_COUNT]
                one, two = jnp.float32(weights[m - 1]) * diff, jnp.float32(-weights[half - m - 1]) * diff
                near = one if near is None else near + one
                opposite = two if opposite is None else opposite + two
            first[r // 4, r % 2, i] = near
            first[r // 4 + 2, r % 2, i] = opposite
            if second is None:
                continue
            zero, eight = jnp.float32(squares[0]), jnp.float32(squares[half])
            near = zero * x[r] + eight * x[r + half]
            opposite = eight * x[r] + zero * x[r + half]
            for m in range(1, half):
                both = x[(r + m) % SAMPLE_COUNT] + x[(r - m) % SAMPLE_COUNT]
                near = near + jnp.float32(squares[m]) * both
                opposite = opposite + jnp.float32(squares[half - m]) * both
            second[r // 4, r % 2, i] = near
            second[r // 4 + 2, r % 2, i] = opposite

    def derive_state(i, c):
        spectral(gat, dt, dt2, i)
        return c

    def derive_term(i, c):
        spectral(sig_gat, sig_dt, None, i)
        return c

    def rows(c):
        return pl.ds(c, 16, stride=4)

    def tiles_of(buffer, t, v, c):
        places = [slide_place(v, h) if c == 3 else other_place(v, c, h) for h in range(2)]
        return jnp.concatenate([buffer[t, j, i] for j, i in places], axis=0)

    def term_tiles(t, v):
        return jnp.concatenate([sig_tem[t, 2 * v], sig_tem[t, 2 * v + 1]], axis=0)

    def offset_of(kind, t):
        group, shift = group_ref[t], shift_ref[t]
        if kind == 1:
            group = jnp.bitwise_and(2 * group + lax.shift_right_arithmetic(shift, 6), SP - 1)
            shift = jnp.bitwise_and(2 * shift, LANES - 1)
        return group, shift

    lane_b = lax.broadcasted_iota(jnp.int32, (VARS, 16, LANES), 2)

    def column_start(kind, t):
        it = kind // 2
        group, shift = offset_of(kind, t)
        first_dst = jnp.bitwise_and(q - group, Q - 1)
        second_dst = jnp.bitwise_and(q - group - 1, Q - 1)
        first = jnp.bitwise_and(z + lax.shift_right_arithmetic(first_dst + group - q, 2), Z - 1)
        second = jnp.bitwise_and(z + lax.shift_right_arithmetic(second_dst + group + 1 - q, 2), Z - 1)
        cols[kind][t][q] = jnp.where(lane_b >= shift, ring[it][t][first], ring[it][t][second])
        column_copy(kind, 1, t).start()
        column_copy(kind, 0, t).start()

    def column_relay(kind, t):
        column_arrival(kind, 1, t).wait_recv()
        column_copy(kind, 2, t).start()

    def column_finish(kind, t):
        column_arrival(kind, 0, t).wait_recv()
        column_arrival(kind, 2, t).wait_recv()
        group, shift = offset_of(kind, t)
        first = cols[kind][t][jnp.bitwise_and(q + group, Q - 1)]
        second = cols[kind][t][jnp.bitwise_and(q + group + 1, Q - 1)]
        both = jnp.where(lane_b >= shift, first, second)
        both = pltpu.roll(both.reshape(VARS * 16, LANES), jnp.bitwise_and(LANES - shift, LANES - 1), 1)
        return both.reshape(VARS, 16, LANES)

    def turn(t):
        cosine, sine = pick(2 * tm + t, cosines), pick(2 * tm + t, sines)
        one, two = sl_b[t, 1], sl_b[t, 2]
        sl_b[t, 1] = cosine * one - sine * two
        sl_b[t, 2] = sine * one + cosine * two

    def slide_term(t, v):
        term = -loss * sl_b[t, v]
        for w in range(VARS):
            term = term + (scale * flux_ref[v, 1, w]) * sl_b[t, w]
        return term

    step_size = jnp.float32(pseudo_step)
    scope = jax.named_scope

    with scope("start0"):
        for t in range(2):
            for v in range(VARS):
                points = ub[0, t, v, rows(3), :]
                ring[0][t][z, v] = points
                for h in range(2):
                    j, i = slide_place(v, h)
                    up[t, j, i] = points[8 * h:8 * h + 8]
            ring_start(0, t)
        out_all(out_copy, 0, "start")
        pack_traces(0)
        for t in range(2):
            for v in range(VARS):
                for c in range(3):
                    points = ub[0, t, v, rows(c), :]
                    for h in range(2):
                        j, i = other_place(v, c, h)
                        up[t, j, i] = points[8 * h:8 * h + 8]
        gat[tm] = up[:, y]
        for kind in (1, 2):
            out_all(out_copy, kind, "start")
            pass_on(kind, 7, 0).start()
    with scope("matrix"):
        build_matrix()
    with scope("volume0"):
        volume_part(0)
    with scope("ring0_1"):
        ring_relay(0, 1, 0)
        ring_relay(0, 1, 1)
    with scope("ring0_2a"):
        ring_relay(0, 2, 0)
    with scope("out_slide"):
        out_all(out_arrival, 0, "wait_recv")
    with scope("derive_slide"):
        lax.fori_loop(0, 5, derive_state, 0)
        back_all(back_copy, 0, "start")
        back_all(back_copy, 4, "start")
        tem[:, y, pl.ds(0, 5)] = dt[y, :, pl.ds(0, 5)]
    with scope("ring0_2b"):
        ring_relay(0, 2, 1)
    with scope("points1"):
        relay_points(1)
    with scope("first0"):
        first_direction(0)
    with scope("ring0_3"):
        ring_relay(0, 3, 0)
    with scope("points2"):
        relay_points(2)
    with scope("ring0_3b"):
        ring_relay(0, 3, 1)
    with scope("ring0_4"):
        for t in range(2):
            ring_relay(0, 4, t)
            column_start(0, t)
    with scope("back_slide"):
        back_all(back_arrival, 0, "wait_recv")
    with scope("w"):
        for t in range(2):
            for v in range(VARS):
                rest = res_ref[t, v, rows(3), :] + tiles_of(tem, t, v, 3)
                ring[1][t][z, v] = ub[0, t, v, rows(3), :] - step_size * rest
            ring_start(1, t)
    with scope("cols1_start"):
        for t in range(2):
            column_start(1, t)
    with scope("rest1"):
        wait_points(1)
        lax.fori_loop(5, 10, derive_state, 0)
        back_all(back_copy, 1, "start")
        back_all(back_copy, 5, "start")
        tem[:, y, pl.ds(5, 5)] = dt[y, :, pl.ds(5, 5)]
    with scope("ring1_1a"):
        ring_relay(1, 1, 0)
    with scope("rest2"):
        wait_points(2)
        lax.fori_loop(10, 20, derive_state, 0)
        back_all(back_copy, 2, "start")
        back_all(back_copy, 6, "start")
        tem[:, y, pl.ds(10, 10)] = dt[y, :, pl.ds(10, 10)]
        tem2[:, y] = dt2[y]
    with scope("ring1_1b"):
        ring_relay(1, 1, 1)
    with scope("ring1_2a"):
        ring_relay(1, 2, 0)
    with scope("cols0_relay"):
        for t in range(2):
            column_relay(0, t)
    with scope("ring1_2b"):
        ring_relay(1, 2, 1)
    with scope("cols0_finish"):
        for t in range(2):
            sl_b[t] = column_finish(0, t)
            turn(t)

    def sliding_term(v, c):
        for t in range(2):
            term = slide_term(t, v)
            sig[t, 2 * v] = term[0:8]
            sig[t, 2 * v + 1] = term[8:16]
        return c

    with scope("sigma"):
        lax.fori_loop(0, VARS, sliding_term, 0)
        out_all(out_copy, 3, "start")
        sig_gat[tm] = sig[:, pl.ds(5 * y, 5)]
    with scope("ring1_3a"):
        ring_relay(1, 3, 0)
    with scope("cols1_relay"):
        for t in range(2):
            column_relay(1, t)
    with scope("back_rest"):
        back_all(back_arrival, 1, "wait_recv")
        back_all(back_arrival, 2, "wait_recv")
    with scope("u1"):
        for t in range(2):
            for v in range(VARS):
                for c in range(4):
                    late = tiles_of(tem, t, v, c)
                    rest = res_ref[t, v, rows(c), :] + late
                    if c == 3:
                        rest = rest + jnp.concatenate([sig[t, 2 * v], sig[t, 2 * v + 1]], axis=0)
                    state = ub[0, t, v, rows(c), :] - step_size * rest
                    ub[1, t, v, rows(c), :] = state
                    ub[2, t, v, rows(c), :] = state - step_size * late
        pack_traces(2)
    with scope("ring1_3b"):
        ring_relay(1, 3, 1)
    with scope("volume1"):
        volume_part(2)
    with scope("ring1_4"):
        for t in range(2):
            ring_relay(1, 4, t)
            column_start(2, t)
    with scope("out_term"):
        out_all(out_arrival, 3, "wait_recv")
    with scope("derive_term"):
        lax.fori_loop(0, 5, derive_term, 0)
        back_all(back_copy, 3, "start")
        sig_tem[:, pl.ds(5 * y, 5)] = sig_dt[y]
    with scope("cols1_finish"):
        for t in range(2):
            sl_b[t] = column_finish(1, t)
            turn(t)

        def twice(v, c):
            for t in range(2):
                tw_b[t, v] = step_size * slide_term(t, v)
            return c

        lax.fori_loop(0, VARS, twice, 0)
    with scope("first1"):
        first_direction(2)
    with scope("cols2_relay"):
        for t in range(2):
            column_relay(2, t)
    with scope("back_late"):
        for kind in (4, 5, 6, 3):
            back_all(back_arrival, kind, "wait_recv")
    with scope("without_slide"):
        for t in range(2):
            for v in range(VARS):
                for c in range(4):
                    late = tiles_of(tem2, t, v, c)
                    if c == 3:
                        late = late + term_tiles(t, v)
                    total = res_ref[t, v, rows(c), :] + (tiles_of(tem, t, v, c) - step_size * late)
                    res_ref[t, v, rows(c), :] = total
                    if c < 3:
                        new_ref[t, v, rows(c), :] = ub[1, t, v, rows(c), :] - step_size * total
    with scope("cols2_finish"):
        for t in range(2):
            sl_b[t] = column_finish(2, t) - tw_b[t]
            turn(t)

    def finish(v, c):
        for t in range(2):
            total = res_ref[t, v, rows(3), :] + slide_term(t, v)
            res_ref[t, v, rows(3), :] = total
            new_ref[t, v, rows(3), :] = ub[1, t, v, rows(3), :] - step_size * total
        return c

    with scope("finish"):
        lax.fori_loop(0, VARS, finish, 0)
    with scope("sends"):
        for kind in range(4):
            out_all(out_copy, kind, "wait_send")
        for kind in range(7):
            back_all(back_copy, kind, "wait_send")
        for kind in (1, 2):
            for k in range(4, 8):
                pass_on(kind, k, 0).wait_send()
        for kind in range(3):
            for hop in range(3):
                for t in range(2):
                    column_copy(kind, hop, t).wait_send()
        for it in range(ITERS):
            for step in range(1, 5):
                for t in range(2):
                    for way, part in ring_chunks(step, t):
                        ring_copy(it, step, way, t, part).wait_send()
            for way in range(2):
                pack_copy(it, way).wait_send()


def per_device(conserved_field, face_neighbours, counterpart_group, counterpart_shift, volume_operator, flux_matrix):
    state = jax.ShapeDtypeStruct(conserved_field.shape, jnp.float32)
    vmem = pl.BlockSpec(memory_space=pltpu.VMEM)
    f32, bf16 = jnp.float32, jnp.bfloat16
    dma = pltpu.SemaphoreType.DMA
    return pl.pallas_call(
        kernel,
        out_shape=(state, state),
        in_specs=[pl.BlockSpec(memory_space=pltpu.HBM)] * 6,
        out_specs=(vmem, vmem),
        scratch_shapes=[
            pltpu.VMEM((2, LANES), jnp.int32),
            pltpu.SMEM((2,), jnp.int32),
            pltpu.SMEM((2,), jnp.int32),
            pltpu.VMEM((2, NODES, NODES), f32),
            pltpu.SMEM((VARS, 2, VARS), f32),
            pltpu.VMEM((3, 2, VARS, NODES, LANES), f32),
            pltpu.VMEM((VARS * NODES, VARS * NODES), bf16),
            pltpu.VMEM((VARS * NODES, VARS * NODES), bf16),
            pltpu.VMEM((2, 4, 20, 8, LANES), f32),
            pltpu.VMEM((TM, 2, 20, 8, LANES), f32),
            pltpu.VMEM((4, 2, 20, 8, LANES), f32),
            pltpu.VMEM((4, 2, 20, 8, LANES), f32),
            pltpu.VMEM((2, 4, 20, 8, LANES), f32),
            pltpu.VMEM((2, 4, 20, 8, LANES), f32),
            pltpu.VMEM((2, 20, 8, LANES), f32),
            pltpu.VMEM((TM, 2, 5, 8, LANES), f32),
            pltpu.VMEM((4, 2, 5, 8, LANES), f32),
            pltpu.VMEM((2, 20, 8, LANES), f32),
            *[pltpu.VMEM((Z, VARS, 16, LANES), f32)] * 4,
            *[pltpu.VMEM((Q, VARS, 16, LANES), f32)] * 6,
            pltpu.VMEM((ITERS, 2, 16, LANES), f32),
            pltpu.VMEM((ITERS, 2, 16, LANES), f32),
            pltpu.VMEM((3, NODES, LANES), f32),
            pltpu.VMEM((2, VARS, 16, LANES), f32),
            pltpu.VMEM((2, VARS, 16, LANES), f32),
            pltpu.VMEM((2, VARS, 16, LANES), f32),
            pltpu.VMEM((2, VARS, 16, LANES), f32),
            dma((6,)),
            dma((4, 7)), dma((4, 7)),
            dma((7, 3)), dma((7, 3)),
            dma((ITERS, 16 * PARTS)), dma((ITERS, 16 * PARTS)),
            dma((3, 6)), dma((3, 6)),
            dma((ITERS, 2)), dma((ITERS, 2)),
            dma((8,)), dma((8,)),
        ],
        compiler_params=pltpu.CompilerParams(
            collective_id=0, has_side_effects=True, vmem_limit_bytes=63 * 1024 * 1024),
        name="iterations",
    )(conserved_field, face_neighbours, counterpart_group, counterpart_shift, volume_operator,
      jnp.transpose(flux_matrix, (1, 0, 2)))


def solution(mesh):
    return jax.shard_map(
        per_device,
        mesh=mesh,
        in_specs=(P("tm", None, None, "space"), P(None, "space"), P("tm"), P("tm"), P(), P()),
        out_specs=(P("tm", None, None, "space"), P("tm", None, None, "space")),
        check_vma=False,
    )
```

```python
import math

import jax
import jax.numpy as jnp
from jax import lax
from jax.experimental import pallas as pl
from jax.experimental.pallas import tpu as pltpu
from jax.sharding import PartitionSpec as P

SAMPLE_COUNT = 16
REACH = 4
ITERS = 2
VARS = 10
NODES = 64
LANES = 128
PARTS = 5
PIECE = VARS // PARTS

lift_scale = 2.0
dissipation = 1.5
angular_speed = 0.5
damping_factor = 4.0
pseudo_step = 0.2

MESH = pl.DeviceIdType.MESH
MOVES = ((2, 1), (1, 1), (3, 1), (0, 1), (2, 0), (1, 0), (3, 0))
TM = 8
SP = 32
Z = 8
Q = 4


def spectral_weights():
    half = SAMPLE_COUNT // 2
    weights = []
    for m in range(1, half):
        total = 0.0
        for k in range(1, half):
            gain = 2.0 * angular_speed * k * math.exp(-damping_factor * (k / half) ** 8) / SAMPLE_COUNT
            total += gain * math.sin(2.0 * math.pi * k * m / SAMPLE_COUNT)
        weights.append(total)
    return weights


def spectral_squares():
    first = [0.0] + spectral_weights() + [0.0]
    full = first + [-first[SAMPLE_COUNT - m] for m in range(SAMPLE_COUNT // 2 + 1, SAMPLE_COUNT)]
    return [
        sum(full[j] * full[(m - j) % SAMPLE_COUNT] for j in range(SAMPLE_COUNT))
        for m in range(SAMPLE_COUNT // 2 + 1)
    ]


def slide_place(v, h):
    index = 2 * v + h
    return index // 5, index % 5


def other_place(v, c, h):
    index = 6 * v + 2 * c + h
    return index // 15, 5 + index % 15


def pick(index, values):
    out = jnp.float32(values[0])
    for k in range(1, len(values)):
        out = jnp.where(index == k, jnp.float32(values[k]), out)
    return out


def kernel(
    u_hbm, fn_hbm, group_hbm, shift_hbm, vol_hbm, flux_hbm,
    new_ref, res_ref, fn_ref, group_ref, shift_ref, vol_ref, flux_ref,
    ub, a_hi, a_lo, up, gat, dt, dt2, tem, tem2, sig, sig_gat, sig_dt, sig_tem, ring_00, ring_01, ring_10, ring_11, cols_00, cols_01, cols_10, cols_11, cols_20, cols_21,
    packs, packed, side, lo_b, up_b, sl_b, tw_b, in_sem, fs, fr, bs, br, zs, zr, cs, cr, ps, pr, xs, xr,
):
    ring = ((ring_00, ring_01), (ring_10, ring_11))
    cols = ((cols_00, cols_01), (cols_10, cols_11), (cols_20, cols_21))
    tm = lax.axis_index("tm")
    sp = lax.axis_index("space")
    z = sp // Q
    q = sp % Q
    y = tm // 2
    side_x = tm % 2

    def space_of(zz, qq):
        return zz * Q + qq

    z_up = space_of((z + 1) % Z, q)
    z_dn = space_of((z + Z - 1) % Z, q)
    mate = space_of(z, q + 1 - 2 * (q % 2))
    cross = space_of(z, (q + 2) % Q)
    after = (sp + 1) % SP
    before = (sp + SP - 1) % SP

    loads = [
        pltpu.make_async_copy(source, target, in_sem.at[k])
        for k, (source, target) in enumerate((
            (u_hbm, ub.at[0]), (flux_hbm, flux_ref), (vol_hbm, vol_ref),
            (fn_hbm, fn_ref), (group_hbm, group_ref), (shift_hbm, shift_ref)))
    ]
    for load in loads:
        load.start()

    barrier = pltpu.get_barrier_semaphore()
    for k in range(1, TM):
        pl.semaphore_signal(barrier, inc=1, device_id={"tm": (tm + k) % TM}, device_id_type=MESH)
    for other in (z_up, z_dn, mate, cross, after, before):
        pl.semaphore_signal(barrier, inc=1, device_id={"space": other}, device_id_type=MESH)
    with jax.named_scope("entry"):
        for load in loads:
            load.wait()
        pl.semaphore_wait(barrier, TM - 1 + 6)

    lane16 = lax.broadcasted_iota(jnp.int32, (16, LANES), 1)
    gidx = sp * LANES + lane16
    back_gap = jnp.bitwise_and(gidx - fn_ref[0:1, :], SP * LANES - 1)
    ahead_gap = jnp.bitwise_and(fn_ref[1:2, :] - gidx, SP * LANES - 1)

    weights = spectral_weights()
    squares = spectral_squares()
    cosines = [math.cos(2.0 * math.pi * k / SAMPLE_COUNT) for k in range(SAMPLE_COUNT)]
    sines = [math.sin(2.0 * math.pi * k / SAMPLE_COUNT) for k in range(SAMPLE_COUNT)]

    OUT = ((0, 5), (5, 5), (10, 10))
    BACK = ((0, 5), (5, 5), (10, 10), None, (0, 5), (5, 5), (10, 10))

    def peer_at(k, sign):
        dy, dx = MOVES[k]
        row = (y + sign * dy + 4) % 4
        return row, row * 2 + (side_x + dx) % 2

    def out_refs(kind, row, place):
        if kind == 3:
            return sig.at[:, pl.ds(5 * row, 5)], sig_gat.at[place]
        tiles = pl.ds(*OUT[kind])
        return up.at[:, row, tiles], gat.at[place, :, tiles]

    def back_refs(kind, row, place):
        if kind == 3:
            return sig_dt.at[row], sig_tem.at[:, pl.ds(5 * place, 5)]
        tiles = pl.ds(*BACK[kind])
        source, target = (dt2, tem2) if kind > 3 else (dt, tem)
        return source.at[row, :, tiles], target.at[:, place, tiles]

    def out_copy(kind, k):
        row, peer = peer_at(k, 1)
        source, target = out_refs(kind, row, tm)
        return pltpu.make_async_remote_copy(
            src_ref=source, dst_ref=target, send_sem=fs.at[kind, k], recv_sem=fr.at[kind, k],
            device_id={"tm": peer}, device_id_type=MESH)

    def out_arrival(kind, k):
        row, peer = peer_at(k, -1)
        source, target = out_refs(kind, row, peer)
        return pltpu.make_async_remote_copy(
            src_ref=source, dst_ref=target, send_sem=fs.at[kind, k], recv_sem=fr.at[kind, k],
            device_id={"tm": peer}, device_id_type=MESH)

    def back_copy(kind, k):
        row, peer = peer_at(k, 1)
        source, target = back_refs(kind, row, y)
        return pltpu.make_async_remote_copy(
            src_ref=source, dst_ref=target, send_sem=bs.at[kind, k - 4], recv_sem=br.at[kind, k - 4],
            device_id={"tm": peer}, device_id_type=MESH)

    def back_arrival(kind, k):
        row, peer = peer_at(k, -1)
        source, target = back_refs(kind, row, row)
        return pltpu.make_async_remote_copy(
            src_ref=source, dst_ref=target, send_sem=bs.at[kind, k - 4], recv_sem=br.at[kind, k - 4],
            device_id={"tm": peer}, device_id_type=MESH)

    def out_all(make, kind, method):
        for k in range(7) if kind in (0, 3) else range(4, 7):
            getattr(make(kind, k), method)()

    def pass_on(kind, k, side):
        row = (y if k == 7 else peer_at(k, -1)[0])
        place = row * 2 + (side_x if side == 0 else 1 - side_x)
        block = gat.at[place, :, pl.ds(*OUT[kind])]
        slot = (kind - 1) * 4 + k - 4
        return pltpu.make_async_remote_copy(
            src_ref=block, dst_ref=block, send_sem=xs.at[slot], recv_sem=xr.at[slot],
            device_id={"tm": y * 2 + 1 - side_x}, device_id_type=MESH)

    def relay_points(kind):
        for k in (5, 6, 4):
            out_arrival(kind, k).wait_recv()
            pass_on(kind, k, 0).start()

    def wait_points(kind):
        for k in (7, 5, 6, 4):
            pass_on(kind, k, 1).wait_recv()

    def back_all(make, kind, method):
        for k in range(4, 7):
            getattr(make(kind, k), method)()

    def ring_slot(step, way, t, part):
        return (((step - 1) * 2 + way) * 2 + t) * PARTS + part

    def ring_copy(it, step, way, t, part):
        if way == 0:
            origin, target = (z + Z - (step - 1)) % Z, z_up
        else:
            origin, target = (z + step - 1) % Z, z_dn
        block = ring[it][t].at[origin, pl.ds(part * PIECE, PIECE)]
        slot = ring_slot(step, way, t, part)
        return pltpu.make_async_remote_copy(
            src_ref=block, dst_ref=block, send_sem=zs.at[it, slot], recv_sem=zr.at[it, slot],
            device_id={"space": target}, device_id_type=MESH)

    def ring_arrival(it, step, way, t, part):
        if way == 0:
            origin, target = (z + Z - step) % Z, z_up
        else:
            origin, target = (z + step) % Z, z_dn
        block = ring[it][t].at[origin, pl.ds(part * PIECE, PIECE)]
        slot = ring_slot(step, way, t, part)
        return pltpu.make_async_remote_copy(
            src_ref=block, dst_ref=block, send_sem=zs.at[it, slot], recv_sem=zr.at[it, slot],
            device_id={"space": target}, device_id_type=MESH)

    def column_copy(kind, hop, t):
        origin, target = ((q, mate), (q, cross), ((q + 2) % Q, mate))[hop]
        block = cols[kind][t].at[origin]
        slot = hop * 2 + t
        return pltpu.make_async_remote_copy(
            src_ref=block, dst_ref=block, send_sem=cs.at[kind, slot], recv_sem=cr.at[kind, slot],
            device_id={"space": target}, device_id_type=MESH)

    def column_arrival(kind, hop, t):
        mate_q = q + 1 - 2 * (q % 2)
        origin, target = ((mate_q, mate), ((q + 2) % Q, cross), ((mate_q + 2) % Q, mate))[hop]
        block = cols[kind][t].at[origin]
        slot = hop * 2 + t
        return pltpu.make_async_remote_copy(
            src_ref=block, dst_ref=block, send_sem=cs.at[kind, slot], recv_sem=cr.at[kind, slot],
            device_id={"space": target}, device_id_type=MESH)

    def pack_copy(it, way):
        target = (after, before)[way]
        return pltpu.make_async_remote_copy(
            src_ref=packs.at[it, way], dst_ref=packed.at[it, way], send_sem=ps.at[it, way], recv_sem=pr.at[it, way],
            device_id={"space": target}, device_id_type=MESH)

    def build_matrix():
        row = lax.broadcasted_iota(jnp.int32, (NODES, LANES), 0)
        lane = lax.broadcasted_iota(jnp.int32, (NODES, LANES), 1)
        first = lane < NODES
        on = row == jnp.bitwise_and(lane, NODES - 1)
        one, zero = jnp.float32(1.0), jnp.float32(0.0)
        lower = jnp.where(on & (row < 16), one, zero)
        upper = jnp.where(on & (row >= 48), one, zero)
        slide = jnp.where(on & (jnp.bitwise_and(row, 3) == 3), one, zero)
        scale = jnp.float32(0.5 * lift_scale)
        side[0] = jnp.concatenate([vol_ref[0], vol_ref[0]], axis=1) + scale * (lower - upper)
        side[1] = jnp.concatenate([vol_ref[1], vol_ref[1]], axis=1) - scale * slide
        side[2] = (scale * jnp.float32(dissipation)) * (lower + upper + slide)

        def row_block(v, carry):
            for j in range(VARS // 2):
                tile = jnp.zeros((NODES, LANES), jnp.float32)
                for d in range(2):
                    factor = jnp.where(first, flux_ref[v, d, 2 * j], flux_ref[v, d, 2 * j + 1])
                    tile = tile + factor * side[d]
                own = jnp.where(first, jnp.where(v == 2 * j, one, zero), jnp.where(v == 2 * j + 1, one, zero))
                tile = tile + own * side[2]
                high = tile.astype(jnp.bfloat16)
                where = (pl.ds(pl.multiple_of(v * NODES, NODES), NODES), pl.ds(j * LANES, LANES))
                a_hi[where] = high
                a_lo[where] = (tile - high.astype(jnp.float32)).astype(jnp.bfloat16)
            return carry

        lax.fori_loop(0, VARS, row_block, 0)

    def volume_part(it):
        u = jnp.concatenate(
            [ub[it, 0].reshape(VARS * NODES, LANES), ub[it, 1].reshape(VARS * NODES, LANES)], axis=1)
        high = u.astype(jnp.bfloat16)
        low = (u - high.astype(jnp.float32)).astype(jnp.bfloat16)
        for part in range(2):
            rows = pl.ds(part * 320, 320)
            out = jnp.dot(a_hi[rows, :], high, preferred_element_type=jnp.float32)
            out = out + jnp.dot(a_hi[rows, :], low, preferred_element_type=jnp.float32)
            out = out + jnp.dot(a_lo[rows, :], high, preferred_element_type=jnp.float32)
            for t in range(2):
                res_ref[t, pl.ds(part * 5, 5)] = out[:, t * LANES:(t + 1) * LANES].reshape(5, NODES, LANES)

    def ring_chunks(step, t):
        ways = (0, 1) if step < 4 else (t,)
        return [(way, part) for part in range(PARTS) for way in ways]

    def ring_start(it, t):
        for way, part in ring_chunks(1, t):
            ring_copy(it, 1, way, t, part).start()

    def ring_relay(it, step, t):
        onward = ring_chunks(step + 1, t) if step < 4 else []
        for way, part in ring_chunks(step, t):
            ring_arrival(it, step, way, t, part).wait_recv()
            if (way, part) in onward:
                ring_copy(it, step + 1, way, t, part).start()

    def pack_traces(it):
        up_pack = jnp.zeros((16, LANES), jnp.float32)
        lo_pack = jnp.zeros((16, LANES), jnp.float32)
        for i in range(2 * VARS):
            mine = (lane16 >= REACH * i) & (lane16 < REACH * (i + 1))
            u_face = ub[it, i // VARS, i % VARS, pl.ds(48, 16), :]
            l_face = ub[it, i // VARS, i % VARS, pl.ds(0, 16), :]
            up_pack = jnp.where(mine, pltpu.roll(u_face, (REACH * i + REACH) % LANES, 1), up_pack)
            lo_pack = jnp.where(mine, pltpu.roll(l_face, REACH * i, 1) if i else l_face, lo_pack)
        packs[it // 2, 0] = up_pack
        packs[it // 2, 1] = lo_pack
        for way in range(2):
            pack_copy(it // 2, way).start()

    scale = jnp.float32(0.5 * lift_scale)
    loss = jnp.float32(0.5 * lift_scale * dissipation)

    def first_direction(it):
        for way in range(2):
            pack_copy(it // 2, way).wait_recv()
        from_before = packed[it // 2, 0]
        from_after = packed[it // 2, 1]
        behind = lane16 - back_gap
        ahead = lane16 + ahead_gap
        for i in range(2 * VARS):
            u_face = ub[it, i // VARS, i % VARS, pl.ds(48, 16), :]
            l_face = ub[it, i // VARS, i % VARS, pl.ds(0, 16), :]
            own = jnp.take_along_axis(u_face, jnp.bitwise_and(behind, LANES - 1), axis=1)
            far = jnp.take_along_axis(from_before, jnp.bitwise_and(behind + REACH * (i + 1), LANES - 1), axis=1)
            lo_b[i // VARS, i % VARS] = jnp.where(behind < 0, far, own)
            own = jnp.take_along_axis(l_face, jnp.bitwise_and(ahead, LANES - 1), axis=1)
            far = jnp.take_along_axis(from_after, jnp.bitwise_and(ahead + REACH * i, LANES - 1), axis=1)
            up_b[i // VARS, i % VARS] = jnp.where(ahead >= LANES, far, own)

        def first_faces(v, c):
            low = -loss * lo_b[:, v]
            upp = -loss * up_b[:, v]
            for w in range(VARS):
                f = scale * flux_ref[v, 0, w]
                low = low - f * lo_b[:, w]
                upp = upp + f * up_b[:, w]
            res_ref[:, v, pl.ds(0, 16), :] += low
            res_ref[:, v, pl.ds(48, 16), :] += upp
            return c

        lax.fori_loop(0, VARS, first_faces, 0)

    half = SAMPLE_COUNT // 2

    def spectral(source, first, second, i):
        x = [source[(side_x + r // 2) % TM, r % 2, i] for r in range(SAMPLE_COUNT)]
        for r in (0, 1, 4, 5):
            near = opposite = None
            for m in range(1, half):
                diff = x[(r + m) % SAMPLE_COUNT] - x[(r - m) % SAMPLE_COUNT]
                one, two = jnp.float32(weights[m - 1]) * diff, jnp.float32(-weights[half - m - 1]) * diff
                near = one if near is None else near + one
                opposite = two if opposite is None else opposite + two
            first[r // 4, r % 2, i] = near
            first[r // 4 + 2, r % 2, i] = opposite
            if second is None:
                continue
            zero, eight = jnp.float32(squares[0]), jnp.float32(squares[half])
            near = zero * x[r] + eight * x[r + half]
            opposite = eight * x[r] + zero * x[r + half]
            for m in range(1, half):
                both = x[(r + m) % SAMPLE_COUNT] + x[(r - m) % SAMPLE_COUNT]
                near = near + jnp.float32(squares[m]) * both
                opposite = opposite + jnp.float32(squares[half - m]) * both
            second[r // 4, r % 2, i] = near
            second[r // 4 + 2, r % 2, i] = opposite

    def derive_state(i, c):
        spectral(gat, dt, dt2, i)
        return c

    def derive_term(i, c):
        spectral(sig_gat, sig_dt, None, i)
        return c

    def rows(c):
        return pl.ds(c, 16, stride=4)

    def tiles_of(buffer, t, v, c):
        places = [slide_place(v, h) if c == 3 else other_place(v, c, h) for h in range(2)]
        return jnp.concatenate([buffer[t, j, i] for j, i in places], axis=0)

    def term_tiles(t, v):
        return jnp.concatenate([sig_tem[t, 2 * v], sig_tem[t, 2 * v + 1]], axis=0)

    def offset_of(kind, t):
        group, shift = group_ref[t], shift_ref[t]
        if kind == 1:
            group = jnp.bitwise_and(2 * group + lax.shift_right_arithmetic(shift, 6), SP - 1)
            shift = jnp.bitwise_and(2 * shift, LANES - 1)
        return group, shift

    lane_b = lax.broadcasted_iota(jnp.int32, (VARS, 16, LANES), 2)

    def column_start(kind, t):
        it = kind // 2
        group, shift = offset_of(kind, t)
        first_dst = jnp.bitwise_and(q - group, Q - 1)
        second_dst = jnp.bitwise_and(q - group - 1, Q - 1)
        first = jnp.bitwise_and(z + lax.shift_right_arithmetic(first_dst + group - q, 2), Z - 1)
        second = jnp.bitwise_and(z + lax.shift_right_arithmetic(second_dst + group + 1 - q, 2), Z - 1)
        cols[kind][t][q] = jnp.where(lane_b >= shift, ring[it][t][first], ring[it][t][second])
        column_copy(kind, 1, t).start()
        column_copy(kind, 0, t).start()

    def column_relay(kind, t):
        column_arrival(kind, 1, t).wait_recv()
        column_copy(kind, 2, t).start()

    def column_finish(kind, t):
        column_arrival(kind, 0, t).wait_recv()
        column_arrival(kind, 2, t).wait_recv()
        group, shift = offset_of(kind, t)
        first = cols[kind][t][jnp.bitwise_and(q + group, Q - 1)]
        second = cols[kind][t][jnp.bitwise_and(q + group + 1, Q - 1)]
        both = jnp.where(lane_b >= shift, first, second)
        both = pltpu.roll(both.reshape(VARS * 16, LANES), jnp.bitwise_and(LANES - shift, LANES - 1), 1)
        return both.reshape(VARS, 16, LANES)

    def turn(t):
        cosine, sine = pick(2 * tm + t, cosines), pick(2 * tm + t, sines)
        one, two = sl_b[t, 1], sl_b[t, 2]
        sl_b[t, 1] = cosine * one - sine * two
        sl_b[t, 2] = sine * one + cosine * two

    def slide_term(t, v):
        term = -loss * sl_b[t, v]
        for w in range(VARS):
            term = term + (scale * flux_ref[v, 1, w]) * sl_b[t, w]
        return term

    step_size = jnp.float32(pseudo_step)
    scope = jax.named_scope

    with scope("start0"):
        for t in range(2):
            for v in range(VARS):
                points = ub[0, t, v, rows(3), :]
                ring[0][t][z, v] = points
                for h in range(2):
                    j, i = slide_place(v, h)
                    up[t, j, i] = points[8 * h:8 * h + 8]
            ring_start(0, t)
        out_all(out_copy, 0, "start")
        pack_traces(0)
        for t in range(2):
            for v in range(VARS):
                for c in range(3):
                    points = ub[0, t, v, rows(c), :]
                    for h in range(2):
                        j, i = other_place(v, c, h)
                        up[t, j, i] = points[8 * h:8 * h + 8]
        gat[tm] = up[:, y]
        for kind in (1, 2):
            out_all(out_copy, kind, "start")
            pass_on(kind, 7, 0).start()
    with scope("matrix"):
        build_matrix()
    with scope("volume0"):
        volume_part(0)
    with scope("ring0_1"):
        ring_relay(0, 1, 0)
        ring_relay(0, 1, 1)
    with scope("ring0_2a"):
        ring_relay(0, 2, 0)
    with scope("out_slide"):
        out_all(out_arrival, 0, "wait_recv")
    with scope("derive_slide"):
        lax.fori_loop(0, 5, derive_state, 0)
        back_all(back_copy, 0, "start")
        back_all(back_copy, 4, "start")
        tem[:, y, pl.ds(0, 5)] = dt[y, :, pl.ds(0, 5)]
    with scope("points1"):
        relay_points(1)
    with scope("ring0_2b"):
        ring_relay(0, 2, 1)
    with scope("first0"):
        first_direction(0)
    with scope("ring0_3"):
        ring_relay(0, 3, 0)
    with scope("points2"):
        relay_points(2)
    with scope("ring0_3b"):
        ring_relay(0, 3, 1)
    with scope("back_slide"):
        back_all(back_arrival, 0, "wait_recv")
    with scope("w"):
        for t in range(2):
            for v in range(VARS):
                rest = res_ref[t, v, rows(3), :] + tiles_of(tem, t, v, 3)
                ring[1][t][z, v] = ub[0, t, v, rows(3), :] - step_size * rest
            ring_start(1, t)
    with scope("ring0_4"):
        for t in range(2):
            ring_relay(0, 4, t)
            column_start(0, t)
    with scope("cols1_start"):
        for t in range(2):
            column_start(1, t)
    with scope("rest1"):
        wait_points(1)
        lax.fori_loop(5, 10, derive_state, 0)
        back_all(back_copy, 1, "start")
        back_all(back_copy, 5, "start")
        tem[:, y, pl.ds(5, 5)] = dt[y, :, pl.ds(5, 5)]
    with scope("ring1_1a"):
        ring_relay(1, 1, 0)
    with scope("rest2"):
        wait_points(2)
        lax.fori_loop(10, 20, derive_state, 0)
        back_all(back_copy, 2, "start")
        back_all(back_copy, 6, "start")
        tem[:, y, pl.ds(10, 10)] = dt[y, :, pl.ds(10, 10)]
        tem2[:, y] = dt2[y]
    with scope("ring1_1b"):
        ring_relay(1, 1, 1)
    with scope("ring1_2a"):
        ring_relay(1, 2, 0)
    with scope("cols0_relay"):
        for t in range(2):
            column_relay(0, t)
    with scope("ring1_2b"):
        ring_relay(1, 2, 1)
    with scope("cols0_finish"):
        for t in range(2):
            sl_b[t] = column_finish(0, t)
            turn(t)

    def sliding_term(v, c):
        for t in range(2):
            term = slide_term(t, v)
            sig[t, 2 * v] = term[0:8]
            sig[t, 2 * v + 1] = term[8:16]
        return c

    with scope("sigma"):
        lax.fori_loop(0, VARS, sliding_term, 0)
        out_all(out_copy, 3, "start")
        sig_gat[tm] = sig[:, pl.ds(5 * y, 5)]
    with scope("ring1_3a"):
        ring_relay(1, 3, 0)
    with scope("cols1_relay"):
        for t in range(2):
            column_relay(1, t)
    with scope("back_rest"):
        back_all(back_arrival, 1, "wait_recv")
        back_all(back_arrival, 2, "wait_recv")
    with scope("u1"):
        for t in range(2):
            for v in range(VARS):
                for c in range(4):
                    late = tiles_of(tem, t, v, c)
                    rest = res_ref[t, v, rows(c), :] + late
                    if c == 3:
                        rest = rest + jnp.concatenate([sig[t, 2 * v], sig[t, 2 * v + 1]], axis=0)
                    state = ub[0, t, v, rows(c), :] - step_size * rest
                    ub[1, t, v, rows(c), :] = state
                    ub[2, t, v, rows(c), :] = state - step_size * late
        pack_traces(2)
    with scope("ring1_3b"):
        ring_relay(1, 3, 1)
    with scope("volume1"):
        volume_part(2)
    with scope("ring1_4"):
        for t in range(2):
            ring_relay(1, 4, t)
            column_start(2, t)
    with scope("out_term"):
        out_all(out_arrival, 3, "wait_recv")
    with scope("derive_term"):
        lax.fori_loop(0, 5, derive_term, 0)
        back_all(back_copy, 3, "start")
        sig_tem[:, pl.ds(5 * y, 5)] = sig_dt[y]
    with scope("cols1_finish"):
        for t in range(2):
            sl_b[t] = column_finish(1, t)
            turn(t)

        def twice(v, c):
            for t in range(2):
                tw_b[t, v] = step_size * slide_term(t, v)
            return c

        lax.fori_loop(0, VARS, twice, 0)
    with scope("first1"):
        first_direction(2)
    with scope("sends_early"):
        for kind in range(3):
            out_all(out_copy, kind, "wait_send")
        for kind in (0, 1, 2, 4, 5):
            back_all(back_copy, kind, "wait_send")
        for kind in (1, 2):
            for k in range(4, 8):
                pass_on(kind, k, 0).wait_send()
        for kind in range(2):
            for hop in range(3):
                for t in range(2):
                    column_copy(kind, hop, t).wait_send()
        for it in range(ITERS):
            for step in range(1, 5 - it):
                for t in range(2):
                    for way, part in ring_chunks(step, t):
                        ring_copy(it, step, way, t, part).wait_send()
            for way in range(2):
                pack_copy(it, way).wait_send()
    with scope("cols2_relay"):
        for t in range(2):
            column_relay(2, t)
    with scope("back_late"):
        for kind in (4, 5, 6, 3):
            back_all(back_arrival, kind, "wait_recv")
    with scope("without_slide"):
        for t in range(2):
            for v in range(VARS):
                for c in range(4):
                    late = tiles_of(tem2, t, v, c)
                    if c == 3:
                        late = late + term_tiles(t, v)
                    total = res_ref[t, v, rows(c), :] + (tiles_of(tem, t, v, c) - step_size * late)
                    res_ref[t, v, rows(c), :] = total
                    if c < 3:
                        new_ref[t, v, rows(c), :] = ub[1, t, v, rows(c), :] - step_size * total
    with scope("cols2_finish"):
        for t in range(2):
            sl_b[t] = column_finish(2, t) - tw_b[t]
            turn(t)

    def finish(v, c):
        for t in range(2):
            total = res_ref[t, v, rows(3), :] + slide_term(t, v)
            res_ref[t, v, rows(3), :] = total
            new_ref[t, v, rows(3), :] = ub[1, t, v, rows(3), :] - step_size * total
        return c

    with scope("finish"):
        lax.fori_loop(0, VARS, finish, 0)
    with scope("sends"):
        out_all(out_copy, 3, "wait_send")
        for kind in (3, 6):
            back_all(back_copy, kind, "wait_send")
        for t in range(2):
            for hop in range(3):
                column_copy(2, hop, t).wait_send()
            for way, part in ring_chunks(4, t):
                ring_copy(1, 4, way, t, part).wait_send()


def per_device(conserved_field, face_neighbours, counterpart_group, counterpart_shift, volume_operator, flux_matrix):
    state = jax.ShapeDtypeStruct(conserved_field.shape, jnp.float32)
    vmem = pl.BlockSpec(memory_space=pltpu.VMEM)
    f32, bf16 = jnp.float32, jnp.bfloat16
    dma = pltpu.SemaphoreType.DMA
    return pl.pallas_call(
        kernel,
        out_shape=(state, state),
        in_specs=[pl.BlockSpec(memory_space=pltpu.HBM)] * 6,
        out_specs=(vmem, vmem),
        scratch_shapes=[
            pltpu.VMEM((2, LANES), jnp.int32),
            pltpu.SMEM((2,), jnp.int32),
            pltpu.SMEM((2,), jnp.int32),
            pltpu.VMEM((2, NODES, NODES), f32),
            pltpu.SMEM((VARS, 2, VARS), f32),
            pltpu.VMEM((3, 2, VARS, NODES, LANES), f32),
            pltpu.VMEM((VARS * NODES, VARS * NODES), bf16),
            pltpu.VMEM((VARS * NODES, VARS * NODES), bf16),
            pltpu.VMEM((2, 4, 20, 8, LANES), f32),
            pltpu.VMEM((TM, 2, 20, 8, LANES), f32),
            pltpu.VMEM((4, 2, 20, 8, LANES), f32),
            pltpu.VMEM((4, 2, 20, 8, LANES), f32),
            pltpu.VMEM((2, 4, 20, 8, LANES), f32),
            pltpu.VMEM((2, 4, 20, 8, LANES), f32),
            pltpu.VMEM((2, 20, 8, LANES), f32),
            pltpu.VMEM((TM, 2, 5, 8, LANES), f32),
            pltpu.VMEM((4, 2, 5, 8, LANES), f32),
            pltpu.VMEM((2, 20, 8, LANES), f32),
            *[pltpu.VMEM((Z, VARS, 16, LANES), f32)] * 4,
            *[pltpu.VMEM((Q, VARS, 16, LANES), f32)] * 6,
            pltpu.VMEM((ITERS, 2, 16, LANES), f32),
            pltpu.VMEM((ITERS, 2, 16, LANES), f32),
            pltpu.VMEM((3, NODES, LANES), f32),
            pltpu.VMEM((2, VARS, 16, LANES), f32),
            pltpu.VMEM((2, VARS, 16, LANES), f32),
            pltpu.VMEM((2, VARS, 16, LANES), f32),
            pltpu.VMEM((2, VARS, 16, LANES), f32),
            dma((6,)),
            dma((4, 7)), dma((4, 7)),
            dma((7, 3)), dma((7, 3)),
            dma((ITERS, 16 * PARTS)), dma((ITERS, 16 * PARTS)),
            dma((3, 6)), dma((3, 6)),
            dma((ITERS, 2)), dma((ITERS, 2)),
            dma((8,)), dma((8,)),
        ],
        compiler_params=pltpu.CompilerParams(
            collective_id=0, has_side_effects=True, vmem_limit_bytes=63 * 1024 * 1024),
        name="iterations",
    )(conserved_field, face_neighbours, counterpart_group, counterpart_shift, volume_operator,
      jnp.transpose(flux_matrix, (1, 0, 2)))


def solution(mesh):
    return jax.shard_map(
        per_device,
        mesh=mesh,
        in_specs=(P("tm", None, None, "space"), P(None, "space"), P("tm"), P("tm"), P(), P()),
        out_specs=(P("tm", None, None, "space"), P("tm", None, None, "space")),
        check_vma=False,
    )
```

```python
import math

import jax
import jax.numpy as jnp
from jax import lax
from jax.experimental import pallas as pl
from jax.experimental.pallas import tpu as pltpu
from jax.sharding import PartitionSpec as P

SAMPLE_COUNT = 16
REACH = 4
ITERS = 2
VARS = 10
NODES = 64
LANES = 128
PARTS = 5
PIECE = VARS // PARTS

lift_scale = 2.0
dissipation = 1.5
angular_speed = 0.5
damping_factor = 4.0
pseudo_step = 0.2

MESH = pl.DeviceIdType.MESH
MOVES = ((2, 1), (1, 1), (3, 1), (0, 1), (2, 0), (1, 0), (3, 0))
TM = 8
SP = 32
Z = 8
Q = 4


def spectral_weights():
    half = SAMPLE_COUNT // 2
    weights = []
    for m in range(1, half):
        total = 0.0
        for k in range(1, half):
            gain = 2.0 * angular_speed * k * math.exp(-damping_factor * (k / half) ** 8) / SAMPLE_COUNT
            total += gain * math.sin(2.0 * math.pi * k * m / SAMPLE_COUNT)
        weights.append(total)
    return weights


def spectral_squares():
    first = [0.0] + spectral_weights() + [0.0]
    full = first + [-first[SAMPLE_COUNT - m] for m in range(SAMPLE_COUNT // 2 + 1, SAMPLE_COUNT)]
    return [
        sum(full[j] * full[(m - j) % SAMPLE_COUNT] for j in range(SAMPLE_COUNT))
        for m in range(SAMPLE_COUNT // 2 + 1)
    ]


def slide_place(v, h):
    index = 2 * v + h
    return index // 5, index % 5


def other_place(v, c, h):
    index = 6 * v + 2 * c + h
    return index // 15, 5 + index % 15


def pick(index, values):
    out = jnp.float32(values[0])
    for k in range(1, len(values)):
        out = jnp.where(index == k, jnp.float32(values[k]), out)
    return out


def kernel(
    u_hbm, fn_hbm, group_hbm, shift_hbm, vol_hbm, flux_hbm,
    new_ref, res_ref, fn_ref, group_ref, shift_ref, vol_ref, flux_ref,
    ub, a_hi, a_lo, up, gat, dt, dt2, tem, tem2, sig, sig_gat, sig_dt, sig_tem, ring_00, ring_01, ring_10, ring_11, cols_00, cols_01, cols_10, cols_11, cols_20, cols_21,
    packs, packed, side, lo_b, up_b, sl_b, tw_b, in_sem, fs, fr, bs, br, zs, zr, cs, cr, ps, pr, xs, xr,
):
    ring = ((ring_00, ring_01), (ring_10, ring_11))
    cols = ((cols_00, cols_01), (cols_10, cols_11), (cols_20, cols_21))
    tm = lax.axis_index("tm")
    sp = lax.axis_index("space")
    z = sp // Q
    q = sp % Q
    y = tm // 2
    side_x = tm % 2

    def space_of(zz, qq):
        return zz * Q + qq

    z_up = space_of((z + 1) % Z, q)
    z_dn = space_of((z + Z - 1) % Z, q)
    mate = space_of(z, q + 1 - 2 * (q % 2))
    cross = space_of(z, (q + 2) % Q)
    after = (sp + 1) % SP
    before = (sp + SP - 1) % SP

    loads = [
        pltpu.make_async_copy(source, target, in_sem.at[k])
        for k, (source, target) in enumerate((
            (u_hbm, ub.at[0]), (flux_hbm, flux_ref), (vol_hbm, vol_ref),
            (fn_hbm, fn_ref), (group_hbm, group_ref), (shift_hbm, shift_ref)))
    ]
    for load in loads:
        load.start()

    barrier = pltpu.get_barrier_semaphore()
    for k in range(1, TM):
        pl.semaphore_signal(barrier, inc=1, device_id={"tm": (tm + k) % TM}, device_id_type=MESH)
    for other in (z_up, z_dn, mate, cross, after, before):
        pl.semaphore_signal(barrier, inc=1, device_id={"space": other}, device_id_type=MESH)
    with jax.named_scope("entry"):
        for load in loads:
            load.wait()
        pl.semaphore_wait(barrier, TM - 1 + 6)

    lane16 = lax.broadcasted_iota(jnp.int32, (16, LANES), 1)
    gidx = sp * LANES + lane16
    back_gap = jnp.bitwise_and(gidx - fn_ref[0:1, :], SP * LANES - 1)
    ahead_gap = jnp.bitwise_and(fn_ref[1:2, :] - gidx, SP * LANES - 1)

    weights = spectral_weights()
    squares = spectral_squares()
    cosines = [math.cos(2.0 * math.pi * k / SAMPLE_COUNT) for k in range(SAMPLE_COUNT)]
    sines = [math.sin(2.0 * math.pi * k / SAMPLE_COUNT) for k in range(SAMPLE_COUNT)]

    OUT = ((0, 5), (5, 5), (10, 10))
    BACK = ((0, 5), (5, 5), (10, 10), None, (0, 5), (5, 5), (10, 10))

    OUT_SEM = (0, 1, 4, 7)

    def settle(view, send=None, receive=None):
        copy = pltpu.make_async_remote_copy(
            src_ref=view, dst_ref=view, send_sem=bs.at[0] if send is None else send,
            recv_sem=br.at[0] if receive is None else receive, device_id={"tm": (tm + 1) % TM}, device_id_type=MESH)
        if send is None:
            copy.wait_recv()
        else:
            copy.wait_send()

    def out_view(kind, count):
        if kind == 3:
            return sig_gat.at[pl.ds(0, count)]
        return gat.at[pl.ds(0, count), :, pl.ds(*OUT[kind])]

    def back_view(kind):
        if kind == 3:
            return sig_tem.at[:, pl.ds(0, 15)]
        return (tem2 if kind > 3 else tem).at[:, pl.ds(0, 3), pl.ds(*BACK[kind])]

    def peer_at(k, sign):
        dy, dx = MOVES[k]
        row = (y + sign * dy + 4) % 4
        return row, row * 2 + (side_x + dx) % 2

    def out_refs(kind, row, place):
        if kind == 3:
            return sig.at[:, pl.ds(5 * row, 5)], sig_gat.at[place]
        tiles = pl.ds(*OUT[kind])
        return up.at[:, row, tiles], gat.at[place, :, tiles]

    def back_refs(kind, row, place):
        if kind == 3:
            return sig_dt.at[row], sig_tem.at[:, pl.ds(5 * place, 5)]
        tiles = pl.ds(*BACK[kind])
        source, target = (dt2, tem2) if kind > 3 else (dt, tem)
        return source.at[row, :, tiles], target.at[:, place, tiles]

    def out_copy(kind, k):
        row, peer = peer_at(k, 1)
        source, target = out_refs(kind, row, tm)
        return pltpu.make_async_remote_copy(
            src_ref=source, dst_ref=target, send_sem=fs.at[kind], recv_sem=fr.at[OUT_SEM[kind] + (k - 4 if kind in (1, 2) else 0)],
            device_id={"tm": peer}, device_id_type=MESH)

    def out_arrival(kind, k):
        row, peer = peer_at(k, -1)
        source, target = out_refs(kind, row, peer)
        return pltpu.make_async_remote_copy(
            src_ref=source, dst_ref=target, send_sem=fs.at[kind], recv_sem=fr.at[OUT_SEM[kind] + (k - 4 if kind in (1, 2) else 0)],
            device_id={"tm": peer}, device_id_type=MESH)

    def back_copy(kind, k):
        row, peer = peer_at(k, 1)
        source, target = back_refs(kind, row, y)
        return pltpu.make_async_remote_copy(
            src_ref=source, dst_ref=target, send_sem=bs.at[kind], recv_sem=br.at[kind],
            device_id={"tm": peer}, device_id_type=MESH)

    def out_start(kind):
        for k in range(7) if kind in (0, 3) else range(4, 7):
            out_copy(kind, k).start()

    def pass_on(kind, k, side):
        row = (y if k == 7 else peer_at(k, -1)[0])
        place = row * 2 + (side_x if side == 0 else 1 - side_x)
        block = gat.at[place, :, pl.ds(*OUT[kind])]
        return pltpu.make_async_remote_copy(
            src_ref=block, dst_ref=block, send_sem=xs.at[kind - 1], recv_sem=xr.at[kind - 1],
            device_id={"tm": y * 2 + 1 - side_x}, device_id_type=MESH)

    def relay_points(kind):
        for k in (5, 6, 4):
            out_arrival(kind, k).wait_recv()
            pass_on(kind, k, 0).start()

    def wait_points(kind):
        settle(out_view(kind, 4), receive=xr.at[kind - 1])

    def back_start(kind):
        for k in range(4, 7):
            back_copy(kind, k).start()

    def ring_slot(step, way, t, part):
        return (((step - 1) * 2 + way) * 2 + t) * PARTS + part

    def ring_copy(it, step, way, t, part):
        if way == 0:
            origin, target = (z + Z - (step - 1)) % Z, z_up
        else:
            origin, target = (z + step - 1) % Z, z_dn
        block = ring[it][t].at[origin, pl.ds(part * PIECE, PIECE)]
        slot = ring_slot(step, way, t, part)
        return pltpu.make_async_remote_copy(
            src_ref=block, dst_ref=block, send_sem=zs.at[it * 2 + t], recv_sem=zr.at[slot],
            device_id={"space": target}, device_id_type=MESH)

    def ring_arrival(it, step, way, t, part):
        if way == 0:
            origin, target = (z + Z - step) % Z, z_up
        else:
            origin, target = (z + step) % Z, z_dn
        block = ring[it][t].at[origin, pl.ds(part * PIECE, PIECE)]
        slot = ring_slot(step, way, t, part)
        return pltpu.make_async_remote_copy(
            src_ref=block, dst_ref=block, send_sem=zs.at[it * 2 + t], recv_sem=zr.at[slot],
            device_id={"space": target}, device_id_type=MESH)

    def column_copy(kind, hop, t):
        origin, target = ((q, mate), (q, cross), ((q + 2) % Q, mate))[hop]
        block = cols[kind][t].at[origin]
        return pltpu.make_async_remote_copy(
            src_ref=block, dst_ref=block, send_sem=cs.at[kind], recv_sem=cr.at[kind * 4 + (2 if hop == 1 else 0) + t],
            device_id={"space": target}, device_id_type=MESH)

    def column_arrival(kind, hop, t):
        mate_q = q + 1 - 2 * (q % 2)
        origin, target = ((mate_q, mate), ((q + 2) % Q, cross), ((mate_q + 2) % Q, mate))[hop]
        block = cols[kind][t].at[origin]
        return pltpu.make_async_remote_copy(
            src_ref=block, dst_ref=block, send_sem=cs.at[kind], recv_sem=cr.at[kind * 4 + (2 if hop == 1 else 0) + t],
            device_id={"space": target}, device_id_type=MESH)

    def pack_copy(it, way):
        target = (after, before)[way]
        return pltpu.make_async_remote_copy(
            src_ref=packs.at[it, way], dst_ref=packed.at[it, way], send_sem=ps.at[it], recv_sem=pr.at[it],
            device_id={"space": target}, device_id_type=MESH)

    def build_matrix():
        row = lax.broadcasted_iota(jnp.int32, (NODES, LANES), 0)
        lane = lax.broadcasted_iota(jnp.int32, (NODES, LANES), 1)
        first = lane < NODES
        on = row == jnp.bitwise_and(lane, NODES - 1)
        one, zero = jnp.float32(1.0), jnp.float32(0.0)
        lower = jnp.where(on & (row < 16), one, zero)
        upper = jnp.where(on & (row >= 48), one, zero)
        slide = jnp.where(on & (jnp.bitwise_and(row, 3) == 3), one, zero)
        scale = jnp.float32(0.5 * lift_scale)
        side[0] = jnp.concatenate([vol_ref[0], vol_ref[0]], axis=1) + scale * (lower - upper)
        side[1] = jnp.concatenate([vol_ref[1], vol_ref[1]], axis=1) - scale * slide
        side[2] = (scale * jnp.float32(dissipation)) * (lower + upper + slide)

        def row_block(v, carry):
            for j in range(VARS // 2):
                tile = jnp.zeros((NODES, LANES), jnp.float32)
                for d in range(2):
                    factor = jnp.where(first, flux_ref[v, d, 2 * j], flux_ref[v, d, 2 * j + 1])
                    tile = tile + factor * side[d]
                own = jnp.where(first, jnp.where(v == 2 * j, one, zero), jnp.where(v == 2 * j + 1, one, zero))
                tile = tile + own * side[2]
                high = tile.astype(jnp.bfloat16)
                where = (pl.ds(pl.multiple_of(v * NODES, NODES), NODES), pl.ds(j * LANES, LANES))
                a_hi[where] = high
                a_lo[where] = (tile - high.astype(jnp.float32)).astype(jnp.bfloat16)
            return carry

        lax.fori_loop(0, VARS, row_block, 0)

    def volume_part(it):
        u = jnp.concatenate(
            [ub[it, 0].reshape(VARS * NODES, LANES), ub[it, 1].reshape(VARS * NODES, LANES)], axis=1)
        high = u.astype(jnp.bfloat16)
        low = (u - high.astype(jnp.float32)).astype(jnp.bfloat16)
        for part in range(2):
            rows = pl.ds(part * 320, 320)
            out = jnp.dot(a_hi[rows, :], high, preferred_element_type=jnp.float32)
            out = out + jnp.dot(a_hi[rows, :], low, preferred_element_type=jnp.float32)
            out = out + jnp.dot(a_lo[rows, :], high, preferred_element_type=jnp.float32)
            for t in range(2):
                res_ref[t, pl.ds(part * 5, 5)] = out[:, t * LANES:(t + 1) * LANES].reshape(5, NODES, LANES)

    def ring_chunks(step, t):
        ways = (0, 1) if step < 4 else (t,)
        return [(way, part) for part in range(PARTS) for way in ways]

    def ring_start(it, t):
        for way, part in ring_chunks(1, t):
            ring_copy(it, 1, way, t, part).start()

    def ring_relay(it, step, t):
        onward = ring_chunks(step + 1, t) if step < 4 else []
        for way, part in ring_chunks(step, t):
            ring_arrival(it, step, way, t, part).wait_recv()
            if (way, part) in onward:
                ring_copy(it, step + 1, way, t, part).start()

    def pack_traces(it):
        up_pack = jnp.zeros((16, LANES), jnp.float32)
        lo_pack = jnp.zeros((16, LANES), jnp.float32)
        for i in range(2 * VARS):
            mine = (lane16 >= REACH * i) & (lane16 < REACH * (i + 1))
            u_face = ub[it, i // VARS, i % VARS, pl.ds(48, 16), :]
            l_face = ub[it, i // VARS, i % VARS, pl.ds(0, 16), :]
            up_pack = jnp.where(mine, pltpu.roll(u_face, (REACH * i + REACH) % LANES, 1), up_pack)
            lo_pack = jnp.where(mine, pltpu.roll(l_face, REACH * i, 1) if i else l_face, lo_pack)
        packs[it // 2, 0] = up_pack
        packs[it // 2, 1] = lo_pack
        for way in range(2):
            pack_copy(it // 2, way).start()

    scale = jnp.float32(0.5 * lift_scale)
    loss = jnp.float32(0.5 * lift_scale * dissipation)

    def first_direction(it):
        settle(packed.at[it // 2], receive=pr.at[it // 2])
        from_before = packed[it // 2, 0]
        from_after = packed[it // 2, 1]
        behind = lane16 - back_gap
        ahead = lane16 + ahead_gap
        for i in range(2 * VARS):
            u_face = ub[it, i // VARS, i % VARS, pl.ds(48, 16), :]
            l_face = ub[it, i // VARS, i % VARS, pl.ds(0, 16), :]
            own = jnp.take_along_axis(u_face, jnp.bitwise_and(behind, LANES - 1), axis=1)
            far = jnp.take_along_axis(from_before, jnp.bitwise_and(behind + REACH * (i + 1), LANES - 1), axis=1)
            lo_b[i // VARS, i % VARS] = jnp.where(behind < 0, far, own)
            own = jnp.take_along_axis(l_face, jnp.bitwise_and(ahead, LANES - 1), axis=1)
            far = jnp.take_along_axis(from_after, jnp.bitwise_and(ahead + REACH * i, LANES - 1), axis=1)
            up_b[i // VARS, i % VARS] = jnp.where(ahead >= LANES, far, own)

        def first_faces(v, c):
            low = -loss * lo_b[:, v]
            upp = -loss * up_b[:, v]
            for w in range(VARS):
                f = scale * flux_ref[v, 0, w]
                low = low - f * lo_b[:, w]
                upp = upp + f * up_b[:, w]
            res_ref[:, v, pl.ds(0, 16), :] += low
            res_ref[:, v, pl.ds(48, 16), :] += upp
            return c

        lax.fori_loop(0, VARS, first_faces, 0)

    half = SAMPLE_COUNT // 2

    def spectral(source, first, second, i):
        x = [source[(side_x + r // 2) % TM, r % 2, i] for r in range(SAMPLE_COUNT)]
        for r in (0, 1, 4, 5):
            near = opposite = None
            for m in range(1, half):
                diff = x[(r + m) % SAMPLE_COUNT] - x[(r - m) % SAMPLE_COUNT]
                one, two = jnp.float32(weights[m - 1]) * diff, jnp.float32(-weights[half - m - 1]) * diff
                near = one if near is None else near + one
                opposite = two if opposite is None else opposite + two
            first[r // 4, r % 2, i] = near
            first[r // 4 + 2, r % 2, i] = opposite
            if second is None:
                continue
            zero, eight = jnp.float32(squares[0]), jnp.float32(squares[half])
            near = zero * x[r] + eight * x[r + half]
            opposite = eight * x[r] + zero * x[r + half]
            for m in range(1, half):
                both = x[(r + m) % SAMPLE_COUNT] + x[(r - m) % SAMPLE_COUNT]
                near = near + jnp.float32(squares[m]) * both
                opposite = opposite + jnp.float32(squares[half - m]) * both
            second[r // 4, r % 2, i] = near
            second[r // 4 + 2, r % 2, i] = opposite

    def derive_state(i, c):
        spectral(gat, dt, dt2, i)
        return c

    def derive_term(i, c):
        spectral(sig_gat, sig_dt, None, i)
        return c

    def rows(c):
        return pl.ds(c, 16, stride=4)

    def tiles_of(buffer, t, v, c):
        places = [slide_place(v, h) if c == 3 else other_place(v, c, h) for h in range(2)]
        return jnp.concatenate([buffer[t, j, i] for j, i in places], axis=0)

    def term_tiles(t, v):
        return jnp.concatenate([sig_tem[t, 2 * v], sig_tem[t, 2 * v + 1]], axis=0)

    def offset_of(kind, t):
        group, shift = group_ref[t], shift_ref[t]
        if kind == 1:
            group = jnp.bitwise_and(2 * group + lax.shift_right_arithmetic(shift, 6), SP - 1)
            shift = jnp.bitwise_and(2 * shift, LANES - 1)
        return group, shift

    lane_b = lax.broadcasted_iota(jnp.int32, (VARS, 16, LANES), 2)

    def column_start(kind, t):
        it = kind // 2
        group, shift = offset_of(kind, t)
        first_dst = jnp.bitwise_and(q - group, Q - 1)
        second_dst = jnp.bitwise_and(q - group - 1, Q - 1)
        first = jnp.bitwise_and(z + lax.shift_right_arithmetic(first_dst + group - q, 2), Z - 1)
        second = jnp.bitwise_and(z + lax.shift_right_arithmetic(second_dst + group + 1 - q, 2), Z - 1)
        cols[kind][t][q] = jnp.where(lane_b >= shift, ring[it][t][first], ring[it][t][second])
        column_copy(kind, 1, t).start()
        column_copy(kind, 0, t).start()

    def column_relay(kind, t):
        column_arrival(kind, 1, t).wait_recv()
        column_copy(kind, 2, t).start()

    def column_finish(kind, t):
        settle(cols[kind][t].at[pl.ds(0, 2)], receive=cr.at[kind * 4 + t])
        group, shift = offset_of(kind, t)
        first = cols[kind][t][jnp.bitwise_and(q + group, Q - 1)]
        second = cols[kind][t][jnp.bitwise_and(q + group + 1, Q - 1)]
        both = jnp.where(lane_b >= shift, first, second)
        both = pltpu.roll(both.reshape(VARS * 16, LANES), jnp.bitwise_and(LANES - shift, LANES - 1), 1)
        return both.reshape(VARS, 16, LANES)

    def turn(t):
        cosine, sine = pick(2 * tm + t, cosines), pick(2 * tm + t, sines)
        one, two = sl_b[t, 1], sl_b[t, 2]
        sl_b[t, 1] = cosine * one - sine * two
        sl_b[t, 2] = sine * one + cosine * two

    def slide_term(t, v):
        term = -loss * sl_b[t, v]
        for w in range(VARS):
            term = term + (scale * flux_ref[v, 1, w]) * sl_b[t, w]
        return term

    step_size = jnp.float32(pseudo_step)
    scope = jax.named_scope

    with scope("start0"):
        for t in range(2):
            for v in range(VARS):
                points = ub[0, t, v, rows(3), :]
                ring[0][t][z, v] = points
                for h in range(2):
                    j, i = slide_place(v, h)
                    up[t, j, i] = points[8 * h:8 * h + 8]
            ring_start(0, t)
        out_start(0)
        pack_traces(0)
        for t in range(2):
            for v in range(VARS):
                for c in range(3):
                    points = ub[0, t, v, rows(c), :]
                    for h in range(2):
                        j, i = other_place(v, c, h)
                        up[t, j, i] = points[8 * h:8 * h + 8]
        gat[tm] = up[:, y]
        for kind in (1, 2):
            out_start(kind)
            pass_on(kind, 7, 0).start()
    with scope("matrix"):
        build_matrix()
    with scope("volume0"):
        volume_part(0)
    with scope("ring0_1"):
        ring_relay(0, 1, 0)
        ring_relay(0, 1, 1)
    with scope("ring0_2a"):
        ring_relay(0, 2, 0)
    with scope("out_slide"):
        settle(out_view(0, 7), receive=fr.at[OUT_SEM[0]])
    with scope("derive_slide"):
        lax.fori_loop(0, 5, derive_state, 0)
        back_start(0)
        back_start(4)
        tem[:, y, pl.ds(0, 5)] = dt[y, :, pl.ds(0, 5)]
    with scope("points1"):
        relay_points(1)
    with scope("ring0_2b"):
        ring_relay(0, 2, 1)
    with scope("first0"):
        first_direction(0)
    with scope("ring0_3"):
        ring_relay(0, 3, 0)
    with scope("points2"):
        relay_points(2)
    with scope("ring0_3b"):
        ring_relay(0, 3, 1)
    with scope("back_slide"):
        settle(back_view(0), receive=br.at[0])
    with scope("w"):
        for t in range(2):
            for v in range(VARS):
                rest = res_ref[t, v, rows(3), :] + tiles_of(tem, t, v, 3)
                ring[1][t][z, v] = ub[0, t, v, rows(3), :] - step_size * rest
            ring_start(1, t)
    with scope("ring0_4"):
        for t in range(2):
            ring_relay(0, 4, t)
            column_start(0, t)
    with scope("cols1_start"):
        for t in range(2):
            column_start(1, t)
    with scope("rest1"):
        wait_points(1)
        lax.fori_loop(5, 10, derive_state, 0)
        back_start(1)
        back_start(5)
        tem[:, y, pl.ds(5, 5)] = dt[y, :, pl.ds(5, 5)]
    with scope("ring1_1a"):
        ring_relay(1, 1, 0)
    with scope("rest2"):
        wait_points(2)
        lax.fori_loop(10, 20, derive_state, 0)
        back_start(2)
        back_start(6)
        tem[:, y, pl.ds(10, 10)] = dt[y, :, pl.ds(10, 10)]
        tem2[:, y] = dt2[y]
    with scope("ring1_1b"):
        ring_relay(1, 1, 1)
    with scope("ring1_2a"):
        ring_relay(1, 2, 0)
    with scope("cols0_relay"):
        for t in range(2):
            column_relay(0, t)
    with scope("ring1_2b"):
        ring_relay(1, 2, 1)
    with scope("cols0_finish"):
        for t in range(2):
            sl_b[t] = column_finish(0, t)
            turn(t)

    def sliding_term(v, c):
        for t in range(2):
            term = slide_term(t, v)
            sig[t, 2 * v] = term[0:8]
            sig[t, 2 * v + 1] = term[8:16]
        return c

    with scope("sigma"):
        lax.fori_loop(0, VARS, sliding_term, 0)
        out_start(3)
        sig_gat[tm] = sig[:, pl.ds(5 * y, 5)]
    with scope("ring1_3a"):
        ring_relay(1, 3, 0)
    with scope("cols1_relay"):
        for t in range(2):
            column_relay(1, t)
    with scope("back_rest"):
        settle(back_view(1), receive=br.at[1])
        settle(back_view(2), receive=br.at[2])
    with scope("u1"):
        for t in range(2):
            for v in range(VARS):
                for c in range(4):
                    late = tiles_of(tem, t, v, c)
                    rest = res_ref[t, v, rows(c), :] + late
                    if c == 3:
                        rest = rest + jnp.concatenate([sig[t, 2 * v], sig[t, 2 * v + 1]], axis=0)
                    state = ub[0, t, v, rows(c), :] - step_size * rest
                    ub[1, t, v, rows(c), :] = state
                    ub[2, t, v, rows(c), :] = state - step_size * late
        pack_traces(2)
    with scope("ring1_3b"):
        ring_relay(1, 3, 1)
    with scope("volume1"):
        volume_part(2)
    with scope("ring1_4"):
        for t in range(2):
            ring_relay(1, 4, t)
            column_start(2, t)
    with scope("out_term"):
        settle(out_view(3, 7), receive=fr.at[OUT_SEM[3]])
    with scope("derive_term"):
        lax.fori_loop(0, 5, derive_term, 0)
        back_start(3)
        sig_tem[:, pl.ds(5 * y, 5)] = sig_dt[y]
    with scope("cols1_finish"):
        for t in range(2):
            sl_b[t] = column_finish(1, t)
            turn(t)

        def twice(v, c):
            for t in range(2):
                tw_b[t, v] = step_size * slide_term(t, v)
            return c

        lax.fori_loop(0, VARS, twice, 0)
    with scope("first1"):
        first_direction(2)
    with scope("sends_early"):
        settle(out_view(0, 7), send=fs.at[0])
        for kind in (1, 2):
            settle(out_view(kind, 3), send=fs.at[kind])
            settle(out_view(kind, 4), send=xs.at[kind - 1])
        for kind in (0, 1, 2, 4, 5):
            settle(back_view(kind), send=bs.at[kind])
        for kind in range(2):
            settle(ring[0][0].at[pl.ds(0, 6)], send=cs.at[kind])
        for t in range(2):
            settle(ring[0][t].at[pl.ds(0, 7)], send=zs.at[t])
        for it in range(ITERS):
            settle(packs.at[it], send=ps.at[it])
    with scope("cols2_relay"):
        for t in range(2):
            column_relay(2, t)
    with scope("back_late"):
        for kind in (4, 5, 6, 3):
            settle(back_view(kind), receive=br.at[kind])
    with scope("without_slide"):
        for t in range(2):
            for v in range(VARS):
                for c in range(4):
                    late = tiles_of(tem2, t, v, c)
                    if c == 3:
                        late = late + term_tiles(t, v)
                    total = res_ref[t, v, rows(c), :] + (tiles_of(tem, t, v, c) - step_size * late)
                    res_ref[t, v, rows(c), :] = total
                    if c < 3:
                        new_ref[t, v, rows(c), :] = ub[1, t, v, rows(c), :] - step_size * total
    with scope("cols2_finish"):
        for t in range(2):
            sl_b[t] = column_finish(2, t) - tw_b[t]
            turn(t)

    def finish(v, c):
        for t in range(2):
            total = res_ref[t, v, rows(3), :] + slide_term(t, v)
            res_ref[t, v, rows(3), :] = total
            new_ref[t, v, rows(3), :] = ub[1, t, v, rows(3), :] - step_size * total
        return c

    with scope("finish"):
        lax.fori_loop(0, VARS, finish, 0)
    with scope("sends"):
        settle(out_view(3, 7), send=fs.at[3])
        for kind in (3, 6):
            settle(back_view(kind), send=bs.at[kind])
        settle(ring[0][0].at[pl.ds(0, 6)], send=cs.at[2])
        for t in range(2):
            settle(ring[1][t].at[pl.ds(0, 7)], send=zs.at[2 + t])


def per_device(conserved_field, face_neighbours, counterpart_group, counterpart_shift, volume_operator, flux_matrix):
    state = pltpu.VMEM(conserved_field.shape, jnp.float32)
    vmem = pl.BlockSpec(memory_space=pltpu.VMEM)
    f32, bf16 = jnp.float32, jnp.bfloat16
    dma = pltpu.SemaphoreType.DMA
    return pl.pallas_call(
        kernel,
        out_shape=(state, state),
        in_specs=[pl.BlockSpec(memory_space=pltpu.HBM)] * 6,
        out_specs=(vmem, vmem),
        scratch_shapes=[
            pltpu.VMEM((2, LANES), jnp.int32),
            pltpu.SMEM((2,), jnp.int32),
            pltpu.SMEM((2,), jnp.int32),
            pltpu.VMEM((2, NODES, NODES), f32),
            pltpu.SMEM((VARS, 2, VARS), f32),
            pltpu.VMEM((3, 2, VARS, NODES, LANES), f32),
            pltpu.VMEM((VARS * NODES, VARS * NODES), bf16),
            pltpu.VMEM((VARS * NODES, VARS * NODES), bf16),
            pltpu.VMEM((2, 4, 20, 8, LANES), f32),
            pltpu.VMEM((TM, 2, 20, 8, LANES), f32),
            pltpu.VMEM((4, 2, 20, 8, LANES), f32),
            pltpu.VMEM((4, 2, 20, 8, LANES), f32),
            pltpu.VMEM((2, 4, 20, 8, LANES), f32),
            pltpu.VMEM((2, 4, 20, 8, LANES), f32),
            pltpu.VMEM((2, 20, 8, LANES), f32),
            pltpu.VMEM((TM, 2, 5, 8, LANES), f32),
            pltpu.VMEM((4, 2, 5, 8, LANES), f32),
            pltpu.VMEM((2, 20, 8, LANES), f32),
            *[pltpu.VMEM((Z, VARS, 16, LANES), f32)] * 4,
            *[pltpu.VMEM((Q, VARS, 16, LANES), f32)] * 6,
            pltpu.VMEM((ITERS, 2, 16, LANES), f32),
            pltpu.VMEM((ITERS, 2, 16, LANES), f32),
            pltpu.VMEM((3, NODES, LANES), f32),
            pltpu.VMEM((2, VARS, 16, LANES), f32),
            pltpu.VMEM((2, VARS, 16, LANES), f32),
            pltpu.VMEM((2, VARS, 16, LANES), f32),
            pltpu.VMEM((2, VARS, 16, LANES), f32),
            dma((6,)),
            dma((4,)), dma((8,)),
            dma((7,)), dma((7,)),
            dma((4,)), dma((16 * PARTS,)),
            dma((3,)), dma((12,)),
            dma((2,)), dma((2,)),
            dma((2,)), dma((2,)),
        ],
        compiler_params=pltpu.CompilerParams(
            collective_id=0, has_side_effects=True, vmem_limit_bytes=60 * 1024 * 1024),
        name="iterations",
    )(conserved_field, face_neighbours, counterpart_group, counterpart_shift, volume_operator,
      jnp.transpose(flux_matrix, (1, 0, 2)))


def solution(mesh):
    return jax.shard_map(
        per_device,
        mesh=mesh,
        in_specs=(P("tm", None, None, "space"), P(None, "space"), P("tm"), P("tm"), P(), P()),
        out_specs=(P("tm", None, None, "space"), P("tm", None, None, "space")),
        check_vma=False,
    )
```

```python
import math

import jax
import jax.numpy as jnp
from jax import lax
from jax.experimental import pallas as pl
from jax.experimental.pallas import tpu as pltpu
from jax.sharding import PartitionSpec as P

SAMPLE_COUNT = 16
REACH = 4
ITERS = 2
VARS = 10
NODES = 64
LANES = 128
PARTS = 5
PIECE = VARS // PARTS

lift_scale = 2.0
dissipation = 1.5
angular_speed = 0.5
damping_factor = 4.0
pseudo_step = 0.2

MESH = pl.DeviceIdType.MESH
MOVES = ((2, 1), (1, 1), (3, 1), (0, 1), (2, 0), (1, 0), (3, 0))
TM = 8
SP = 32
Z = 8
Q = 4


def spectral_weights():
    half = SAMPLE_COUNT // 2
    weights = []
    for m in range(1, half):
        total = 0.0
        for k in range(1, half):
            gain = 2.0 * angular_speed * k * math.exp(-damping_factor * (k / half) ** 8) / SAMPLE_COUNT
            total += gain * math.sin(2.0 * math.pi * k * m / SAMPLE_COUNT)
        weights.append(total)
    return weights


def spectral_squares():
    first = [0.0] + spectral_weights() + [0.0]
    full = first + [-first[SAMPLE_COUNT - m] for m in range(SAMPLE_COUNT // 2 + 1, SAMPLE_COUNT)]
    return [
        sum(full[j] * full[(m - j) % SAMPLE_COUNT] for j in range(SAMPLE_COUNT))
        for m in range(SAMPLE_COUNT // 2 + 1)
    ]


def slide_place(v, h):
    index = 2 * v + h
    return index // 5, index % 5


def other_place(v, c, h):
    index = 6 * v + 2 * c + h
    return index // 15, 5 + index % 15


def pick(index, values):
    out = jnp.float32(values[0])
    for k in range(1, len(values)):
        out = jnp.where(index == k, jnp.float32(values[k]), out)
    return out


def kernel(
    u_hbm, fn_hbm, group_hbm, shift_hbm, vol_hbm, flux_hbm,
    new_ref, res_ref, fn_ref, group_ref, shift_ref, vol_ref, flux_ref,
    ub, a_hi, a_lo, up, gat, dt, dt2, tem, tem2, sig, sig_gat, sig_dt, sig_tem, ring_00, ring_01, ring_10, ring_11, cols_00, cols_01, cols_10, cols_11, cols_20, cols_21,
    packs, packed, side, lo_b, up_b, sl_b, tw_b, in_sem, fs, fr, bs, br, zs, zr, cs, cr, ps, pr, xs, xr,
):
    ring = ((ring_00, ring_01), (ring_10, ring_11))
    cols = ((cols_00, cols_01), (cols_10, cols_11), (cols_20, cols_21))
    tm = lax.axis_index("tm")
    sp = lax.axis_index("space")
    z = sp // Q
    q = sp % Q
    y = tm // 2
    side_x = tm % 2

    def space_of(zz, qq):
        return zz * Q + qq

    z_up = space_of((z + 1) % Z, q)
    z_dn = space_of((z + Z - 1) % Z, q)
    mate = space_of(z, q + 1 - 2 * (q % 2))
    cross = space_of(z, (q + 2) % Q)
    after = (sp + 1) % SP
    before = (sp + SP - 1) % SP

    loads = [
        pltpu.make_async_copy(source, target, in_sem.at[k])
        for k, (source, target) in enumerate((
            *((u_hbm.at[t, pl.ds(5 * h, 5)], ub.at[0, t, pl.ds(5 * h, 5)]) for t in range(2) for h in range(2)),
            (flux_hbm, flux_ref), (vol_hbm, vol_ref),
            (fn_hbm, fn_ref), (group_hbm, group_ref), (shift_hbm, shift_ref)))
    ]
    for load in loads:
        load.start()

    barrier = pltpu.get_barrier_semaphore()
    for k in range(1, TM):
        pl.semaphore_signal(barrier, inc=1, device_id={"tm": (tm + k) % TM}, device_id_type=MESH)
    for other in (z_up, z_dn, mate, cross, after, before):
        pl.semaphore_signal(barrier, inc=1, device_id={"space": other}, device_id_type=MESH)
    with jax.named_scope("entry"):
        for load in loads[:4]:
            load.wait()
        pl.semaphore_wait(barrier, TM - 1 + 6)

    lane16 = lax.broadcasted_iota(jnp.int32, (16, LANES), 1)

    weights = spectral_weights()
    squares = spectral_squares()
    cosines = [math.cos(2.0 * math.pi * k / SAMPLE_COUNT) for k in range(SAMPLE_COUNT)]
    sines = [math.sin(2.0 * math.pi * k / SAMPLE_COUNT) for k in range(SAMPLE_COUNT)]

    OUT = ((0, 5), (5, 5), (10, 10))
    BACK = ((0, 5), (5, 5), (10, 10), None, (0, 5), (5, 5), (10, 10))

    OUT_SEM = (0, 1, 4, 7)

    def settle(view, send=None, receive=None):
        copy = pltpu.make_async_remote_copy(
            src_ref=view, dst_ref=view, send_sem=bs.at[0] if send is None else send,
            recv_sem=br.at[0] if receive is None else receive, device_id={"tm": (tm + 1) % TM}, device_id_type=MESH)
        if send is None:
            copy.wait_recv()
        else:
            copy.wait_send()

    def out_view(kind, count):
        if kind == 3:
            return sig_gat.at[pl.ds(0, count)]
        return gat.at[pl.ds(0, count), :, pl.ds(*OUT[kind])]

    def back_view(kind):
        if kind == 3:
            return sig_tem.at[:, pl.ds(0, 15)]
        return (tem2 if kind > 3 else tem).at[:, pl.ds(0, 3), pl.ds(*BACK[kind])]

    def peer_at(k, sign):
        dy, dx = MOVES[k]
        row = (y + sign * dy + 4) % 4
        return row, row * 2 + (side_x + dx) % 2

    def out_refs(kind, row, place):
        if kind == 3:
            return sig.at[:, pl.ds(5 * row, 5)], sig_gat.at[place]
        tiles = pl.ds(*OUT[kind])
        return up.at[:, row, tiles], gat.at[place, :, tiles]

    def back_refs(kind, row, place):
        if kind == 3:
            return sig_dt.at[row], sig_tem.at[:, pl.ds(5 * place, 5)]
        tiles = pl.ds(*BACK[kind])
        source, target = (dt2, tem2) if kind > 3 else (dt, tem)
        return source.at[row, :, tiles], target.at[:, place, tiles]

    def out_copy(kind, k):
        row, peer = peer_at(k, 1)
        source, target = out_refs(kind, row, tm)
        return pltpu.make_async_remote_copy(
            src_ref=source, dst_ref=target, send_sem=fs.at[kind], recv_sem=fr.at[OUT_SEM[kind] + (k - 4 if kind in (1, 2) else 0)],
            device_id={"tm": peer}, device_id_type=MESH)

    def out_arrival(kind, k):
        row, peer = peer_at(k, -1)
        source, target = out_refs(kind, row, peer)
        return pltpu.make_async_remote_copy(
            src_ref=source, dst_ref=target, send_sem=fs.at[kind], recv_sem=fr.at[OUT_SEM[kind] + (k - 4 if kind in (1, 2) else 0)],
            device_id={"tm": peer}, device_id_type=MESH)

    def back_copy(kind, k):
        row, peer = peer_at(k, 1)
        source, target = back_refs(kind, row, y)
        return pltpu.make_async_remote_copy(
            src_ref=source, dst_ref=target, send_sem=bs.at[kind], recv_sem=br.at[kind],
            device_id={"tm": peer}, device_id_type=MESH)

    def out_start(kind):
        for k in range(7) if kind in (0, 3) else range(4, 7):
            out_copy(kind, k).start()

    def pass_on(kind, k, side):
        row = (y if k == 7 else peer_at(k, -1)[0])
        place = row * 2 + (side_x if side == 0 else 1 - side_x)
        block = gat.at[place, :, pl.ds(*OUT[kind])]
        return pltpu.make_async_remote_copy(
            src_ref=block, dst_ref=block, send_sem=xs.at[kind - 1], recv_sem=xr.at[kind - 1],
            device_id={"tm": y * 2 + 1 - side_x}, device_id_type=MESH)

    def relay_points(kind, moves):
        for k in moves:
            out_arrival(kind, k).wait_recv()
            pass_on(kind, k, 0).start()

    def wait_points(kind):
        settle(out_view(kind, 4), receive=xr.at[kind - 1])

    def back_start(kind):
        for k in range(4, 7):
            back_copy(kind, k).start()

    def ring_slot(step, way, t, part):
        return 12 * PARTS + t if step == 4 else (((step - 1) * 2 + way) * 2 + t) * PARTS + part

    def ring_copy(it, step, way, t, part):
        if way == 0:
            origin, target = (z + Z - (step - 1)) % Z, z_up
        else:
            origin, target = (z + step - 1) % Z, z_dn
        block = ring[it][t].at[origin, pl.ds(part * PIECE, PIECE)]
        slot = ring_slot(step, way, t, part)
        return pltpu.make_async_remote_copy(
            src_ref=block, dst_ref=block, send_sem=zs.at[it * 2 + t], recv_sem=zr.at[slot],
            device_id={"space": target}, device_id_type=MESH)

    def ring_arrival(it, step, way, t, part):
        if way == 0:
            origin, target = (z + Z - step) % Z, z_up
        else:
            origin, target = (z + step) % Z, z_dn
        block = ring[it][t].at[origin, pl.ds(part * PIECE, PIECE)]
        slot = ring_slot(step, way, t, part)
        return pltpu.make_async_remote_copy(
            src_ref=block, dst_ref=block, send_sem=zs.at[it * 2 + t], recv_sem=zr.at[slot],
            device_id={"space": target}, device_id_type=MESH)

    def column_copy(kind, hop, t):
        origin, target = ((q, mate), (q, cross), ((q + 2) % Q, mate))[hop]
        block = cols[kind][t].at[origin]
        place = kind * 4 + t + (2 if hop == 1 else 0)
        return pltpu.make_async_remote_copy(
            src_ref=block, dst_ref=block, send_sem=cs.at[kind], recv_sem=cr.at[place],
            device_id={"space": target}, device_id_type=MESH)

    def pack_copy(it, way):
        target = (after, before)[way]
        return pltpu.make_async_remote_copy(
            src_ref=packs.at[it, way], dst_ref=packed.at[it, way], send_sem=ps.at[it], recv_sem=pr.at[it],
            device_id={"space": target}, device_id_type=MESH)

    def build_matrix():
        row = lax.broadcasted_iota(jnp.int32, (NODES, LANES), 0)
        lane = lax.broadcasted_iota(jnp.int32, (NODES, LANES), 1)
        first = lane < NODES
        on = row == jnp.bitwise_and(lane, NODES - 1)
        one, zero = jnp.float32(1.0), jnp.float32(0.0)
        lower = jnp.where(on & (row < 16), one, zero)
        upper = jnp.where(on & (row >= 48), one, zero)
        slide = jnp.where(on & (jnp.bitwise_and(row, 3) == 3), one, zero)
        scale = jnp.float32(0.5 * lift_scale)
        side[0] = jnp.concatenate([vol_ref[0], vol_ref[0]], axis=1) + scale * (lower - upper)
        side[1] = jnp.concatenate([vol_ref[1], vol_ref[1]], axis=1) - scale * slide
        side[2] = (scale * jnp.float32(dissipation)) * (lower + upper + slide)

        def row_block(v, carry):
            for j in range(VARS // 2):
                tile = jnp.zeros((NODES, LANES), jnp.float32)
                for d in range(2):
                    factor = jnp.where(first, flux_ref[v, d, 2 * j], flux_ref[v, d, 2 * j + 1])
                    tile = tile + factor * side[d]
                own = jnp.where(first, jnp.where(v == 2 * j, one, zero), jnp.where(v == 2 * j + 1, one, zero))
                tile = tile + own * side[2]
                high = tile.astype(jnp.bfloat16)
                where = (pl.ds(pl.multiple_of(v * NODES, NODES), NODES), pl.ds(j * LANES, LANES))
                a_hi[where] = high
                a_lo[where] = (tile - high.astype(jnp.float32)).astype(jnp.bfloat16)
            return carry

        lax.fori_loop(0, VARS, row_block, 0)

    def volume_part(it):
        u = jnp.concatenate(
            [ub[it, 0].reshape(VARS * NODES, LANES), ub[it, 1].reshape(VARS * NODES, LANES)], axis=1)
        high = u.astype(jnp.bfloat16)
        low = (u - high.astype(jnp.float32)).astype(jnp.bfloat16)
        for part in range(2):
            rows = pl.ds(part * 320, 320)
            out = jnp.dot(a_hi[rows, :], high, preferred_element_type=jnp.float32)
            out = out + jnp.dot(a_hi[rows, :], low, preferred_element_type=jnp.float32)
            out = out + jnp.dot(a_lo[rows, :], high, preferred_element_type=jnp.float32)
            for t in range(2):
                res_ref[t, pl.ds(part * 5, 5)] = out[:, t * LANES:(t + 1) * LANES].reshape(5, NODES, LANES)

    def ring_chunks(step, t):
        ways = (0, 1) if step < 4 else (t,)
        return [(way, part) for part in range(PARTS) for way in ways]

    def ring_start(it, t):
        for way, part in ring_chunks(1, t):
            ring_copy(it, 1, way, t, part).start()

    def ring_relay(it, step, t):
        if step == 4:
            settle(ring[it][t].at[0], receive=zr.at[ring_slot(4, t, t, 0)])
            return
        onward = ring_chunks(step + 1, t)
        for way, part in ring_chunks(step, t):
            ring_arrival(it, step, way, t, part).wait_recv()
            if (way, part) in onward:
                ring_copy(it, step + 1, way, t, part).start()

    def pack_traces(it):
        up_pack = jnp.zeros((16, LANES), jnp.float32)
        lo_pack = jnp.zeros((16, LANES), jnp.float32)
        for i in range(2 * VARS):
            mine = (lane16 >= REACH * i) & (lane16 < REACH * (i + 1))
            u_face = ub[it, i // VARS, i % VARS, pl.ds(48, 16), :]
            l_face = ub[it, i // VARS, i % VARS, pl.ds(0, 16), :]
            up_pack = jnp.where(mine, pltpu.roll(u_face, (REACH * i + REACH) % LANES, 1), up_pack)
            lo_pack = jnp.where(mine, pltpu.roll(l_face, REACH * i, 1) if i else l_face, lo_pack)
        packs[it // 2, 0] = up_pack
        packs[it // 2, 1] = lo_pack
        for way in range(2):
            pack_copy(it // 2, way).start()

    scale = jnp.float32(0.5 * lift_scale)
    loss = jnp.float32(0.5 * lift_scale * dissipation)

    def first_direction(it):
        settle(packed.at[it // 2], receive=pr.at[it // 2])
        gidx = sp * LANES + lane16
        back_gap = jnp.bitwise_and(gidx - fn_ref[0:1, :], SP * LANES - 1)
        ahead_gap = jnp.bitwise_and(fn_ref[1:2, :] - gidx, SP * LANES - 1)
        from_before = packed[it // 2, 0]
        from_after = packed[it // 2, 1]
        behind = lane16 - back_gap
        ahead = lane16 + ahead_gap
        for i in range(2 * VARS):
            u_face = ub[it, i // VARS, i % VARS, pl.ds(48, 16), :]
            l_face = ub[it, i // VARS, i % VARS, pl.ds(0, 16), :]
            own = jnp.take_along_axis(u_face, jnp.bitwise_and(behind, LANES - 1), axis=1)
            far = jnp.take_along_axis(from_before, jnp.bitwise_and(behind + REACH * (i + 1), LANES - 1), axis=1)
            lo_b[i // VARS, i % VARS] = jnp.where(behind < 0, far, own)
            own = jnp.take_along_axis(l_face, jnp.bitwise_and(ahead, LANES - 1), axis=1)
            far = jnp.take_along_axis(from_after, jnp.bitwise_and(ahead + REACH * i, LANES - 1), axis=1)
            up_b[i // VARS, i % VARS] = jnp.where(ahead >= LANES, far, own)

        def first_faces(v, c):
            low = -loss * lo_b[:, v]
            upp = -loss * up_b[:, v]
            for w in range(VARS):
                f = scale * flux_ref[v, 0, w]
                low = low - f * lo_b[:, w]
                upp = upp + f * up_b[:, w]
            res_ref[:, v, pl.ds(0, 16), :] += low
            res_ref[:, v, pl.ds(48, 16), :] += upp
            return c

        lax.fori_loop(0, VARS, first_faces, 0)

    half = SAMPLE_COUNT // 2

    def spectral(source, first, second, i):
        x = [source[(side_x + r // 2) % TM, r % 2, i] for r in range(SAMPLE_COUNT)]
        for r in (0, 1, 4, 5):
            near = opposite = None
            for m in range(1, half):
                diff = x[(r + m) % SAMPLE_COUNT] - x[(r - m) % SAMPLE_COUNT]
                one, two = jnp.float32(weights[m - 1]) * diff, jnp.float32(-weights[half - m - 1]) * diff
                near = one if near is None else near + one
                opposite = two if opposite is None else opposite + two
            first[r // 4, r % 2, i] = near
            first[r // 4 + 2, r % 2, i] = opposite
            if second is None:
                continue
            zero, eight = jnp.float32(squares[0]), jnp.float32(squares[half])
            near = zero * x[r] + eight * x[r + half]
            opposite = eight * x[r] + zero * x[r + half]
            for m in range(1, half):
                both = x[(r + m) % SAMPLE_COUNT] + x[(r - m) % SAMPLE_COUNT]
                near = near + jnp.float32(squares[m]) * both
                opposite = opposite + jnp.float32(squares[half - m]) * both
            second[r // 4, r % 2, i] = near
            second[r // 4 + 2, r % 2, i] = opposite

    def derive_state(i, c):
        spectral(gat, dt, dt2, i)
        return c

    def derive_term(i, c):
        spectral(sig_gat, sig_dt, None, i)
        return c

    def rows(c):
        return pl.ds(c, 16, stride=4)

    def tiles_of(buffer, t, v, c):
        places = [slide_place(v, h) if c == 3 else other_place(v, c, h) for h in range(2)]
        return jnp.concatenate([buffer[t, j, i] for j, i in places], axis=0)

    def term_tiles(t, v):
        return jnp.concatenate([sig_tem[t, 2 * v], sig_tem[t, 2 * v + 1]], axis=0)

    def offset_of(kind, t):
        group, shift = group_ref[t], shift_ref[t]
        if kind == 1:
            group = jnp.bitwise_and(2 * group + lax.shift_right_arithmetic(shift, 6), SP - 1)
            shift = jnp.bitwise_and(2 * shift, LANES - 1)
        return group, shift

    lane_b = lax.broadcasted_iota(jnp.int32, (VARS, 16, LANES), 2)

    def column_start(kind, t):
        it = kind // 2
        group, shift = offset_of(kind, t)
        first_dst = jnp.bitwise_and(q - group, Q - 1)
        second_dst = jnp.bitwise_and(q - group - 1, Q - 1)
        first = jnp.bitwise_and(z + lax.shift_right_arithmetic(first_dst + group - q, 2), Z - 1)
        second = jnp.bitwise_and(z + lax.shift_right_arithmetic(second_dst + group + 1 - q, 2), Z - 1)
        cols[kind][t][q] = jnp.where(lane_b >= shift, ring[it][t][first], ring[it][t][second])
        column_copy(kind, 1, t).start()
        column_copy(kind, 0, t).start()

    def column_relay(kind, t):
        settle(cols[kind][t].at[0], receive=cr.at[kind * 4 + 2 + t])
        column_copy(kind, 2, t).start()

    def column_finish(kind, t):
        settle(cols[kind][t].at[pl.ds(0, 2)], receive=cr.at[kind * 4 + t])
        group, shift = offset_of(kind, t)
        first = cols[kind][t][jnp.bitwise_and(q + group, Q - 1)]
        second = cols[kind][t][jnp.bitwise_and(q + group + 1, Q - 1)]
        both = jnp.where(lane_b >= shift, first, second)
        both = pltpu.roll(both.reshape(VARS * 16, LANES), jnp.bitwise_and(LANES - shift, LANES - 1), 1)
        return both.reshape(VARS, 16, LANES)

    def turn(t):
        cosine, sine = pick(2 * tm + t, cosines), pick(2 * tm + t, sines)
        one, two = sl_b[t, 1], sl_b[t, 2]
        sl_b[t, 1] = cosine * one - sine * two
        sl_b[t, 2] = sine * one + cosine * two

    def slide_term(t, v):
        term = -loss * sl_b[t, v]
        for w in range(VARS):
            term = term + (scale * flux_ref[v, 1, w]) * sl_b[t, w]
        return term

    step_size = jnp.float32(pseudo_step)
    scope = jax.named_scope

    with scope("start0"):
        for t in range(2):
            for v in range(VARS):
                points = ub[0, t, v, rows(3), :]
                ring[0][t][z, v] = points
                for h in range(2):
                    j, i = slide_place(v, h)
                    up[t, j, i] = points[8 * h:8 * h + 8]
            ring_start(0, t)
        out_start(0)
        pack_traces(0)
        for t in range(2):
            for v in range(VARS):
                for c in range(3):
                    points = ub[0, t, v, rows(c), :]
                    for h in range(2):
                        j, i = other_place(v, c, h)
                        up[t, j, i] = points[8 * h:8 * h + 8]
        gat[tm] = up[:, y]
        for kind in (1, 2):
            out_start(kind)
            pass_on(kind, 7, 0).start()
    with scope("matrix"):
        for load in loads[4:]:
            load.wait()
        build_matrix()
    with scope("volume0"):
        volume_part(0)
    with scope("ring0_1"):
        ring_relay(0, 1, 0)
        ring_relay(0, 1, 1)
    with scope("ring0_2a"):
        ring_relay(0, 2, 0)
    with scope("out_slide"):
        settle(out_view(0, 7), receive=fr.at[OUT_SEM[0]])
    with scope("derive_slide"):
        lax.fori_loop(0, 5, derive_state, 0)
        back_start(0)
        back_start(4)
        tem[:, y, pl.ds(0, 5)] = dt[y, :, pl.ds(0, 5)]
    with scope("points1"):
        relay_points(1, (5, 6, 4))
    with scope("ring0_2b"):
        ring_relay(0, 2, 1)
    with scope("first0"):
        first_direction(0)
    with scope("ring0_3"):
        ring_relay(0, 3, 0)
    with scope("points2"):
        relay_points(2, (5, 6, 4))
    with scope("ring0_3b"):
        ring_relay(0, 3, 1)
    with scope("back_slide"):
        settle(back_view(0), receive=br.at[0])
    with scope("w"):
        for t in range(2):
            for v in range(VARS):
                rest = res_ref[t, v, rows(3), :] + tiles_of(tem, t, v, 3)
                ring[1][t][z, v] = ub[0, t, v, rows(3), :] - step_size * rest
            ring_start(1, t)
    with scope("ring0_4"):
        for t in range(2):
            ring_relay(0, 4, t)
            column_start(0, t)
    with scope("cols1_start"):
        for t in range(2):
            column_start(1, t)
    with scope("rest1"):
        wait_points(1)
        lax.fori_loop(5, 10, derive_state, 0)
        back_start(1)
        back_start(5)
        tem[:, y, pl.ds(5, 5)] = dt[y, :, pl.ds(5, 5)]
    with scope("ring1_1a"):
        ring_relay(1, 1, 0)
    with scope("rest2"):
        wait_points(2)
        lax.fori_loop(10, 20, derive_state, 0)
        back_start(2)
        back_start(6)
        tem[:, y, pl.ds(10, 10)] = dt[y, :, pl.ds(10, 10)]
        tem2[:, y] = dt2[y]
    with scope("ring1_1b"):
        ring_relay(1, 1, 1)
    with scope("ring1_2a"):
        ring_relay(1, 2, 0)
    with scope("cols0_relay"):
        for t in range(2):
            column_relay(0, t)
    with scope("ring1_2b"):
        ring_relay(1, 2, 1)
    with scope("cols0_finish"):
        for t in range(2):
            sl_b[t] = column_finish(0, t)
            turn(t)

    def sliding_term(v, c):
        for t in range(2):
            term = slide_term(t, v)
            sig[t, 2 * v] = term[0:8]
            sig[t, 2 * v + 1] = term[8:16]
        return c

    with scope("sigma"):
        lax.fori_loop(0, VARS, sliding_term, 0)
        out_start(3)
        sig_gat[tm] = sig[:, pl.ds(5 * y, 5)]
    with scope("ring1_3a"):
        ring_relay(1, 3, 0)
    with scope("cols1_relay"):
        for t in range(2):
            column_relay(1, t)
    with scope("back_rest"):
        settle(back_view(1), receive=br.at[1])
        settle(back_view(2), receive=br.at[2])
    with scope("u1"):
        for t in range(2):
            for v in range(VARS):
                for c in range(4):
                    late = tiles_of(tem, t, v, c)
                    rest = res_ref[t, v, rows(c), :] + late
                    if c == 3:
                        rest = rest + jnp.concatenate([sig[t, 2 * v], sig[t, 2 * v + 1]], axis=0)
                    state = ub[0, t, v, rows(c), :] - step_size * rest
                    ub[1, t, v, rows(c), :] = state
                    ub[2, t, v, rows(c), :] = state - step_size * late
        pack_traces(2)
    with scope("ring1_3b"):
        ring_relay(1, 3, 1)
    with scope("volume1"):
        volume_part(2)
    with scope("ring1_4"):
        for t in range(2):
            ring_relay(1, 4, t)
            column_start(2, t)
    with scope("out_term"):
        settle(out_view(3, 7), receive=fr.at[OUT_SEM[3]])
    with scope("derive_term"):
        lax.fori_loop(0, 5, derive_term, 0)
        back_start(3)
        sig_tem[:, pl.ds(5 * y, 5)] = sig_dt[y]
    with scope("cols1_finish"):
        for t in range(2):
            sl_b[t] = column_finish(1, t)
            turn(t)

        def twice(v, c):
            for t in range(2):
                tw_b[t, v] = step_size * slide_term(t, v)
            return c

        lax.fori_loop(0, VARS, twice, 0)
    with scope("first1"):
        first_direction(2)
    with scope("sends_early"):
        new_ref[...] = ub[1]
        settle(out_view(0, 7), send=fs.at[0])
        for kind in (1, 2):
            settle(out_view(kind, 3), send=fs.at[kind])
            settle(out_view(kind, 4), send=xs.at[kind - 1])
        for kind in (0, 1, 2, 4, 5):
            settle(back_view(kind), send=bs.at[kind])
        for kind in range(2):
            settle(ring[0][0].at[pl.ds(0, 6)], send=cs.at[kind])
        for t in range(2):
            settle(ring[0][t].at[pl.ds(0, 7)], send=zs.at[t])
        for it in range(ITERS):
            settle(packs.at[it], send=ps.at[it])
    with scope("cols2_relay"):
        for t in range(2):
            column_relay(2, t)
    for t in range(2):
        with scope("cols2_finish%d" % t):
            sl_b[t] = column_finish(2, t) - tw_b[t]
            turn(t)

        def slide_part(v, c, t=t):
            res_ref[t, v, rows(3), :] += slide_term(t, v)
            return c

        with scope("slide_part%d" % t):
            lax.fori_loop(0, VARS, slide_part, 0)
    with scope("back_late"):
        for kind in (4, 5, 6, 3):
            settle(back_view(kind), receive=br.at[kind])
    with scope("finish"):
        for t in range(2):
            for v in range(VARS):
                for c in range(4):
                    late = tiles_of(tem2, t, v, c)
                    if c == 3:
                        late = late + term_tiles(t, v)
                    total = res_ref[t, v, rows(c), :] + (tiles_of(tem, t, v, c) - step_size * late)
                    res_ref[t, v, rows(c), :] = jnp.float32(0.5) * total
    with scope("sends"):
        settle(out_view(3, 7), send=fs.at[3])
        for kind in (3, 6):
            settle(back_view(kind), send=bs.at[kind])
        settle(ring[0][0].at[pl.ds(0, 6)], send=cs.at[2])
        for t in range(2):
            settle(ring[1][t].at[pl.ds(0, 7)], send=zs.at[2 + t])


def per_device(conserved_field, face_neighbours, counterpart_group, counterpart_shift, volume_operator, flux_matrix):
    state = pltpu.VMEM(conserved_field.shape, jnp.float32)
    vmem = pl.BlockSpec(memory_space=pltpu.VMEM)
    f32, bf16 = jnp.float32, jnp.bfloat16
    dma = pltpu.SemaphoreType.DMA
    before, half = pl.pallas_call(
        kernel,
        out_shape=(state, state),
        in_specs=[pl.BlockSpec(memory_space=pltpu.HBM)] * 6,
        out_specs=(vmem, vmem),
        scratch_shapes=[
            pltpu.VMEM((2, LANES), jnp.int32),
            pltpu.SMEM((2,), jnp.int32),
            pltpu.SMEM((2,), jnp.int32),
            pltpu.VMEM((2, NODES, NODES), f32),
            pltpu.SMEM((VARS, 2, VARS), f32),
            pltpu.VMEM((3, 2, VARS, NODES, LANES), f32),
            pltpu.VMEM((VARS * NODES, VARS * NODES), bf16),
            pltpu.VMEM((VARS * NODES, VARS * NODES), bf16),
            pltpu.VMEM((2, 4, 20, 8, LANES), f32),
            pltpu.VMEM((TM, 2, 20, 8, LANES), f32),
            pltpu.VMEM((4, 2, 20, 8, LANES), f32),
            pltpu.VMEM((4, 2, 20, 8, LANES), f32),
            pltpu.VMEM((2, 4, 20, 8, LANES), f32),
            pltpu.VMEM((2, 4, 20, 8, LANES), f32),
            pltpu.VMEM((2, 20, 8, LANES), f32),
            pltpu.VMEM((TM, 2, 5, 8, LANES), f32),
            pltpu.VMEM((4, 2, 5, 8, LANES), f32),
            pltpu.VMEM((2, 20, 8, LANES), f32),
            *[pltpu.VMEM((Z, VARS, 16, LANES), f32)] * 4,
            *[pltpu.VMEM((Q, VARS, 16, LANES), f32)] * 6,
            pltpu.VMEM((ITERS, 2, 16, LANES), f32),
            pltpu.VMEM((ITERS, 2, 16, LANES), f32),
            pltpu.VMEM((3, NODES, LANES), f32),
            pltpu.VMEM((2, VARS, 16, LANES), f32),
            pltpu.VMEM((2, VARS, 16, LANES), f32),
            pltpu.VMEM((2, VARS, 16, LANES), f32),
            pltpu.VMEM((2, VARS, 16, LANES), f32),
            dma((9,)),
            dma((4,)), dma((8,)),
            dma((7,)), dma((7,)),
            dma((4,)), dma((12 * PARTS + 2,)),
            dma((3,)), dma((12,)),
            dma((2,)), dma((2,)),
            dma((2,)), dma((2,)),
        ],
        compiler_params=pltpu.CompilerParams(
            collective_id=0, has_side_effects=True, vmem_limit_bytes=60 * 1024 * 1024),
        name="iterations",
    )(conserved_field, face_neighbours, counterpart_group, counterpart_shift, volume_operator,
      jnp.transpose(flux_matrix, (1, 0, 2)))
    return before - jnp.float32(2.0 * pseudo_step) * half, half + half


def solution(mesh):
    return jax.shard_map(
        per_device,
        mesh=mesh,
        in_specs=(P("tm", None, None, "space"), P(None, "space"), P("tm"), P("tm"), P(), P()),
        out_specs=(P("tm", None, None, "space"), P("tm", None, None, "space")),
        check_vma=False,
    )
```

```python
import math

import jax
import jax.numpy as jnp
from jax import lax
from jax.experimental import pallas as pl
from jax.experimental.pallas import tpu as pltpu
from jax.sharding import PartitionSpec as P

SAMPLE_COUNT = 16
REACH = 4
ITERS = 2
VARS = 10
NODES = 64
LANES = 128
PARTS = 5
PIECE = VARS // PARTS
GROUPS = (6, 4)

lift_scale = 2.0
dissipation = 1.5
angular_speed = 0.5
damping_factor = 4.0
pseudo_step = 0.2

MESH = pl.DeviceIdType.MESH
MOVES = ((2, 1), (1, 1), (3, 1), (0, 1), (2, 0), (1, 0), (3, 0))
TM = 8
SP = 32
Z = 8
Q = 4


def spectral_weights():
    half = SAMPLE_COUNT // 2
    weights = []
    for m in range(1, half):
        total = 0.0
        for k in range(1, half):
            gain = 2.0 * angular_speed * k * math.exp(-damping_factor * (k / half) ** 8) / SAMPLE_COUNT
            total += gain * math.sin(2.0 * math.pi * k * m / SAMPLE_COUNT)
        weights.append(total)
    return weights


def spectral_squares():
    first = [0.0] + spectral_weights() + [0.0]
    full = first + [-first[SAMPLE_COUNT - m] for m in range(SAMPLE_COUNT // 2 + 1, SAMPLE_COUNT)]
    return [
        sum(full[j] * full[(m - j) % SAMPLE_COUNT] for j in range(SAMPLE_COUNT))
        for m in range(SAMPLE_COUNT // 2 + 1)
    ]


def slide_place(v, h):
    index = 2 * v + h
    return index // 5, index % 5


def other_place(v, c, h):
    index = 6 * v + 2 * c + h
    return index // 15, 5 + index % 15


def pick(index, values):
    out = jnp.float32(values[0])
    for k in range(1, len(values)):
        out = jnp.where(index == k, jnp.float32(values[k]), out)
    return out


def kernel(
    u_hbm, fn_hbm, group_hbm, shift_hbm, vol_hbm, flux_hbm,
    new_ref, res_ref, fn_ref, group_ref, shift_ref, vol_ref, flux_ref,
    ub, a_hi, a_lo, up, gat, dt, dt2, tem, tem2, sig, sig_gat, sig_dt, sig_tem, ring_000, ring_001, ring_010, ring_011, ring_100, ring_101, ring_110, ring_111, cols_00, cols_01, cols_10, cols_11, cols_20, cols_21,
    packs, packed, side, lo_b, up_b, sl_b, tw_b, in_sem, fs, fr, bs, br, zs, zr, cs, cr, ps, pr, xs, xr,
):
    ring = (((ring_000, ring_001), (ring_010, ring_011)), ((ring_100, ring_101), (ring_110, ring_111)))
    cols = ((cols_00, cols_01), (cols_10, cols_11), (cols_20, cols_21))
    tm = lax.axis_index("tm")
    sp = lax.axis_index("space")
    z = sp // Q
    q = sp % Q
    y = tm // 2
    side_x = tm % 2

    def space_of(zz, qq):
        return zz * Q + qq

    z_up = space_of((z + 1) % Z, q)
    z_dn = space_of((z + Z - 1) % Z, q)
    mate = space_of(z, q + 1 - 2 * (q % 2))
    cross = space_of(z, (q + 2) % Q)
    after = (sp + 1) % SP
    before = (sp + SP - 1) % SP

    loads = [
        pltpu.make_async_copy(source, target, in_sem.at[k])
        for k, (source, target) in enumerate((
            *((u_hbm.at[t, pl.ds(5 * h, 5)], ub.at[0, t, pl.ds(5 * h, 5)]) for t in range(2) for h in range(2)),
            (flux_hbm, flux_ref), (vol_hbm, vol_ref),
            (fn_hbm, fn_ref), (group_hbm, group_ref), (shift_hbm, shift_ref)))
    ]
    for load in loads:
        load.start()

    barrier = pltpu.get_barrier_semaphore()
    for k in range(1, TM):
        pl.semaphore_signal(barrier, inc=1, device_id={"tm": (tm + k) % TM}, device_id_type=MESH)
    for other in (z_up, z_dn, mate, cross, after, before):
        pl.semaphore_signal(barrier, inc=1, device_id={"space": other}, device_id_type=MESH)
    with jax.named_scope("entry"):
        for load in loads[:4]:
            load.wait()
        pl.semaphore_wait(barrier, TM - 1 + 6)

    lane16 = lax.broadcasted_iota(jnp.int32, (16, LANES), 1)

    weights = spectral_weights()
    squares = spectral_squares()
    cosines = [math.cos(2.0 * math.pi * k / SAMPLE_COUNT) for k in range(SAMPLE_COUNT)]
    sines = [math.sin(2.0 * math.pi * k / SAMPLE_COUNT) for k in range(SAMPLE_COUNT)]

    OUT = ((0, 5), (5, 5), (10, 10))
    BACK = ((0, 5), (5, 5), (10, 10), None, (0, 5), (5, 5), (10, 10))

    OUT_SEM = (0, 1, 4, 7)

    def settle(view, send=None, receive=None):
        copy = pltpu.make_async_remote_copy(
            src_ref=view, dst_ref=view, send_sem=bs.at[0] if send is None else send,
            recv_sem=br.at[0] if receive is None else receive, device_id={"tm": (tm + 1) % TM}, device_id_type=MESH)
        if send is None:
            copy.wait_recv()
        else:
            copy.wait_send()

    def out_view(kind, count):
        if kind == 3:
            return sig_gat.at[pl.ds(0, count)]
        return gat.at[pl.ds(0, count), :, pl.ds(*OUT[kind])]

    def back_view(kind):
        if kind == 3:
            return sig_tem.at[:, pl.ds(0, 15)]
        return (tem2 if kind > 3 else tem).at[:, pl.ds(0, 3), pl.ds(*BACK[kind])]

    def peer_at(k, sign):
        dy, dx = MOVES[k]
        row = (y + sign * dy + 4) % 4
        return row, row * 2 + (side_x + dx) % 2

    def out_refs(kind, row, place):
        if kind == 3:
            return sig.at[:, pl.ds(5 * row, 5)], sig_gat.at[place]
        tiles = pl.ds(*OUT[kind])
        return up.at[:, row, tiles], gat.at[place, :, tiles]

    def back_refs(kind, row, place):
        if kind == 3:
            return sig_dt.at[row], sig_tem.at[:, pl.ds(5 * place, 5)]
        tiles = pl.ds(*BACK[kind])
        source, target = (dt2, tem2) if kind > 3 else (dt, tem)
        return source.at[row, :, tiles], target.at[:, place, tiles]

    def out_copy(kind, k):
        row, peer = peer_at(k, 1)
        source, target = out_refs(kind, row, tm)
        return pltpu.make_async_remote_copy(
            src_ref=source, dst_ref=target, send_sem=fs.at[kind], recv_sem=fr.at[OUT_SEM[kind] + (k - 4 if kind in (1, 2) else 0)],
            device_id={"tm": peer}, device_id_type=MESH)

    def out_arrival(kind, k):
        row, peer = peer_at(k, -1)
        source, target = out_refs(kind, row, peer)
        return pltpu.make_async_remote_copy(
            src_ref=source, dst_ref=target, send_sem=fs.at[kind], recv_sem=fr.at[OUT_SEM[kind] + (k - 4 if kind in (1, 2) else 0)],
            device_id={"tm": peer}, device_id_type=MESH)

    def back_copy(kind, k):
        row, peer = peer_at(k, 1)
        source, target = back_refs(kind, row, y)
        return pltpu.make_async_remote_copy(
            src_ref=source, dst_ref=target, send_sem=bs.at[kind], recv_sem=br.at[kind],
            device_id={"tm": peer}, device_id_type=MESH)

    def out_start(kind):
        for k in range(7) if kind in (0, 3) else range(4, 7):
            out_copy(kind, k).start()

    def pass_on(kind, k, side):
        row = (y if k == 7 else peer_at(k, -1)[0])
        place = row * 2 + (side_x if side == 0 else 1 - side_x)
        block = gat.at[place, :, pl.ds(*OUT[kind])]
        return pltpu.make_async_remote_copy(
            src_ref=block, dst_ref=block, send_sem=xs.at[kind - 1], recv_sem=xr.at[kind - 1],
            device_id={"tm": y * 2 + 1 - side_x}, device_id_type=MESH)

    def relay_points(kind, moves):
        for k in moves:
            out_arrival(kind, k).wait_recv()
            pass_on(kind, k, 0).start()

    def wait_points(kind):
        settle(out_view(kind, 4), receive=xr.at[kind - 1])

    def back_start(kind):
        for k in range(4, 7):
            back_copy(kind, k).start()

    def ring_slot(step, way, t, part):
        if step == 4:
            return 12 * PARTS + 2 * t + group_of(part)
        return (((step - 1) * 2 + way) * 2 + t) * PARTS + part

    def group_of(part):
        return int(part * PIECE >= GROUPS[0])

    def ring_block(it, t, origin, part):
        group = group_of(part)
        return ring[it][t][group].at[origin, pl.ds(part * PIECE - group * GROUPS[0], PIECE)]

    def ring_own(it, t, v, points):
        group = int(v >= GROUPS[0])
        ring[it][t][group][z, v - group * GROUPS[0]] = points

    def ring_copy(it, step, way, t, part):
        if way == 0:
            origin, target = (z + Z - (step - 1)) % Z, z_up
        else:
            origin, target = (z + step - 1) % Z, z_dn
        block = ring_block(it, t, origin, part)
        slot = ring_slot(step, way, t, part)
        return pltpu.make_async_remote_copy(
            src_ref=block, dst_ref=block, send_sem=zs.at[it * 2 + t], recv_sem=zr.at[slot],
            device_id={"space": target}, device_id_type=MESH)

    def ring_arrival(it, step, way, t, part):
        if way == 0:
            origin, target = (z + Z - step) % Z, z_up
        else:
            origin, target = (z + step) % Z, z_dn
        block = ring_block(it, t, origin, part)
        slot = ring_slot(step, way, t, part)
        return pltpu.make_async_remote_copy(
            src_ref=block, dst_ref=block, send_sem=zs.at[it * 2 + t], recv_sem=zr.at[slot],
            device_id={"space": target}, device_id_type=MESH)

    def members(group):
        return pl.ds(group * GROUPS[0], GROUPS[group])

    def column_copy(kind, hop, t, group):
        origin, target = ((q, mate), (q, cross), ((q + 2) % Q, mate))[hop]
        block = cols[kind][t].at[origin, members(group)]
        place = kind * 6 + (2 + 2 * t + group if hop == 1 else t)
        return pltpu.make_async_remote_copy(
            src_ref=block, dst_ref=block, send_sem=cs.at[kind], recv_sem=cr.at[place],
            device_id={"space": target}, device_id_type=MESH)

    def pack_copy(it, way):
        target = (after, before)[way]
        return pltpu.make_async_remote_copy(
            src_ref=packs.at[it, way], dst_ref=packed.at[it, way], send_sem=ps.at[it], recv_sem=pr.at[it],
            device_id={"space": target}, device_id_type=MESH)

    def build_matrix():
        row = lax.broadcasted_iota(jnp.int32, (NODES, LANES), 0)
        lane = lax.broadcasted_iota(jnp.int32, (NODES, LANES), 1)
        first = lane < NODES
        on = row == jnp.bitwise_and(lane, NODES - 1)
        one, zero = jnp.float32(1.0), jnp.float32(0.0)
        lower = jnp.where(on & (row < 16), one, zero)
        upper = jnp.where(on & (row >= 48), one, zero)
        slide = jnp.where(on & (jnp.bitwise_and(row, 3) == 3), one, zero)
        scale = jnp.float32(0.5 * lift_scale)
        side[0] = jnp.concatenate([vol_ref[0], vol_ref[0]], axis=1) + scale * (lower - upper)
        side[1] = jnp.concatenate([vol_ref[1], vol_ref[1]], axis=1) - scale * slide
        side[2] = (scale * jnp.float32(dissipation)) * (lower + upper + slide)

        def row_block(v, carry):
            for j in range(VARS // 2):
                tile = jnp.zeros((NODES, LANES), jnp.float32)
                for d in range(2):
                    factor = jnp.where(first, flux_ref[v, d, 2 * j], flux_ref[v, d, 2 * j + 1])
                    tile = tile + factor * side[d]
                own = jnp.where(first, jnp.where(v == 2 * j, one, zero), jnp.where(v == 2 * j + 1, one, zero))
                tile = tile + own * side[2]
                high = tile.astype(jnp.bfloat16)
                where = (pl.ds(pl.multiple_of(v * NODES, NODES), NODES), pl.ds(j * LANES, LANES))
                a_hi[where] = high
                a_lo[where] = (tile - high.astype(jnp.float32)).astype(jnp.bfloat16)
            return carry

        lax.fori_loop(0, VARS, row_block, 0)

    def volume_part(it):
        u = jnp.concatenate(
            [ub[it, 0].reshape(VARS * NODES, LANES), ub[it, 1].reshape(VARS * NODES, LANES)], axis=1)
        high = u.astype(jnp.bfloat16)
        low = (u - high.astype(jnp.float32)).astype(jnp.bfloat16)
        for part in range(2):
            rows = pl.ds(part * 320, 320)
            out = jnp.dot(a_hi[rows, :], high, preferred_element_type=jnp.float32)
            out = out + jnp.dot(a_hi[rows, :], low, preferred_element_type=jnp.float32)
            out = out + jnp.dot(a_lo[rows, :], high, preferred_element_type=jnp.float32)
            for t in range(2):
                res_ref[t, pl.ds(part * 5, 5)] = out[:, t * LANES:(t + 1) * LANES].reshape(5, NODES, LANES)

    def ring_chunks(step, t):
        ways = (0, 1) if step < 4 else (t,)
        return [(way, part) for part in range(PARTS) for way in ways]

    def ring_start(it, t):
        for way, part in ring_chunks(1, t):
            ring_copy(it, 1, way, t, part).start()

    def ring_relay(it, step, t):
        onward = ring_chunks(step + 1, t)
        for way, part in ring_chunks(step, t):
            ring_arrival(it, step, way, t, part).wait_recv()
            if (way, part) in onward:
                ring_copy(it, step + 1, way, t, part).start()

    def ring_last(it, t, group):
        settle(ring[it][t][group].at[0], receive=zr.at[12 * PARTS + 2 * t + group])

    def pack_traces(it):
        up_pack = jnp.zeros((16, LANES), jnp.float32)
        lo_pack = jnp.zeros((16, LANES), jnp.float32)
        for i in range(2 * VARS):
            mine = (lane16 >= REACH * i) & (lane16 < REACH * (i + 1))
            u_face = ub[it, i // VARS, i % VARS, pl.ds(48, 16), :]
            l_face = ub[it, i // VARS, i % VARS, pl.ds(0, 16), :]
            up_pack = jnp.where(mine, pltpu.roll(u_face, (REACH * i + REACH) % LANES, 1), up_pack)
            lo_pack = jnp.where(mine, pltpu.roll(l_face, REACH * i, 1) if i else l_face, lo_pack)
        packs[it // 2, 0] = up_pack
        packs[it // 2, 1] = lo_pack
        for way in range(2):
            pack_copy(it // 2, way).start()

    scale = jnp.float32(0.5 * lift_scale)
    loss = jnp.float32(0.5 * lift_scale * dissipation)

    def first_direction(it):
        settle(packed.at[it // 2], receive=pr.at[it // 2])
        gidx = sp * LANES + lane16
        back_gap = jnp.bitwise_and(gidx - fn_ref[0:1, :], SP * LANES - 1)
        ahead_gap = jnp.bitwise_and(fn_ref[1:2, :] - gidx, SP * LANES - 1)
        from_before = packed[it // 2, 0]
        from_after = packed[it // 2, 1]
        behind = lane16 - back_gap
        ahead = lane16 + ahead_gap
        for i in range(2 * VARS):
            u_face = ub[it, i // VARS, i % VARS, pl.ds(48, 16), :]
            l_face = ub[it, i // VARS, i % VARS, pl.ds(0, 16), :]
            own = jnp.take_along_axis(u_face, jnp.bitwise_and(behind, LANES - 1), axis=1)
            far = jnp.take_along_axis(from_before, jnp.bitwise_and(behind + REACH * (i + 1), LANES - 1), axis=1)
            lo_b[i // VARS, i % VARS] = jnp.where(behind < 0, far, own)
            own = jnp.take_along_axis(l_face, jnp.bitwise_and(ahead, LANES - 1), axis=1)
            far = jnp.take_along_axis(from_after, jnp.bitwise_and(ahead + REACH * i, LANES - 1), axis=1)
            up_b[i // VARS, i % VARS] = jnp.where(ahead >= LANES, far, own)

        def first_faces(v, c):
            low = -loss * lo_b[:, v]
            upp = -loss * up_b[:, v]
            for w in range(VARS):
                f = scale * flux_ref[v, 0, w]
                low = low - f * lo_b[:, w]
                upp = upp + f * up_b[:, w]
            res_ref[:, v, pl.ds(0, 16), :] += low
            res_ref[:, v, pl.ds(48, 16), :] += upp
            return c

        lax.fori_loop(0, VARS, first_faces, 0)

    half = SAMPLE_COUNT // 2

    def spectral(source, first, second, i):
        x = [source[(side_x + r // 2) % TM, r % 2, i] for r in range(SAMPLE_COUNT)]
        for r in (0, 1, 4, 5):
            near = opposite = None
            for m in range(1, half):
                diff = x[(r + m) % SAMPLE_COUNT] - x[(r - m) % SAMPLE_COUNT]
                one, two = jnp.float32(weights[m - 1]) * diff, jnp.float32(-weights[half - m - 1]) * diff
                near = one if near is None else near + one
                opposite = two if opposite is None else opposite + two
            first[r // 4, r % 2, i] = near
            first[r // 4 + 2, r % 2, i] = opposite
            if second is None:
                continue
            zero, eight = jnp.float32(squares[0]), jnp.float32(squares[half])
            near = zero * x[r] + eight * x[r + half]
            opposite = eight * x[r] + zero * x[r + half]
            for m in range(1, half):
                both = x[(r + m) % SAMPLE_COUNT] + x[(r - m) % SAMPLE_COUNT]
                near = near + jnp.float32(squares[m]) * both
                opposite = opposite + jnp.float32(squares[half - m]) * both
            second[r // 4, r % 2, i] = near
            second[r // 4 + 2, r % 2, i] = opposite

    def derive_state(i, c):
        spectral(gat, dt, dt2, i)
        return c

    def derive_term(i, c):
        spectral(sig_gat, sig_dt, None, i)
        return c

    def rows(c):
        return pl.ds(c, 16, stride=4)

    def tiles_of(buffer, t, v, c):
        places = [slide_place(v, h) if c == 3 else other_place(v, c, h) for h in range(2)]
        return jnp.concatenate([buffer[t, j, i] for j, i in places], axis=0)

    def term_tiles(t, v):
        return jnp.concatenate([sig_tem[t, 2 * v], sig_tem[t, 2 * v + 1]], axis=0)

    def offset_of(kind, t):
        group, shift = group_ref[t], shift_ref[t]
        if kind == 1:
            group = jnp.bitwise_and(2 * group + lax.shift_right_arithmetic(shift, 6), SP - 1)
            shift = jnp.bitwise_and(2 * shift, LANES - 1)
        return group, shift

    lane_b = lax.broadcasted_iota(jnp.int32, (VARS, 16, LANES), 2)

    def column_start(kind, t, group):
        it = kind // 2
        block, shift = offset_of(kind, t)
        first_dst = jnp.bitwise_and(q - block, Q - 1)
        second_dst = jnp.bitwise_and(q - block - 1, Q - 1)
        first = jnp.bitwise_and(z + lax.shift_right_arithmetic(first_dst + block - q, 2), Z - 1)
        second = jnp.bitwise_and(z + lax.shift_right_arithmetic(second_dst + block + 1 - q, 2), Z - 1)
        source = ring[it][t][group]
        lanes = lax.broadcasted_iota(jnp.int32, (GROUPS[group], 16, LANES), 2)
        cols[kind][t][q, members(group)] = jnp.where(lanes >= shift, source[first], source[second])
        column_copy(kind, 1, t, group).start()
        column_copy(kind, 0, t, group).start()

    def column_relay(kind, t):
        for group in range(2):
            settle(cols[kind][t].at[0, members(group)], receive=cr.at[kind * 6 + 2 + 2 * t + group])
            column_copy(kind, 2, t, group).start()

    def column_finish(kind, t):
        settle(cols[kind][t].at[pl.ds(0, 2)], receive=cr.at[kind * 6 + t])
        group, shift = offset_of(kind, t)
        first = cols[kind][t][jnp.bitwise_and(q + group, Q - 1)]
        second = cols[kind][t][jnp.bitwise_and(q + group + 1, Q - 1)]
        both = jnp.where(lane_b >= shift, first, second)
        both = pltpu.roll(both.reshape(VARS * 16, LANES), jnp.bitwise_and(LANES - shift, LANES - 1), 1)
        return both.reshape(VARS, 16, LANES)

    def turn(t):
        cosine, sine = pick(2 * tm + t, cosines), pick(2 * tm + t, sines)
        one, two = sl_b[t, 1], sl_b[t, 2]
        sl_b[t, 1] = cosine * one - sine * two
        sl_b[t, 2] = sine * one + cosine * two

    def slide_term(t, v):
        term = -loss * sl_b[t, v]
        for w in range(VARS):
            term = term + (scale * flux_ref[v, 1, w]) * sl_b[t, w]
        return term

    step_size = jnp.float32(pseudo_step)
    scope = jax.named_scope

    with scope("start0"):
        for t in range(2):
            for v in range(VARS):
                points = ub[0, t, v, rows(3), :]
                ring_own(0, t, v, points)
                for h in range(2):
                    j, i = slide_place(v, h)
                    up[t, j, i] = points[8 * h:8 * h + 8]
            ring_start(0, t)
        out_start(0)
        pack_traces(0)
        for t in range(2):
            for v in range(VARS):
                for c in range(3):
                    points = ub[0, t, v, rows(c), :]
                    for h in range(2):
                        j, i = other_place(v, c, h)
                        up[t, j, i] = points[8 * h:8 * h + 8]
        gat[tm] = up[:, y]
        for kind in (1, 2):
            out_start(kind)
            pass_on(kind, 7, 0).start()
    with scope("matrix"):
        for load in loads[4:]:
            load.wait()
        build_matrix()
    with scope("volume0"):
        volume_part(0)
    with scope("ring0_1"):
        ring_relay(0, 1, 0)
        ring_relay(0, 1, 1)
    with scope("ring0_2a"):
        ring_relay(0, 2, 0)
    with scope("out_slide"):
        settle(out_view(0, 7), receive=fr.at[OUT_SEM[0]])
    with scope("derive_slide"):
        lax.fori_loop(0, 5, derive_state, 0)
        back_start(0)
        back_start(4)
        tem[:, y, pl.ds(0, 5)] = dt[y, :, pl.ds(0, 5)]
    with scope("points1"):
        relay_points(1, (5, 6, 4))
    with scope("ring0_2b"):
        ring_relay(0, 2, 1)
    with scope("first0"):
        first_direction(0)
    with scope("ring0_3"):
        ring_relay(0, 3, 0)
    with scope("points2"):
        relay_points(2, (5, 6, 4))
    with scope("ring0_3b"):
        ring_relay(0, 3, 1)
    with scope("back_slide"):
        settle(back_view(0), receive=br.at[0])
    with scope("w"):
        for t in range(2):
            for v in range(VARS):
                rest = res_ref[t, v, rows(3), :] + tiles_of(tem, t, v, 3)
                ring_own(1, t, v, ub[0, t, v, rows(3), :] - step_size * rest)
            ring_start(1, t)
    with scope("ring0_4"):
        for t in range(2):
            for group in range(2):
                ring_last(0, t, group)
                column_start(0, t, group)
    with scope("cols1_start"):
        for t in range(2):
            for group in range(2):
                column_start(1, t, group)
    with scope("rest1"):
        wait_points(1)
        lax.fori_loop(5, 10, derive_state, 0)
        back_start(1)
        back_start(5)
        tem[:, y, pl.ds(5, 5)] = dt[y, :, pl.ds(5, 5)]
    with scope("ring1_1a"):
        ring_relay(1, 1, 0)
    with scope("rest2"):
        wait_points(2)
        lax.fori_loop(10, 20, derive_state, 0)
        back_start(2)
        back_start(6)
        tem[:, y, pl.ds(10, 10)] = dt[y, :, pl.ds(10, 10)]
        tem2[:, y] = dt2[y]
    with scope("ring1_1b"):
        ring_relay(1, 1, 1)
    with scope("ring1_2a"):
        ring_relay(1, 2, 0)
    with scope("cols0_relay"):
        for t in range(2):
            column_relay(0, t)
    with scope("ring1_2b"):
        ring_relay(1, 2, 1)
    with scope("cols0_finish"):
        for t in range(2):
            sl_b[t] = column_finish(0, t)
            turn(t)

    def sliding_term(v, c):
        for t in range(2):
            term = slide_term(t, v)
            sig[t, 2 * v] = term[0:8]
            sig[t, 2 * v + 1] = term[8:16]
        return c

    with scope("sigma"):
        lax.fori_loop(0, VARS, sliding_term, 0)
        out_start(3)
        sig_gat[tm] = sig[:, pl.ds(5 * y, 5)]
    with scope("ring1_3a"):
        ring_relay(1, 3, 0)
    with scope("cols1_relay"):
        for t in range(2):
            column_relay(1, t)
    with scope("back_rest"):
        settle(back_view(1), receive=br.at[1])
        settle(back_view(2), receive=br.at[2])
    with scope("u1"):
        for t in range(2):
            for v in range(VARS):
                for c in range(4):
                    late = tiles_of(tem, t, v, c)
                    rest = res_ref[t, v, rows(c), :] + late
                    if c == 3:
                        rest = rest + jnp.concatenate([sig[t, 2 * v], sig[t, 2 * v + 1]], axis=0)
                    state = ub[0, t, v, rows(c), :] - step_size * rest
                    ub[1, t, v, rows(c), :] = state
                    ub[2, t, v, rows(c), :] = state - step_size * late
        pack_traces(2)
    with scope("ring1_3b"):
        ring_relay(1, 3, 1)
    with scope("volume1"):
        volume_part(2)
    with scope("ring1_4"):
        for t in range(2):
            for group in range(2):
                ring_last(1, t, group)
                column_start(2, t, group)
    with scope("out_term"):
        settle(out_view(3, 7), receive=fr.at[OUT_SEM[3]])
    with scope("derive_term"):
        lax.fori_loop(0, 5, derive_term, 0)
        back_start(3)
        sig_tem[:, pl.ds(5 * y, 5)] = sig_dt[y]
    with scope("cols1_finish"):
        for t in range(2):
            sl_b[t] = column_finish(1, t)
            turn(t)

        def twice(v, c):
            for t in range(2):
                tw_b[t, v] = step_size * slide_term(t, v)
            return c

        lax.fori_loop(0, VARS, twice, 0)
    with scope("first1"):
        first_direction(2)
    with scope("sends_early"):
        new_ref[...] = ub[1]
        settle(out_view(0, 7), send=fs.at[0])
        for kind in (1, 2):
            settle(out_view(kind, 3), send=fs.at[kind])
            settle(out_view(kind, 4), send=xs.at[kind - 1])
        for kind in (0, 1, 2, 4, 5):
            settle(back_view(kind), send=bs.at[kind])
        for kind in range(2):
            settle(gat.at[pl.ds(0, 6), 0], send=cs.at[kind])
        for t in range(2):
            settle(gat.at[pl.ds(0, 7), 0], send=zs.at[t])
        for it in range(ITERS):
            settle(packs.at[it], send=ps.at[it])
    with scope("cols2_relay"):
        for t in range(2):
            column_relay(2, t)
    for t in range(2):
        with scope("cols2_finish%d" % t):
            sl_b[t] = column_finish(2, t) - tw_b[t]
            turn(t)

        def slide_part(v, c, t=t):
            res_ref[t, v, rows(3), :] += slide_term(t, v)
            return c

        with scope("slide_part%d" % t):
            lax.fori_loop(0, VARS, slide_part, 0)
    with scope("back_late"):
        for kind in (4, 5, 6, 3):
            settle(back_view(kind), receive=br.at[kind])
    with scope("finish"):
        for t in range(2):
            for v in range(VARS):
                for c in range(4):
                    late = tiles_of(tem2, t, v, c)
                    if c == 3:
                        late = late + term_tiles(t, v)
                    total = res_ref[t, v, rows(c), :] + (tiles_of(tem, t, v, c) - step_size * late)
                    res_ref[t, v, rows(c), :] = jnp.float32(0.5) * total
    with scope("sends"):
        settle(out_view(3, 7), send=fs.at[3])
        for kind in (3, 6):
            settle(back_view(kind), send=bs.at[kind])
        settle(gat.at[pl.ds(0, 6), 0], send=cs.at[2])
        for t in range(2):
            settle(gat.at[pl.ds(0, 7), 0], send=zs.at[2 + t])


def per_device(conserved_field, face_neighbours, counterpart_group, counterpart_shift, volume_operator, flux_matrix):
    state = pltpu.VMEM(conserved_field.shape, jnp.float32)
    vmem = pl.BlockSpec(memory_space=pltpu.VMEM)
    f32, bf16 = jnp.float32, jnp.bfloat16
    dma = pltpu.SemaphoreType.DMA
    before, half = pl.pallas_call(
        kernel,
        out_shape=(state, state),
        in_specs=[pl.BlockSpec(memory_space=pltpu.HBM)] * 6,
        out_specs=(vmem, vmem),
        scratch_shapes=[
            pltpu.VMEM((2, LANES), jnp.int32),
            pltpu.SMEM((2,), jnp.int32),
            pltpu.SMEM((2,), jnp.int32),
            pltpu.VMEM((2, NODES, NODES), f32),
            pltpu.SMEM((VARS, 2, VARS), f32),
            pltpu.VMEM((3, 2, VARS, NODES, LANES), f32),
            pltpu.VMEM((VARS * NODES, VARS * NODES), bf16),
            pltpu.VMEM((VARS * NODES, VARS * NODES), bf16),
            pltpu.VMEM((2, 4, 20, 8, LANES), f32),
            pltpu.VMEM((TM, 2, 20, 8, LANES), f32),
            pltpu.VMEM((4, 2, 20, 8, LANES), f32),
            pltpu.VMEM((4, 2, 20, 8, LANES), f32),
            pltpu.VMEM((2, 4, 20, 8, LANES), f32),
            pltpu.VMEM((2, 4, 20, 8, LANES), f32),
            pltpu.VMEM((2, 20, 8, LANES), f32),
            pltpu.VMEM((TM, 2, 5, 8, LANES), f32),
            pltpu.VMEM((4, 2, 5, 8, LANES), f32),
            pltpu.VMEM((2, 20, 8, LANES), f32),
            *[pltpu.VMEM((Z, count, 16, LANES), f32) for count in GROUPS] * 4,
            *[pltpu.VMEM((Q, VARS, 16, LANES), f32)] * 6,
            pltpu.VMEM((ITERS, 2, 16, LANES), f32),
            pltpu.VMEM((ITERS, 2, 16, LANES), f32),
            pltpu.VMEM((3, NODES, LANES), f32),
            pltpu.VMEM((2, VARS, 16, LANES), f32),
            pltpu.VMEM((2, VARS, 16, LANES), f32),
            pltpu.VMEM((2, VARS, 16, LANES), f32),
            pltpu.VMEM((2, VARS, 16, LANES), f32),
            dma((9,)),
            dma((4,)), dma((8,)),
            dma((7,)), dma((7,)),
            dma((4,)), dma((12 * PARTS + 4,)),
            dma((3,)), dma((18,)),
            dma((2,)), dma((2,)),
            dma((2,)), dma((2,)),
        ],
        compiler_params=pltpu.CompilerParams(
            collective_id=0, has_side_effects=True, vmem_limit_bytes=60 * 1024 * 1024),
        name="iterations",
    )(conserved_field, face_neighbours, counterpart_group, counterpart_shift, volume_operator,
      jnp.transpose(flux_matrix, (1, 0, 2)))
    return before - jnp.float32(2.0 * pseudo_step) * half, half + half


def solution(mesh):
    return jax.shard_map(
        per_device,
        mesh=mesh,
        in_specs=(P("tm", None, None, "space"), P(None, "space"), P("tm"), P("tm"), P(), P()),
        out_specs=(P("tm", None, None, "space"), P("tm", None, None, "space")),
        check_vma=False,
    )
```

```python
import math

import jax
import jax.numpy as jnp
from jax import lax
from jax.experimental import pallas as pl
from jax.experimental.pallas import tpu as pltpu
from jax.sharding import PartitionSpec as P

SAMPLE_COUNT = 16
REACH = 4
ITERS = 2
VARS = 10
NODES = 64
LANES = 128
PARTS = 5
PIECE = VARS // PARTS
GROUPS = (6, 4)

lift_scale = 2.0
dissipation = 1.5
angular_speed = 0.5
damping_factor = 4.0
pseudo_step = 0.2

MESH = pl.DeviceIdType.MESH
MOVES = ((2, 1), (1, 1), (3, 1), (0, 1), (2, 0), (1, 0), (3, 0))
TM = 8
SP = 32
Z = 8
Q = 4


def spectral_weights():
    half = SAMPLE_COUNT // 2
    weights = []
    for m in range(1, half):
        total = 0.0
        for k in range(1, half):
            gain = 2.0 * angular_speed * k * math.exp(-damping_factor * (k / half) ** 8) / SAMPLE_COUNT
            total += gain * math.sin(2.0 * math.pi * k * m / SAMPLE_COUNT)
        weights.append(total)
    return weights


def spectral_squares():
    first = [0.0] + spectral_weights() + [0.0]
    full = first + [-first[SAMPLE_COUNT - m] for m in range(SAMPLE_COUNT // 2 + 1, SAMPLE_COUNT)]
    return [
        sum(full[j] * full[(m - j) % SAMPLE_COUNT] for j in range(SAMPLE_COUNT))
        for m in range(SAMPLE_COUNT // 2 + 1)
    ]


def slide_place(v, h):
    index = 2 * v + h
    return index // 5, index % 5


def other_place(v, c, h):
    index = 6 * v + 2 * c + h
    return index // 15, 5 + index % 15


def pick(index, values):
    out = jnp.float32(values[0])
    for k in range(1, len(values)):
        out = jnp.where(index == k, jnp.float32(values[k]), out)
    return out


def kernel(
    u_hbm, fn_hbm, group_hbm, shift_hbm, vol_hbm, flux_hbm,
    new_ref, res_ref, fn_ref, group_ref, shift_ref, vol_ref, flux_ref,
    ub, a_hi, a_lo, up, gat, dt, dt2, tem, tem2, sig, sig_gat, sig_dt, sig_tem, ring_000, ring_001, ring_010, ring_011, ring_100, ring_101, ring_110, ring_111, cols_00, cols_01, cols_10, cols_11, cols_20, cols_21,
    packs, packed, side, lo_b, up_b, sl_b, tw_b, in_sem, fs, fr, bs, br, zs, zr, cs, cr, ps, pr, xs, xr,
):
    ring = (((ring_000, ring_001), (ring_010, ring_011)), ((ring_100, ring_101), (ring_110, ring_111)))
    cols = ((cols_00, cols_01), (cols_10, cols_11), (cols_20, cols_21))
    tm = lax.axis_index("tm")
    sp = lax.axis_index("space")
    z = sp // Q
    q = sp % Q
    y = tm // 2
    side_x = tm % 2

    def space_of(zz, qq):
        return zz * Q + qq

    z_up = space_of((z + 1) % Z, q)
    z_dn = space_of((z + Z - 1) % Z, q)
    mate = space_of(z, q + 1 - 2 * (q % 2))
    cross = space_of(z, (q + 2) % Q)
    after = (sp + 1) % SP
    before = (sp + SP - 1) % SP

    loads = [
        pltpu.make_async_copy(source, target, in_sem.at[k])
        for k, (source, target) in enumerate((
            *((u_hbm.at[t, pl.ds(5 * h, 5)], ub.at[0, t, pl.ds(5 * h, 5)]) for t in range(2) for h in range(2)),
            (flux_hbm, flux_ref), (vol_hbm, vol_ref),
            (fn_hbm, fn_ref), (group_hbm, group_ref), (shift_hbm, shift_ref)))
    ]
    for load in loads:
        load.start()

    barrier = pltpu.get_barrier_semaphore()
    for k in range(1, TM):
        pl.semaphore_signal(barrier, inc=1, device_id={"tm": (tm + k) % TM}, device_id_type=MESH)
    for other in (z_up, z_dn, mate, cross, after, before):
        pl.semaphore_signal(barrier, inc=1, device_id={"space": other}, device_id_type=MESH)
    with jax.named_scope("entry"):
        for load in loads[:4]:
            load.wait()
        pl.semaphore_wait(barrier, TM - 1 + 6)

    lane16 = lax.broadcasted_iota(jnp.int32, (16, LANES), 1)

    weights = spectral_weights()
    squares = spectral_squares()
    cosines = [math.cos(2.0 * math.pi * k / SAMPLE_COUNT) for k in range(SAMPLE_COUNT)]
    sines = [math.sin(2.0 * math.pi * k / SAMPLE_COUNT) for k in range(SAMPLE_COUNT)]

    OUT = ((0, 5), (5, 5), (10, 10))
    BACK = ((0, 5), (5, 5), (10, 10), None, (0, 5), (5, 5), (10, 10))

    OUT_SEM = (0, 1, 4, 7)

    def settle(view, send=None, receive=None):
        copy = pltpu.make_async_remote_copy(
            src_ref=view, dst_ref=view, send_sem=bs.at[0] if send is None else send,
            recv_sem=br.at[0] if receive is None else receive, device_id={"tm": (tm + 1) % TM}, device_id_type=MESH)
        if send is None:
            copy.wait_recv()
        else:
            copy.wait_send()

    def out_view(kind, count):
        if kind == 3:
            return sig_gat.at[pl.ds(0, count)]
        return gat.at[pl.ds(0, count), :, pl.ds(*OUT[kind])]

    def back_view(kind):
        if kind == 3:
            return sig_tem.at[:, pl.ds(0, 15)]
        return (tem2 if kind > 3 else tem).at[:, pl.ds(0, 3), pl.ds(*BACK[kind])]

    def peer_at(k, sign):
        dy, dx = MOVES[k]
        row = (y + sign * dy + 4) % 4
        return row, row * 2 + (side_x + dx) % 2

    def out_refs(kind, row, place):
        if kind == 3:
            return sig.at[:, pl.ds(5 * row, 5)], sig_gat.at[place]
        tiles = pl.ds(*OUT[kind])
        return up.at[:, row, tiles], gat.at[place, :, tiles]

    def back_refs(kind, row, place):
        if kind == 3:
            return sig_dt.at[row], sig_tem.at[:, pl.ds(5 * place, 5)]
        tiles = pl.ds(*BACK[kind])
        source, target = (dt2, tem2) if kind > 3 else (dt, tem)
        return source.at[row, :, tiles], target.at[:, place, tiles]

    def out_copy(kind, k):
        row, peer = peer_at(k, 1)
        source, target = out_refs(kind, row, tm)
        return pltpu.make_async_remote_copy(
            src_ref=source, dst_ref=target, send_sem=fs.at[kind], recv_sem=fr.at[OUT_SEM[kind] + (k - 4 if kind in (1, 2) else 0)],
            device_id={"tm": peer}, device_id_type=MESH)

    def out_arrival(kind, k):
        row, peer = peer_at(k, -1)
        source, target = out_refs(kind, row, peer)
        return pltpu.make_async_remote_copy(
            src_ref=source, dst_ref=target, send_sem=fs.at[kind], recv_sem=fr.at[OUT_SEM[kind] + (k - 4 if kind in (1, 2) else 0)],
            device_id={"tm": peer}, device_id_type=MESH)

    def back_copy(kind, k):
        row, peer = peer_at(k, 1)
        source, target = back_refs(kind, row, y)
        return pltpu.make_async_remote_copy(
            src_ref=source, dst_ref=target, send_sem=bs.at[kind], recv_sem=br.at[kind],
            device_id={"tm": peer}, device_id_type=MESH)

    def out_start(kind):
        for k in range(7) if kind in (0, 3) else range(4, 7):
            out_copy(kind, k).start()

    def pass_on(kind, k, side):
        row = (y if k == 7 else peer_at(k, -1)[0])
        place = row * 2 + (side_x if side == 0 else 1 - side_x)
        block = gat.at[place, :, pl.ds(*OUT[kind])]
        return pltpu.make_async_remote_copy(
            src_ref=block, dst_ref=block, send_sem=xs.at[kind - 1], recv_sem=xr.at[kind - 1],
            device_id={"tm": y * 2 + 1 - side_x}, device_id_type=MESH)

    def relay_points(kind, moves):
        for k in moves:
            out_arrival(kind, k).wait_recv()
            pass_on(kind, k, 0).start()

    def wait_points(kind):
        settle(out_view(kind, 4), receive=xr.at[kind - 1])

    def back_start(kind):
        for k in range(4, 7):
            back_copy(kind, k).start()

    def ring_slot(step, way, t, part):
        if step == 4:
            return 12 * PARTS + 2 * t + group_of(part)
        return (((step - 1) * 2 + way) * 2 + t) * PARTS + part

    def group_of(part):
        return int(part * PIECE >= GROUPS[0])

    def ring_block(it, t, origin, part):
        group = group_of(part)
        return ring[it][t][group].at[origin, pl.ds(part * PIECE - group * GROUPS[0], PIECE)]

    def ring_own(it, t, v, points):
        group = int(v >= GROUPS[0])
        ring[it][t][group][z, v - group * GROUPS[0]] = points

    def ring_copy(it, step, way, t, part):
        if way == 0:
            origin, target = (z + Z - (step - 1)) % Z, z_up
        else:
            origin, target = (z + step - 1) % Z, z_dn
        block = ring_block(it, t, origin, part)
        slot = ring_slot(step, way, t, part)
        return pltpu.make_async_remote_copy(
            src_ref=block, dst_ref=block, send_sem=zs.at[it * 2 + t], recv_sem=zr.at[slot],
            device_id={"space": target}, device_id_type=MESH)

    def ring_arrival(it, step, way, t, part):
        if way == 0:
            origin, target = (z + Z - step) % Z, z_up
        else:
            origin, target = (z + step) % Z, z_dn
        block = ring_block(it, t, origin, part)
        slot = ring_slot(step, way, t, part)
        return pltpu.make_async_remote_copy(
            src_ref=block, dst_ref=block, send_sem=zs.at[it * 2 + t], recv_sem=zr.at[slot],
            device_id={"space": target}, device_id_type=MESH)

    def members(group):
        return pl.ds(group * GROUPS[0], GROUPS[group])

    def column_copy(kind, hop, t, group):
        origin, target = ((q, mate), (q, cross), ((q + 2) % Q, mate))[hop]
        block = cols[kind][t].at[origin, members(group)]
        place = kind * 6 + (2 + 2 * t + group if hop == 1 else t)
        return pltpu.make_async_remote_copy(
            src_ref=block, dst_ref=block, send_sem=cs.at[kind], recv_sem=cr.at[place],
            device_id={"space": target}, device_id_type=MESH)

    def pack_copy(it, way):
        target = (after, before)[way]
        return pltpu.make_async_remote_copy(
            src_ref=packs.at[it, way], dst_ref=packed.at[it, way], send_sem=ps.at[it], recv_sem=pr.at[it],
            device_id={"space": target}, device_id_type=MESH)

    def build_matrix():
        row = lax.broadcasted_iota(jnp.int32, (NODES, LANES), 0)
        lane = lax.broadcasted_iota(jnp.int32, (NODES, LANES), 1)
        first = lane < NODES
        on = row == jnp.bitwise_and(lane, NODES - 1)
        one, zero = jnp.float32(1.0), jnp.float32(0.0)
        lower = jnp.where(on & (row < 16), one, zero)
        upper = jnp.where(on & (row >= 48), one, zero)
        slide = jnp.where(on & (jnp.bitwise_and(row, 3) == 3), one, zero)
        scale = jnp.float32(0.5 * lift_scale)
        side[0] = jnp.concatenate([vol_ref[0], vol_ref[0]], axis=1) + scale * (lower - upper)
        side[1] = jnp.concatenate([vol_ref[1], vol_ref[1]], axis=1) - scale * slide
        side[2] = (scale * jnp.float32(dissipation)) * (lower + upper + slide)

        def row_block(v, carry):
            for j in range(VARS // 2):
                tile = jnp.zeros((NODES, LANES), jnp.float32)
                for d in range(2):
                    factor = jnp.where(first, flux_ref[v, d, 2 * j], flux_ref[v, d, 2 * j + 1])
                    tile = tile + factor * side[d]
                own = jnp.where(first, jnp.where(v == 2 * j, one, zero), jnp.where(v == 2 * j + 1, one, zero))
                tile = tile + own * side[2]
                high = tile.astype(jnp.bfloat16)
                where = (pl.ds(pl.multiple_of(v * NODES, NODES), NODES), pl.ds(j * LANES, LANES))
                a_hi[where] = high
                a_lo[where] = (tile - high.astype(jnp.float32)).astype(jnp.bfloat16)
            return carry

        lax.fori_loop(0, VARS, row_block, 0)

    def volume_part(it):
        u = jnp.concatenate(
            [ub[it, 0].reshape(VARS * NODES, LANES), ub[it, 1].reshape(VARS * NODES, LANES)], axis=1)
        high = u.astype(jnp.bfloat16)
        low = (u - high.astype(jnp.float32)).astype(jnp.bfloat16)
        for part in range(2):
            rows = pl.ds(part * 320, 320)
            out = jnp.dot(a_hi[rows, :], high, preferred_element_type=jnp.float32)
            out = out + jnp.dot(a_hi[rows, :], low, preferred_element_type=jnp.float32)
            out = out + jnp.dot(a_lo[rows, :], high, preferred_element_type=jnp.float32)
            for t in range(2):
                res_ref[t, pl.ds(part * 5, 5)] = out[:, t * LANES:(t + 1) * LANES].reshape(5, NODES, LANES)

    def ring_chunks(step, t):
        ways = (0, 1) if step < 4 else (t,)
        return [(way, part) for part in range(PARTS) for way in ways]

    def ring_start(it, t):
        for way, part in ring_chunks(1, t):
            ring_copy(it, 1, way, t, part).start()

    def ring_relay(it, step, t):
        onward = ring_chunks(step + 1, t)
        for way, part in ring_chunks(step, t):
            ring_arrival(it, step, way, t, part).wait_recv()
            if (way, part) in onward:
                ring_copy(it, step + 1, way, t, part).start()

    def ring_last(it, t, group):
        settle(ring[it][t][group].at[0], receive=zr.at[12 * PARTS + 2 * t + group])

    def pack_traces(it):
        up_pack = jnp.zeros((16, LANES), jnp.float32)
        lo_pack = jnp.zeros((16, LANES), jnp.float32)
        for i in range(2 * VARS):
            mine = (lane16 >= REACH * i) & (lane16 < REACH * (i + 1))
            u_face = ub[it, i // VARS, i % VARS, pl.ds(48, 16), :]
            l_face = ub[it, i // VARS, i % VARS, pl.ds(0, 16), :]
            up_pack = jnp.where(mine, pltpu.roll(u_face, (REACH * i + REACH) % LANES, 1), up_pack)
            lo_pack = jnp.where(mine, pltpu.roll(l_face, REACH * i, 1) if i else l_face, lo_pack)
        packs[it // 2, 0] = up_pack
        packs[it // 2, 1] = lo_pack
        for way in range(2):
            pack_copy(it // 2, way).start()

    scale = jnp.float32(0.5 * lift_scale)
    loss = jnp.float32(0.5 * lift_scale * dissipation)

    def first_direction(it):
        settle(packed.at[it // 2], receive=pr.at[it // 2])
        gidx = sp * LANES + lane16
        back_gap = jnp.bitwise_and(gidx - fn_ref[0:1, :], SP * LANES - 1)
        ahead_gap = jnp.bitwise_and(fn_ref[1:2, :] - gidx, SP * LANES - 1)
        from_before = packed[it // 2, 0]
        from_after = packed[it // 2, 1]
        behind = lane16 - back_gap
        ahead = lane16 + ahead_gap
        for i in range(2 * VARS):
            u_face = ub[it, i // VARS, i % VARS, pl.ds(48, 16), :]
            l_face = ub[it, i // VARS, i % VARS, pl.ds(0, 16), :]
            own = jnp.take_along_axis(u_face, jnp.bitwise_and(behind, LANES - 1), axis=1)
            far = jnp.take_along_axis(from_before, jnp.bitwise_and(behind + REACH * (i + 1), LANES - 1), axis=1)
            lo_b[i // VARS, i % VARS] = jnp.where(behind < 0, far, own)
            own = jnp.take_along_axis(l_face, jnp.bitwise_and(ahead, LANES - 1), axis=1)
            far = jnp.take_along_axis(from_after, jnp.bitwise_and(ahead + REACH * i, LANES - 1), axis=1)
            up_b[i // VARS, i % VARS] = jnp.where(ahead >= LANES, far, own)

        def first_faces(v, c):
            low = -loss * lo_b[:, v]
            upp = -loss * up_b[:, v]
            for w in range(VARS):
                f = scale * flux_ref[v, 0, w]
                low = low - f * lo_b[:, w]
                upp = upp + f * up_b[:, w]
            res_ref[:, v, pl.ds(0, 16), :] += low
            res_ref[:, v, pl.ds(48, 16), :] += upp
            return c

        lax.fori_loop(0, VARS, first_faces, 0)

    half = SAMPLE_COUNT // 2

    def spectral(source, first, second, i):
        x = [source[(side_x + r // 2) % TM, r % 2, i] for r in range(SAMPLE_COUNT)]
        for r in (0, 1, 4, 5):
            near = opposite = None
            for m in range(1, half):
                diff = x[(r + m) % SAMPLE_COUNT] - x[(r - m) % SAMPLE_COUNT]
                one, two = jnp.float32(weights[m - 1]) * diff, jnp.float32(-weights[half - m - 1]) * diff
                near = one if near is None else near + one
                opposite = two if opposite is None else opposite + two
            first[r // 4, r % 2, i] = near
            first[r // 4 + 2, r % 2, i] = opposite
            if second is None:
                continue
            zero, eight = jnp.float32(squares[0]), jnp.float32(squares[half])
            near = zero * x[r] + eight * x[r + half]
            opposite = eight * x[r] + zero * x[r + half]
            for m in range(1, half):
                both = x[(r + m) % SAMPLE_COUNT] + x[(r - m) % SAMPLE_COUNT]
                near = near + jnp.float32(squares[m]) * both
                opposite = opposite + jnp.float32(squares[half - m]) * both
            second[r // 4, r % 2, i] = near
            second[r // 4 + 2, r % 2, i] = opposite

    def derive_state(i, c):
        spectral(gat, dt, dt2, i)
        return c

    def derive_term(i, c):
        spectral(sig_gat, sig_dt, None, i)
        return c

    def rows(c):
        return pl.ds(c, 16, stride=4)

    def tiles_of(buffer, t, v, c):
        places = [slide_place(v, h) if c == 3 else other_place(v, c, h) for h in range(2)]
        return jnp.concatenate([buffer[t, j, i] for j, i in places], axis=0)

    def term_tiles(t, v):
        return jnp.concatenate([sig_tem[t, 2 * v], sig_tem[t, 2 * v + 1]], axis=0)

    def offset_of(kind, t):
        group, shift = group_ref[t], shift_ref[t]
        if kind == 1:
            group = jnp.bitwise_and(2 * group + lax.shift_right_arithmetic(shift, 6), SP - 1)
            shift = jnp.bitwise_and(2 * shift, LANES - 1)
        return group, shift

    lane_b = lax.broadcasted_iota(jnp.int32, (VARS, 16, LANES), 2)

    def column_start(kind, t, group):
        it = kind // 2
        block, shift = offset_of(kind, t)
        first_dst = jnp.bitwise_and(q - block, Q - 1)
        second_dst = jnp.bitwise_and(q - block - 1, Q - 1)
        first = jnp.bitwise_and(z + lax.shift_right_arithmetic(first_dst + block - q, 2), Z - 1)
        second = jnp.bitwise_and(z + lax.shift_right_arithmetic(second_dst + block + 1 - q, 2), Z - 1)
        source = ring[it][t][group]
        lanes = lax.broadcasted_iota(jnp.int32, (GROUPS[group], 16, LANES), 2)
        cols[kind][t][q, members(group)] = jnp.where(lanes >= shift, source[first], source[second])
        column_copy(kind, 1, t, group).start()
        column_copy(kind, 0, t, group).start()

    def column_relay(kind, t):
        for group in range(2):
            settle(cols[kind][t].at[0, members(group)], receive=cr.at[kind * 6 + 2 + 2 * t + group])
            column_copy(kind, 2, t, group).start()

    def column_finish(kind, t):
        settle(cols[kind][t].at[pl.ds(0, 2)], receive=cr.at[kind * 6 + t])
        group, shift = offset_of(kind, t)
        first = cols[kind][t][jnp.bitwise_and(q + group, Q - 1)]
        second = cols[kind][t][jnp.bitwise_and(q + group + 1, Q - 1)]
        both = jnp.where(lane_b >= shift, first, second)
        both = pltpu.roll(both.reshape(VARS * 16, LANES), jnp.bitwise_and(LANES - shift, LANES - 1), 1)
        return both.reshape(VARS, 16, LANES)

    def turn(t):
        cosine, sine = pick(2 * tm + t, cosines), pick(2 * tm + t, sines)
        one, two = sl_b[t, 1], sl_b[t, 2]
        sl_b[t, 1] = cosine * one - sine * two
        sl_b[t, 2] = sine * one + cosine * two

    def slide_term(t, v):
        term = -loss * sl_b[t, v]
        for w in range(VARS):
            term = term + (scale * flux_ref[v, 1, w]) * sl_b[t, w]
        return term

    step_size = jnp.float32(pseudo_step)
    scope = jax.named_scope

    with scope("start0"):
        for t in range(2):
            for v in range(VARS):
                points = ub[0, t, v, rows(3), :]
                ring_own(0, t, v, points)
                for h in range(2):
                    j, i = slide_place(v, h)
                    up[t, j, i] = points[8 * h:8 * h + 8]
            ring_start(0, t)
        out_start(0)
        pack_traces(0)
        for t in range(2):
            for v in range(VARS):
                for c in range(3):
                    points = ub[0, t, v, rows(c), :]
                    for h in range(2):
                        j, i = other_place(v, c, h)
                        up[t, j, i] = points[8 * h:8 * h + 8]
        gat[tm] = up[:, y]
        for kind in (1, 2):
            out_start(kind)
            pass_on(kind, 7, 0).start()
    with scope("matrix"):
        for load in loads[4:]:
            load.wait()
        build_matrix()
    with scope("volume0"):
        volume_part(0)
    with scope("ring0_1"):
        ring_relay(0, 1, 0)
        ring_relay(0, 1, 1)
    with scope("ring0_2a"):
        ring_relay(0, 2, 0)
    with scope("out_slide"):
        settle(out_view(0, 7), receive=fr.at[OUT_SEM[0]])
    with scope("derive_slide"):
        lax.fori_loop(0, 5, derive_state, 0)
        back_start(0)
        back_start(4)
        tem[:, y, pl.ds(0, 5)] = dt[y, :, pl.ds(0, 5)]
    with scope("points1"):
        relay_points(1, (5, 6, 4))
    with scope("ring0_2b"):
        ring_relay(0, 2, 1)
    with scope("first0"):
        first_direction(0)
    with scope("ring0_3"):
        ring_relay(0, 3, 0)
    with scope("points2"):
        relay_points(2, (5, 6, 4))
    with scope("ring0_3b"):
        ring_relay(0, 3, 1)
    with scope("back_slide"):
        settle(back_view(0), receive=br.at[0])
    with scope("w"):
        for t in range(2):
            for v in range(VARS):
                rest = res_ref[t, v, rows(3), :] + tiles_of(tem, t, v, 3)
                ring_own(1, t, v, ub[0, t, v, rows(3), :] - step_size * rest)
            ring_start(1, t)
    with scope("ring0_4"):
        for t in range(2):
            for group in range(2):
                ring_last(0, t, group)
                column_start(0, t, group)
    with scope("cols1_start"):
        for t in range(2):
            for group in range(2):
                column_start(1, t, group)
    with scope("rest1"):
        wait_points(1)
        lax.fori_loop(5, 10, derive_state, 0)
        back_start(1)
        back_start(5)
        tem[:, y, pl.ds(5, 5)] = dt[y, :, pl.ds(5, 5)]
    with scope("ring1_1a"):
        ring_relay(1, 1, 0)
    with scope("rest2"):
        wait_points(2)
        lax.fori_loop(10, 20, derive_state, 0)
        back_start(2)
        back_start(6)
        tem[:, y, pl.ds(10, 10)] = dt[y, :, pl.ds(10, 10)]
        tem2[:, y] = dt2[y]
    with scope("ring1_1b"):
        ring_relay(1, 1, 1)
    with scope("ring1_2a"):
        ring_relay(1, 2, 0)
    with scope("cols0_relay"):
        for t in range(2):
            column_relay(0, t)
    with scope("ring1_2b"):
        ring_relay(1, 2, 1)
    with scope("cols0_finish"):
        for t in range(2):
            sl_b[t] = column_finish(0, t)
            turn(t)

    def sliding_term(v, c):
        for t in range(2):
            term = slide_term(t, v)
            sig[t, 2 * v] = term[0:8]
            sig[t, 2 * v + 1] = term[8:16]
        return c

    with scope("sigma"):
        lax.fori_loop(0, VARS, sliding_term, 0)
        out_start(3)
        sig_gat[tm] = sig[:, pl.ds(5 * y, 5)]
    with scope("ring1_3a"):
        ring_relay(1, 3, 0)
    with scope("cols1_relay"):
        for t in range(2):
            column_relay(1, t)
    with scope("back_rest"):
        settle(back_view(1), receive=br.at[1])
        settle(back_view(2), receive=br.at[2])
    with scope("u1"):
        for t in range(2):
            for v in range(VARS):
                for c in range(4):
                    late = tiles_of(tem, t, v, c)
                    rest = res_ref[t, v, rows(c), :] + late
                    if c == 3:
                        rest = rest + jnp.concatenate([sig[t, 2 * v], sig[t, 2 * v + 1]], axis=0)
                    state = ub[0, t, v, rows(c), :] - step_size * rest
                    ub[1, t, v, rows(c), :] = state
                    ub[2, t, v, rows(c), :] = state - step_size * late
        pack_traces(2)
    with scope("ring1_3b"):
        ring_relay(1, 3, 1)
    with scope("volume1"):
        volume_part(2)
    with scope("ring1_4"):
        for t in range(2):
            for group in range(2):
                ring_last(1, t, group)
                column_start(2, t, group)
    with scope("out_term"):
        settle(out_view(3, 7), receive=fr.at[OUT_SEM[3]])
    with scope("derive_term"):
        lax.fori_loop(0, 5, derive_term, 0)
        back_start(3)
        sig_tem[:, pl.ds(5 * y, 5)] = sig_dt[y]
    with scope("cols1_finish"):
        for t in range(2):
            sl_b[t] = column_finish(1, t)
            turn(t)

        def twice(v, c):
            for t in range(2):
                tw_b[t, v] = step_size * slide_term(t, v)
            return c

        lax.fori_loop(0, VARS, twice, 0)
    with scope("first1"):
        first_direction(2)
    with scope("sends_early"):
        settle(out_view(0, 7), send=fs.at[0])
        for kind in (1, 2):
            settle(out_view(kind, 3), send=fs.at[kind])
            settle(out_view(kind, 4), send=xs.at[kind - 1])
        for kind in (0, 1, 2, 4, 5):
            settle(back_view(kind), send=bs.at[kind])
        for kind in range(2):
            settle(gat.at[pl.ds(0, 6), 0], send=cs.at[kind])
        for t in range(2):
            settle(gat.at[pl.ds(0, 7), 0], send=zs.at[t])
        for it in range(ITERS):
            settle(packs.at[it], send=ps.at[it])
    with scope("cols2_relay"):
        for t in range(2):
            column_relay(2, t)
    for t in range(2):
        with scope("cols2_finish%d" % t):
            sl_b[t] = column_finish(2, t) - tw_b[t]
            turn(t)

        def slide_part(v, c, t=t):
            res_ref[t, v, rows(3), :] += slide_term(t, v)
            return c

        with scope("slide_part%d" % t):
            lax.fori_loop(0, VARS, slide_part, 0)
    with scope("back_late"):
        for kind in (4, 5, 6, 3):
            settle(back_view(kind), receive=br.at[kind])
    with scope("finish"):
        for t in range(2):
            for v in range(VARS):
                for c in range(4):
                    late = tiles_of(tem2, t, v, c)
                    if c == 3:
                        late = late + term_tiles(t, v)
                    total = res_ref[t, v, rows(c), :] + (tiles_of(tem, t, v, c) - step_size * late)
                    res_ref[t, v, rows(c), :] = total
                    new_ref[t, v, rows(c), :] = ub[1, t, v, rows(c), :] - step_size * total
    with scope("sends"):
        settle(out_view(3, 7), send=fs.at[3])
        for kind in (3, 6):
            settle(back_view(kind), send=bs.at[kind])
        settle(gat.at[pl.ds(0, 6), 0], send=cs.at[2])
        for t in range(2):
            settle(gat.at[pl.ds(0, 7), 0], send=zs.at[2 + t])


def write_out(new_ref, res_ref, new_hbm, res_hbm, sem):
    copies = [
        pltpu.make_async_copy(source, target, sem.at[k])
        for k, (source, target) in enumerate(((new_ref, new_hbm), (res_ref, res_hbm)))
    ]
    for copy in copies:
        copy.start()
    for copy in copies:
        copy.wait()


def per_device(conserved_field, face_neighbours, counterpart_group, counterpart_shift, volume_operator, flux_matrix):
    state = pltpu.VMEM(conserved_field.shape, jnp.float32)
    vmem = pl.BlockSpec(memory_space=pltpu.VMEM)
    f32, bf16 = jnp.float32, jnp.bfloat16
    dma = pltpu.SemaphoreType.DMA
    after, residual = pl.pallas_call(
        kernel,
        out_shape=(state, state),
        in_specs=[pl.BlockSpec(memory_space=pltpu.HBM)] * 6,
        out_specs=(vmem, vmem),
        scratch_shapes=[
            pltpu.VMEM((2, LANES), jnp.int32),
            pltpu.SMEM((2,), jnp.int32),
            pltpu.SMEM((2,), jnp.int32),
            pltpu.VMEM((2, NODES, NODES), f32),
            pltpu.SMEM((VARS, 2, VARS), f32),
            pltpu.VMEM((3, 2, VARS, NODES, LANES), f32),
            pltpu.VMEM((VARS * NODES, VARS * NODES), bf16),
            pltpu.VMEM((VARS * NODES, VARS * NODES), bf16),
            pltpu.VMEM((2, 4, 20, 8, LANES), f32),
            pltpu.VMEM((TM, 2, 20, 8, LANES), f32),
            pltpu.VMEM((4, 2, 20, 8, LANES), f32),
            pltpu.VMEM((4, 2, 20, 8, LANES), f32),
            pltpu.VMEM((2, 4, 20, 8, LANES), f32),
            pltpu.VMEM((2, 4, 20, 8, LANES), f32),
            pltpu.VMEM((2, 20, 8, LANES), f32),
            pltpu.VMEM((TM, 2, 5, 8, LANES), f32),
            pltpu.VMEM((4, 2, 5, 8, LANES), f32),
            pltpu.VMEM((2, 20, 8, LANES), f32),
            *[pltpu.VMEM((Z, count, 16, LANES), f32) for count in GROUPS] * 4,
            *[pltpu.VMEM((Q, VARS, 16, LANES), f32)] * 6,
            pltpu.VMEM((ITERS, 2, 16, LANES), f32),
            pltpu.VMEM((ITERS, 2, 16, LANES), f32),
            pltpu.VMEM((3, NODES, LANES), f32),
            pltpu.VMEM((2, VARS, 16, LANES), f32),
            pltpu.VMEM((2, VARS, 16, LANES), f32),
            pltpu.VMEM((2, VARS, 16, LANES), f32),
            pltpu.VMEM((2, VARS, 16, LANES), f32),
            dma((9,)),
            dma((4,)), dma((8,)),
            dma((7,)), dma((7,)),
            dma((4,)), dma((12 * PARTS + 4,)),
            dma((3,)), dma((18,)),
            dma((2,)), dma((2,)),
            dma((2,)), dma((2,)),
        ],
        compiler_params=pltpu.CompilerParams(
            collective_id=0, has_side_effects=True, vmem_limit_bytes=60 * 1024 * 1024),
        name="iterations",
    )(conserved_field, face_neighbours, counterpart_group, counterpart_shift, volume_operator,
      jnp.transpose(flux_matrix, (1, 0, 2)))
    shape = jax.ShapeDtypeStruct(conserved_field.shape, f32)
    return pl.pallas_call(
        write_out,
        out_shape=(shape, shape),
        in_specs=(vmem, vmem),
        out_specs=(pl.BlockSpec(memory_space=pltpu.HBM),) * 2,
        scratch_shapes=[dma((2,))],
        name="write_out",
    )(pltpu.with_memory_space_constraint(after, pltpu.VMEM), pltpu.with_memory_space_constraint(residual, pltpu.VMEM))


def solution(mesh):
    return jax.shard_map(
        per_device,
        mesh=mesh,
        in_specs=(P("tm", None, None, "space"), P(None, "space"), P("tm"), P("tm"), P(), P()),
        out_specs=(P("tm", None, None, "space"), P("tm", None, None, "space")),
        check_vma=False,
    )
```
